32 devices in a mesh: dp: 8 (over y, x, core), opt: 4 (over z).
Axes of the slice: x: 2, y: 2, z: 4, core: 2. Of those that a mesh axis runs over, the one named last changes fastest.
Arguments:
- images: bfloat16 [256, 14, 14, 512], P(('dp', 'opt')), may hold values from -6 to 6
- cotangent: bfloat16 [256, 14, 14, 512], P(('dp', 'opt')), may hold values from -6 to 6
- counts: int32 [32], P(('dp', 'opt')), may hold values from 1 to 8, as said below
- rel_index: int32 [49, 49], replicated, may hold values from 0 to 168, as said below
- params: float32 [3158016], P('opt'), may hold values from -3 to 250
- moment1: float32 [3158016], P('opt'), may hold values from -3840 to 3840
- moment2: float32 [3158016], P('opt'), may hold values from 0 to 6400
- rates: float32 [15], replicated, may hold values from 0 to 1
Outputs:
- block_out: bfloat16 [256, 14, 14, 512], P(('dp', 'opt'))
- input_grad: float32 [256, 14, 14, 512], P(('dp', 'opt'))
- param_grad: float32 [3158016], P('opt')
- new_params: float32 [3158016], P('opt')
- new_moment1: float32 [3158016], P('opt')
- new_moment2: float32 [3158016], P('opt')
The draws below stay inside these ranges and needn't reach their ends.
Inputs may be any that keep to these rules, and one draw needn't show every extreme that they name: `counts`: some device has 8 live images and another one in every draw. `rel_index`: two pairs of cells share a bucket exactly when their offsets within the window are equal.
All inputs are finite; a program needn't handle non-finite values.
Results may differ from the reference program's by a relative error of at most 0.02.
Values may be sent and summed in bfloat16 or wider, within the bound.
A program may use at most 256 MiB of HBM per device.

```python
import math
import jax
import jax.numpy as jnp
from jax import lax

D = 512
HEADS = 16
HEAD_DIM = 32
HID = 2048
SIDE = 14
WIN = 7
SHIFT = 3
STEP = 2
GROUPS = 15
IMG_CAP = 8
TAB = 169
SLOTS = 256
PARAMS = 3158016


RATE_BASE = [0.15, 0.2, 0.04, 0.2, 0.2, 0.4, 0.1, 0.2, 0.15, 0.2, 0.04, 0.2, 0.02, 0.2, 0.004]


GRAD_SCALE = [1.7, 1.7, 1.0, 1.0, 1.0, 0.3, 0.5, 1.2, 0.6, 0.6, 0.3, 0.3, 0.65, 1.0, 1.0]


def group_starts_drawn():
    lengths = [D, D, 3 * D * D, D, D, TAB * HEADS, D * D, D, D, D, D * HID, HID, HID * D, D]
    starts = [0]
    for length in lengths:
        starts.append(starts[-1] + length)
    return starts


def per_group(index, table):
    starts = group_starts_drawn()
    value = jnp.zeros(index.shape, jnp.float32) + table[0]
    for group in range(1, len(starts)):
        value = jnp.where(index >= starts[group], jnp.float32(table[group]), value)
    return value


def draw_params(key, part):
    index = lax.iota(jnp.int32, PARAMS)
    starts = group_starts_drawn()
    scales = [0.0, 0.2, D ** (-0.5), 0.2, 0.2, 0.5, (D // 8) ** (-0.5), 0.2, 0.0, 0.2, D ** (-0.5), 0.2, HID ** (-0.5), 0.2, 0.02]
    noise = jnp.clip(jax.random.normal(jax.random.fold_in(key, 1), (PARAMS,), jnp.float32), -6.0, 6.0)
    spread = jax.random.uniform(jax.random.fold_in(key, 2), (PARAMS,), jnp.float32)
    values = per_group(index, scales) * noise
    is_gain = (index < starts[1]) | (index >= starts[8]) & (index < starts[9])
    values = jnp.where(is_gain, 0.6 + 0.8 * spread, values)
    return values


def moment_noise(key):
    first = jnp.clip(jax.random.normal(jax.random.fold_in(key, 11), (PARAMS,), jnp.float32), -6.0, 6.0)
    second = jnp.clip(jax.random.normal(jax.random.fold_in(key, 12), (PARAMS,), jnp.float32), -6.0, 6.0)
    index = lax.iota(jnp.int32, PARAMS)
    tokens_live = SLOTS * SIDE * SIDE * (IMG_CAP + 1) / (2.0 * IMG_CAP)
    scale = per_group(index, GRAD_SCALE) * math.sqrt(tokens_live)
    return (first, second, scale)


def draw_moment1(key, part):
    first, second, scale = moment_noise(key)
    return 0.1 * scale * first


def draw_moment2(key, part):
    first, second, scale = moment_noise(key)
    return 0.001 * scale * scale * (first * first + 0.1 * second * second + 0.01)


def draw_rates(key, part):
    factor = jnp.exp(jax.random.uniform(key, (GROUPS,), jnp.float32, -0.5, 0.5))
    return jnp.array(RATE_BASE, jnp.float32) * factor


def draw_counts(key, part):
    devices_count = SLOTS // IMG_CAP
    values = jax.random.randint(jax.random.fold_in(key, 21), (devices_count,), 1, IMG_CAP + 1)
    anchor = jax.random.randint(jax.random.fold_in(key, 22), (), 0, devices_count)
    position = lax.iota(jnp.int32, devices_count)
    values = jnp.where(position == anchor, IMG_CAP, values)
    values = jnp.where(position == jnp.mod(anchor + 1, devices_count), 1, values)
    return values.astype(jnp.int32)


def draw_rel_index(key, part):
    order = jax.random.permutation(jax.random.fold_in(key, 31), TAB)
    cells = lax.iota(jnp.int32, WIN * WIN)
    first = cells[:, None]
    second = cells[None, :]
    offset = (first // WIN - second // WIN + WIN - 1) * (2 * WIN - 1) + (first % WIN - second % WIN + WIN - 1)
    return order[offset].astype(jnp.int32)


def steps_of(key, dims, shards, smallest, largest):
    def one(axis_at, shards_of):
        heights = jax.random.uniform(jax.random.fold_in(jax.random.fold_in(key, 6), axis_at), (shards_of,), jnp.float32, smallest / len(shards), largest / len(shards))
        return jnp.repeat(jnp.exp(heights), dims[axis_at] // shards_of).reshape((-1,) + (1,) * (len(dims) - axis_at - 1))

    factor_of = one(*shards[0])
    for cut in shards[1:]:
        factor_of = factor_of * one(*cut)
    return factor_of


def centred(key, extent, scale, bound, shards=(), kind=jnp.bfloat16):
    level = steps_of(key, extent, shards, -0.22, 0.18) if shards else 1.0
    values = jax.random.normal(key, extent, jnp.float32) * scale * level
    return jnp.minimum(jnp.maximum(values, -bound), bound).astype(kind)


def setup_inputs(seed: int = 0) -> dict:
    splits = jax.random.split(jax.random.key(seed), 9)
    images = centred(splits[0], (SLOTS, SIDE, SIDE, D), 1.0, 6.0, ((0, 32),))
    cotangent = centred(splits[1], (SLOTS, SIDE, SIDE, D), 1.0, 6.0, ((0, 32),))
    counts = draw_counts(jax.random.fold_in(splits[8], 71), 0)
    rel_index = draw_rel_index(jax.random.fold_in(splits[8], 71), 0)
    params = draw_params(jax.random.fold_in(splits[8], 71), 0)
    moment1 = draw_moment1(jax.random.fold_in(splits[8], 71), 0)
    moment2 = draw_moment2(jax.random.fold_in(splits[8], 71), 0)
    rates = draw_rates(jax.random.fold_in(splits[8], 71), 0)
    return {"images": images, "cotangent": cotangent, "counts": counts, "rel_index": rel_index, "params": params, "moment1": moment1, "moment2": moment2, "rates": rates}


HIGH = lax.Precision.HIGHEST
DECAY = [0.0, 0.0, 0.05, 0.0, 0.0, 0.0, 0.05, 0.0, 0.0, 0.0, 0.05, 0.0, 0.05, 0.0, 0.0]

@jax.custom_vjp
def low(v):
    return lax.optimization_barrier(v.astype(jnp.bfloat16)).astype(jnp.float32)

@jax.custom_vjp
def low_back(v):
    return v

def low_keep(v):
    return (low(v), None)

def low_pass(kept, grad):
    return (grad,)

def back_keep(v):
    return (v, None)

def back_low(kept, grad):
    return (low(grad),)
low.defvjp(low_keep, low_pass)
low_back.defvjp(back_keep, back_low)

def group_starts():
    lengths = [D, D, 3 * D * D, D, D, TAB * HEADS, D * D, D, D, D, D * HID, HID, HID * D, D]
    starts = [0]
    for length in lengths:
        starts.append(starts[-1] + length)
    return starts

def region_map():
    cells = lax.iota(jnp.int32, SIDE)
    band = (cells >= SIDE - WIN).astype(jnp.int32) + (cells >= SIDE - SHIFT).astype(jnp.int32)
    return (band[:, None] * 3 + band[None, :]).astype(jnp.int32)

def layer_norm(field, gain, shift):
    center = lax.optimization_barrier(jnp.mean(field, -1, keepdims=True))
    deviation = field - center
    spread = lax.optimization_barrier(jnp.mean(deviation * deviation, -1, keepdims=True))
    return deviation * lax.rsqrt(spread + 1e-05) * gain + shift

def to_windows(field):
    count, side, width = (field.shape[0], field.shape[1], field.shape[-1])
    blocks = side // WIN
    field = field.reshape(count, blocks, WIN, blocks, WIN, width).transpose(0, 1, 3, 2, 4, 5)
    return field.reshape(count * blocks * blocks * WIN * WIN, width)

def from_windows(rows, count, side):
    blocks = side // WIN
    width = rows.shape[-1]
    field = rows.reshape(count, blocks, blocks, WIN, WIN, width).transpose(0, 1, 3, 2, 4, 5)
    return field.reshape(count, side, side, width)

def block(flat, images, rel_index):
    weights = low(flat)
    starts = group_starts()
    pieces = [weights[starts[g]:starts[g + 1]] for g in range(14)]
    gain_one, bias_one, w_qkv, query_bias, value_bias, table, w_proj, proj_bias = pieces[:8]
    gain_two, bias_two, w_fc1, fc1_bias, w_fc2, fc2_bias = pieces[8:]
    count = images.shape[0]
    blocks = SIDE // WIN
    windows = blocks * blocks
    span = WIN * WIN
    normed = low(layer_norm(images, gain_one, bias_one))
    shifted = to_windows(jnp.roll(normed, (-SHIFT, -SHIFT), (1, 2)))
    qkv_bias = jnp.concatenate([query_bias, jnp.zeros((D,), jnp.float32), value_bias])
    qkv = low_back(jnp.dot(shifted, w_qkv.reshape(D, 3 * D), precision=HIGH) + qkv_bias)
    shape = (count, windows, span, HEADS, HEAD_DIM)
    query = low(qkv[:, :D] * HEAD_DIM ** (-0.5)).reshape(shape)
    keys = low(qkv[:, D:2 * D]).reshape(shape)
    values = low(qkv[:, 2 * D:]).reshape(shape)
    position = table.reshape(TAB, HEADS)[rel_index].transpose(2, 0, 1)
    region_rows = to_windows(region_map().reshape(1, SIDE, SIDE, 1)).reshape(windows, span)
    masking = jnp.where(region_rows[:, :, None] == region_rows[:, None, :], 0.0, -100.0).astype(jnp.float32)
    scores = jnp.einsum('bwqhd,bwkhd->bwhqk', query, keys, precision=HIGH)
    scores = low_back(scores + position[None, None] + masking[None, :, None])
    probs = jax.nn.softmax(scores, axis=-1)
    attended = jnp.einsum('bwhqk,bwkhd->bwqhd', low(probs), values, precision=HIGH)
    attended = low_back(low(attended)).reshape(count * windows * span, D)
    projected = low_back(jnp.dot(attended, w_proj.reshape(D, D), precision=HIGH) + proj_bias)
    middle = images + jnp.roll(from_windows(projected, count, SIDE), (SHIFT, SHIFT), (1, 2))
    hidden_in = low(layer_norm(middle, gain_two, bias_two)).reshape(-1, D)
    pre = low_back(jnp.dot(hidden_in, w_fc1.reshape(D, HID), precision=HIGH) + fc1_bias)
    act = low(jax.nn.gelu(pre, approximate=False))
    mlp = jnp.dot(act, w_fc2.reshape(HID, D), precision=HIGH) + fc2_bias
    return middle + mlp.reshape(middle.shape)

def adam_update(weights, first, second, grad, rates, start):
    index = start + lax.iota(jnp.int32, weights.shape[0])
    starts = group_starts()
    rate = jnp.zeros_like(weights) + rates[0]
    decay = jnp.zeros_like(weights)
    for group in range(1, len(starts)):
        after = index >= starts[group]
        rate = jnp.where(after, rates[group], rate)
        decay = jnp.where(after, DECAY[group], decay)
    first_new = 0.9 * first + 0.1 * grad
    second_new = 0.999 * second + 0.001 * grad * grad
    first_hat = first_new / (1.0 - 0.9 ** STEP)
    second_hat = second_new / (1.0 - 0.999 ** STEP)
    weights_new = weights - rate * (first_hat / (jnp.sqrt(second_hat) + 1e-08) + decay * weights)
    return (weights_new, first_new, second_new)

def reference(images, cotangent, counts, rel_index, params, moment1, moment2, rates):
    group_images = IMG_CAP * 4
    steps_count = SLOTS // group_images
    slot_ids = jnp.arange(SLOTS, dtype=jnp.int32)
    live = (slot_ids % IMG_CAP < counts[slot_ids // IMG_CAP]).astype(jnp.float32)
    shape = (steps_count, group_images, SIDE, SIDE, D)
    inputs = (images.reshape(shape), cotangent.reshape(shape), live.reshape(steps_count, group_images))

    def step(total, item):
        image_group, cot_group, alive = item

        def forward(flat, field):
            return block(flat, field, rel_index)
        outputs, back = jax.vjp(forward, params, image_group.astype(jnp.float32))
        grad_flat, grad_field = back(cot_group.astype(jnp.float32) * alive[:, None, None, None])
        return (total + grad_flat, (outputs.astype(jnp.bfloat16), grad_field))
    grad, (outputs, field_grads) = lax.scan(step, jnp.zeros((PARAMS,), jnp.float32), inputs)
    new_params, new_first, new_second = adam_update(params, moment1, moment2, grad, rates, 0)
    full = (SLOTS, SIDE, SIDE, D)
    return (outputs.reshape(full), field_grads.reshape(full), grad, new_params, new_first, new_second)
```

```python
import math
import jax
import jax.numpy as jnp
from jax import lax
from jax.experimental import pallas as pl
from jax.experimental.pallas import tpu as pltpu

D = 512
HEADS = 16
HEAD_DIM = 32
HID = 2048
SIDE = 14
WIN = 7
SHIFT = 3
TAB = 169
F32 = jnp.float32
BF16 = jnp.bfloat16

IMGS = 8
SPAN = WIN * WIN
WROWS = SPAN * IMGS
ROWS = 4 * WROWS
RS = ROWS + 64
BLK = 224
NBLK = ROWS // BLK
WB = 4 * IMGS
SCALE = HEAD_DIM ** -0.5

R_G1, R_B1, R_QKV, R_BQ, R_BV, R_TAB = 0, 4, 8, 6152, 6156, 6160
R_PROJ, R_BP, R_G2, R_B2, R_W1, R_C1, R_W2, R_C2, R_END = 6181, 8229, 8233, 8237, 8241, 16433, 16449, 24641, 24645
LANE = 16
BROW = 6176


def segments(w):
    if w == 0:
        return [(SHIFT, WIN, 0)]
    return [(WIN + SHIFT, WIN - SHIFT, 0), (0, SHIFT, WIN - SHIFT)]


def window_copies(hbm, vmem, sem, inward):
    out = []
    n = 0
    for wy in range(2):
        for wx in range(2):
            for ys, yl, yo in segments(wy):
                for xs, xl, xo in segments(wx):
                    a = hbm.at[pl.ds(ys, yl), pl.ds(xs, xl)]
                    b = vmem.at[pl.ds((2 * wy + wx) * WIN + yo, yl), pl.ds(xo, xl)]
                    out.append(pltpu.make_async_copy(a, b, sem.at[n]) if inward else pltpu.make_async_copy(b, a, sem.at[n]))
                    n += 1
    return out


NSEG = 9


def dot(a, b):
    return lax.dot_general(a, b, (((1,), (0,)), ((), ())), preferred_element_type=F32)


def dot_nt(a, b):
    return lax.dot_general(a, b, (((1,), (1,)), ((), ())), preferred_element_type=F32)


def dot_tn(a, b):
    return lax.dot_general(a, b, (((0,), (0,)), ((), ())), preferred_element_type=F32)


def norm_stats(x):
    mean = jnp.mean(x, -1, keepdims=True)
    dev = x - mean
    var = jnp.mean(dev * dev, -1, keepdims=True)
    r = lax.rsqrt(var + 1e-05)
    return dev * r, r


def unit_rows(ref3, unit, units):
    return ref3[pl.ds(unit, units)].astype(F32).reshape(units * 8, 128)


def vec_from(fs, row, width, shift):
    parts = []
    lane = lax.broadcasted_iota(jnp.int32, (1, 128), 1)
    for c in range(width // 128):
        a = fs[pl.ds(row + c, 1), :]
        if shift:
            b = fs[pl.ds(row + c + 1, 1), :]
            a = jnp.where(lane < 128 - LANE, pltpu.roll(a, 128 - LANE, 1), pltpu.roll(b, 128 - LANE, 1))
        parts.append(a)
    return jnp.concatenate(parts, 1)


def take_matrix(fs, row, dst, nrows, ncb, shift, step=128):
    lane = lax.broadcasted_iota(jnp.int32, (step, 128), 1)

    def body(t, _):
        base = row + t * (step * ncb)
        r0 = pl.multiple_of(t * step, step)
        for c in range(ncb):
            a = fs[pl.ds(base + c, step, stride=ncb), :]
            if shift:
                b = fs[pl.ds(base + c + 1, step, stride=ncb), :]
                a = jnp.where(lane < 128 - LANE, pltpu.roll(a, 128 - LANE, 1), pltpu.roll(b, 128 - LANE, 1))
            dst[pl.ds(r0, step), c * 128:(c + 1) * 128] = a.astype(BF16)
        return 0

    lax.fori_loop(0, nrows // step, body, 0)


def lane_head():
    return lax.broadcasted_iota(jnp.int32, (64, 128), 1) // HEAD_DIM


def block_diag(v, heads):
    zero = jnp.zeros_like(v)
    return jnp.concatenate([jnp.where(heads == h, v, zero) for h in range(4)], 0)


def diag_sum(r, heads):
    out = r[0:64]
    for h in range(1, 4):
        out = jnp.where(heads == h, r[64 * h:64 * h + 64], out)
    return out


def take_rows(fs, start):
    v = fs[pl.ds(start, 56, stride=IMGS), :]
    v = jnp.where(lax.broadcasted_iota(jnp.int32, (56, 128), 0) < SPAN, v, 0.0)
    return jnp.concatenate([v, jnp.zeros((8, 128), F32)], 0)


def put_rows(fs, start, v):
    fs[pl.ds(start, 48, stride=IMGS), :] = v[0:48]
    fs[pl.ds(start + 48 * IMGS, 1), :] = v[48:49]


def build_bias(tab3, rel_ref, big, bias):
    rel = rel_ref[...]
    row = lax.shift_right_arithmetic(rel, 3)
    low = rel & 7
    oh = (lax.broadcasted_iota(jnp.int32, (32, 4096), 0) == row).astype(F32).astype(BF16)
    tab = jnp.concatenate([tab3, jnp.zeros((8, 128), F32)], 0).astype(BF16)
    r = dot_tn(tab, oh)
    acc = jnp.zeros((16, 4096), F32)
    for j in range(8):
        acc = acc + jnp.where(low == j, r[16 * j:16 * j + 16], 0.0)
    for kk in range(32):
        big[kk * 16:kk * 16 + 16, :] = acc[:, kk * 128:kk * 128 + 128]
    k = lax.broadcasted_iota(jnp.int32, (64, 256), 0)
    q = lax.broadcasted_iota(jnp.int32, (64, 256), 1) & 63
    ki = lax.shift_right_arithmetic(k * 37, 8)
    kj = k - ki * 7
    qi = lax.shift_right_arithmetic(q * 37, 8)
    qj = q - qi * 7
    cut = WIN - SHIFT
    same_y = (ki < cut) == (qi < cut)
    same_x = (kj < cut) == (qj < cut)
    lane = lax.broadcasted_iota(jnp.int32, (32, 128), 1)
    for g in range(4):
        for pair in range(2):
            h = 4 * g + 2 * pair
            a = big[pl.ds(h, 32, stride=16), :]
            b = big[pl.ds(h + 1, 32, stride=16), :]
            even = jnp.where(lane < 64, a, pltpu.roll(b, 64, 1))
            odd = jnp.where(lane < 64, pltpu.roll(a, 64, 1), b)
            big[pl.ds(1024 + g * 256 + pair * 128, 32, stride=2), :] = even
            big[pl.ds(1024 + g * 256 + pair * 128 + 1, 32, stride=2), :] = odd
    for g in range(4):
        pos = jnp.concatenate([big[1024 + g * 256:1024 + g * 256 + 64, :], big[1024 + g * 256 + 128:1024 + g * 256 + 192, :]], 1)
        for w in range(4):
            keep = None
            if w == 1:
                keep = same_x
            elif w == 2:
                keep = same_y
            elif w == 3:
                keep = same_y & same_x
            val = pos if keep is None else pos + jnp.where(keep, 0.0, -100.0)
            bias[w * 4 + g] = jnp.where(k < SPAN, val, -1e30)


def kernel_a(x_hbm, flat_hbm, rel_ref,
             wqkv_o, wp_o, w1_o, w2_o, vec_o, hw_o, ob_o, qkv_o, p_o,
             x_v, flat_v, fs, os_, bias, wqkv, wp, w1, w2, vec, hw, ob, qkvb, pb, xsem, fsem, osem, wsem):
    cps = window_copies(x_hbm, x_v, xsem, True)
    for c in cps:
        c.start()
    fcp = pltpu.make_async_copy(flat_hbm, flat_v, fsem)
    fcp.start()
    fcp.wait()
    nA = BROW // 8
    def conv(t, _):
        fs[pl.ds(pl.multiple_of(t * 128, 128), 128), :] = unit_rows(flat_v, t * 16, 16)
        return 0
    lax.fori_loop(0, nA // 16, conv, 0)
    fs[(nA // 16) * 128:BROW + 8, :] = unit_rows(flat_v, (nA // 16) * 16, nA + 1 - (nA // 16) * 16)
    take_matrix(fs, R_QKV, wqkv, D, 12, False)
    vec[0:1, :] = vec_from(fs, R_G1, D, False)
    vec[1:2, :] = vec_from(fs, R_B1, D, False)
    vec[2:3, :] = vec_from(fs, R_BQ, D, False)
    vec[3:4, :] = vec_from(fs, R_BV, D, False)
    build_bias(fs[R_TAB:R_TAB + 24, :], rel_ref, os_, bias)
    for c in cps:
        c.wait()
    gain = vec[0:1, :]
    shift = vec[1:2, :]
    bq = vec[2:3, :]
    bv = vec[3:4, :]

    def rows(t, _):
        r0 = pl.multiple_of(t * BLK, BLK)
        x = x_v[pl.ds(4 * t, 4)].reshape(BLK, D).astype(F32)
        xhat, _r = norm_stats(x)
        h = (xhat * gain + shift).astype(BF16)
        hw[pl.ds(r0, BLK), :] = h
        for c in range(12):
            y = dot(h, wqkv[:, c * 128:(c + 1) * 128])
            if c < 4:
                y = (y + bq[:, c * 128:(c + 1) * 128]) * SCALE
            if c >= 8:
                y = y + bv[:, (c - 8) * 128:(c - 7) * 128]
            fs[pl.ds(c * RS + r0, BLK), :] = y
        return 0
    lax.fori_loop(0, NBLK, rows, 0)

    heads = lane_head()

    def attend(i, _):
        w = lax.shift_right_arithmetic(i, 3)
        b = i & 7
        base = w * WROWS + b
        for g in range(4):
            q = take_rows(fs, g * RS + base).astype(BF16)
            k = take_rows(fs, (4 + g) * RS + base).astype(BF16)
            v = take_rows(fs, (8 + g) * RS + base).astype(BF16)
            qkvb[i, g] = q
            qkvb[i, 4 + g] = k
            qkvb[i, 8 + g] = v
            s = dot_nt(k, block_diag(q, heads)) + bias[w * 4 + g]
            m = jnp.max(s, 0, keepdims=True)
            e = jnp.exp(s - m)
            p = (e * (1.0 / jnp.sum(e, 0, keepdims=True))).astype(BF16)
            pb[i, g] = p
            o = diag_sum(dot_tn(p, v), heads)
            put_rows(os_, g * RS + base, o)
        return 0
    lax.fori_loop(0, WB, attend, 0)

    def outs(t, _):
        r0 = pl.multiple_of(t * BLK, BLK)
        for g in range(4):
            ob[pl.ds(r0, BLK), g * 128:(g + 1) * 128] = os_[pl.ds(g * RS + r0, BLK), :].astype(BF16)
        return 0
    lax.fori_loop(0, NBLK, outs, 0)
    cos = [pltpu.make_async_copy(a, b, osem.at[n]) for n, (a, b) in enumerate([(hw, hw_o), (ob, ob_o), (qkvb, qkv_o), (pb, p_o)])]
    for c in cos:
        c.start()
    nB = flat_v.shape[0] - BROW // 8
    def conv2(t, _):
        fs[pl.ds(pl.multiple_of(t * 64, 64), 64), :] = unit_rows(flat_v, BROW // 8 + t * 8, 8)
        return 0
    lax.fori_loop(0, nB // 8, conv2, 0)
    take_matrix(fs, R_PROJ - BROW, wp, D, 4, True)
    take_matrix(fs, R_W1 - BROW, w1, D, 16, True)
    take_matrix(fs, R_W2 - BROW, w2, HID, 4, True)
    for n, r in enumerate((R_BP, R_G2, R_B2, R_C2)):
        vec[4 + n:5 + n, :] = vec_from(fs, r - BROW, D, True)
    for n in range(4):
        vec[8 + n:9 + n, :] = vec_from(fs, R_C1 - BROW + 4 * n, D, True)
    wos = [pltpu.make_async_copy(a, b, wsem.at[n]) for n, (a, b) in enumerate([(wqkv, wqkv_o), (wp, wp_o), (w1, w1_o), (w2, w2_o), (vec, vec_o)])]
    for c in wos:
        c.start()
    for c in cos + wos:
        c.wait()


def call_a(x, flat, rel):
    units = flat.shape[0]
    any_ = pl.BlockSpec(memory_space=pl.ANY)
    sds = jax.ShapeDtypeStruct
    outs = [sds((D, 3 * D), BF16), sds((D, D), BF16), sds((D, HID), BF16), sds((HID, D), BF16), sds((16, D), F32),
            sds((ROWS, D), BF16), sds((ROWS, D), BF16), sds((WB, 12, 64, 128), BF16), sds((WB, 4, 64, 256), BF16)]
    return pl.pallas_call(
        kernel_a,
        out_shape=outs,
        in_specs=[any_, any_, pl.BlockSpec(memory_space=pltpu.VMEM)],
        out_specs=[any_] * len(outs),
        scratch_shapes=[
            pltpu.VMEM((28, 7, 8, D), BF16), pltpu.VMEM((units, 8, 128), BF16), pltpu.VMEM((12 * RS, 128), F32), pltpu.VMEM((4 * RS, 128), F32),
            pltpu.VMEM((16, 64, 256), F32), pltpu.VMEM((D, 3 * D), BF16), pltpu.VMEM((D, D), BF16), pltpu.VMEM((D, HID), BF16), pltpu.VMEM((HID, D), BF16),
            pltpu.VMEM((16, D), F32), pltpu.VMEM((ROWS, D), BF16), pltpu.VMEM((ROWS, D), BF16), pltpu.VMEM((WB, 12, 64, 128), BF16), pltpu.VMEM((WB, 4, 64, 256), BF16),
            pltpu.SemaphoreType.DMA((NSEG,)), pltpu.SemaphoreType.DMA, pltpu.SemaphoreType.DMA((4,)), pltpu.SemaphoreType.DMA((5,)),
        ],
        compiler_params=pltpu.CompilerParams(vmem_limit_bytes=64000000),
        name="attend",
    )(x, flat, rel)


def rel_lanes(rel_index):
    t = jnp.full((64, 64), -1, jnp.int32).at[:SPAN, :SPAN].set(rel_index.T)
    return t.reshape(1, 4096)


CH = 512
INV_SQRT2 = 0.7071067811865476
INV_SQRT2PI = 0.3989422804014327


def gelu_parts(u):
    e = jnp.exp(u * u * -0.5)
    t = 1.0 / (1.0 + jnp.abs(u) * (0.3275911 * INV_SQRT2))
    half = t * (0.127414796 + t * (-0.142248368 + t * (0.7107068705 + t * (-0.7265760135 + t * 0.5307027145)))) * e
    cdf = jnp.where(u >= 0, 1.0 - half, half)
    return cdf, e * INV_SQRT2PI


def put_matrix(fs, row, get, nrows, ncb, step=128):
    lane = lax.broadcasted_iota(jnp.int32, (step, 128), 1)


def acc_rows(ref, i, v):
    ref[8 * i:8 * i + 8, 0:v.shape[1]] += jnp.sum(v.reshape(v.shape[0] // 8, 8, v.shape[1]), 0)


def kernel_b(x_hbm, cot_hbm, ob_hbm, wp, w1, w2, vec, counts,
             y_hbm, dx1_o, dwp_o, dw1_o, dw2_o, vg_o,
             x_v, dy_v, ob, yv, a, du, h2, dx1, e, acc, xsem, csem, ysem, osem):
    cps = window_copies(x_hbm, x_v, xsem, True) + window_copies(cot_hbm, dy_v, csem, True)
    cps.append(pltpu.make_async_copy(ob_hbm, ob, osem.at[0]))
    for c in cps:
        c.start()
    acc[...] = jnp.zeros_like(acc)
    for c in cps:
        c.wait()
    bp, g2, b2, c2 = (vec[n:n + 1, :] for n in range(4, 8))
    count = counts[0]

    def rows(t, _):
        r0 = pl.multiple_of(t * BLK, BLK)
        x = x_v[pl.ds(4 * t, 4)].reshape(BLK, D).astype(F32)
        alive = lax.broadcasted_iota(jnp.int32, (4, 7, 8, D), 2) < count
        dy = jnp.where(alive, dy_v[pl.ds(4 * t, 4)].astype(F32), 0.0)
        dyb = dy.astype(BF16)
        dy_v[pl.ds(4 * t, 4)] = dyb
        dy = dy.reshape(BLK, D)
        dyb = dyb.reshape(BLK, D)
        x1 = x + dot(ob[pl.ds(r0, BLK), :], wp[...]) + bp
        xhat, r = norm_stats(x1)
        h = (xhat * g2 + b2).astype(BF16)
        h2[pl.ds(r0, BLK), :] = h
        y = x1 + c2
        dh = jnp.zeros((BLK, D), F32)
        for j in range(HID // CH):
            cs = slice(j * CH, (j + 1) * CH)
            u = dot(h, w1[:, cs]) + vec[8 + j:9 + j, :]
            cdf, pdf = gelu_parts(u)
            av = (u * cdf).astype(BF16)
            a[pl.ds(r0, BLK), cs] = av
            y = y + dot(av, w2[cs, :])
            da = dot_nt(dyb, w2[cs, :])
            duv = da * (cdf + u * pdf)
            acc_rows(acc, 4 + j, duv)
            dub = duv.astype(BF16)
            du[pl.ds(r0, BLK), cs] = dub
            dh = dh + dot_nt(dub, w1[:, cs])
        yv[pl.ds(4 * t, 4)] = y.reshape(4, 7, 8, D).astype(BF16)
        acc_rows(acc, 0, dy)
        acc_rows(acc, 1, dh * xhat)
        acc_rows(acc, 2, dh)
        dg = dh * g2
        dt = r * (dg - jnp.mean(dg, -1, keepdims=True) - xhat * jnp.mean(dg * xhat, -1, keepdims=True))
        dxv = dy + dt
        acc_rows(acc, 3, dxv)
        dx1[pl.ds(r0, BLK), :] = dxv
        e[pl.ds(r0, BLK), :] = dxv.astype(BF16)
        return 0
    lax.fori_loop(0, NBLK, rows, 0)
    ycs = window_copies(y_hbm, yv, ysem, False)
    for c in ycs:
        c.start()
    dcp = pltpu.make_async_copy(dx1, dx1_o, osem.at[1])
    dcp.start()
    vg_o[...] = jnp.sum(acc[...].reshape(8, 8, D), 1)
    dyf = dy_v[...].reshape(ROWS, D)

    def w2rows(t, _):
        r0 = pl.multiple_of(t * 256, 256)
        dw2_o[pl.ds(r0, 256), :] = dot_tn(a[:, pl.ds(r0, 256)], dyf)
        return 0
    lax.fori_loop(0, HID // 256, w2rows, 0)

    def w1rows(t, _):
        r0 = pl.multiple_of(t * 256, 256)
        dw1_o[:, pl.ds(r0, 256)] = dot_tn(h2[...], du[:, pl.ds(r0, 256)])
        return 0
    lax.fori_loop(0, HID // 256, w1rows, 0)
    dwp_o[...] = dot_tn(ob[...], e[...])
    dcp.wait()
    for c in ycs:
        c.wait()


def call_b(x, cot, ob, wp, w1, w2, vec, counts):
    any_ = pl.BlockSpec(memory_space=pl.ANY)
    vm = pl.BlockSpec(memory_space=pltpu.VMEM)
    sds = jax.ShapeDtypeStruct
    outs = [sds((14, 14, 8, D), BF16), sds((ROWS, D), F32), sds((D, D), F32), sds((D, HID), F32), sds((HID, D), F32), sds((8, D), F32)]
    big = pltpu.VMEM((28, 7, 8, D), BF16)
    return pl.pallas_call(
        kernel_b,
        out_shape=outs,
        in_specs=[any_, any_, any_, vm, vm, vm, vm, pl.BlockSpec(memory_space=pltpu.SMEM)],
        out_specs=[any_, any_, vm, vm, vm, vm],
        scratch_shapes=[
            big, big, pltpu.VMEM((ROWS, D), BF16), big, pltpu.VMEM((ROWS, HID), BF16), pltpu.VMEM((ROWS, HID), BF16), pltpu.VMEM((ROWS, D), BF16),
            pltpu.VMEM((ROWS, D), F32), pltpu.VMEM((ROWS, D), BF16), pltpu.VMEM((64, D), F32),
            pltpu.SemaphoreType.DMA((NSEG,)), pltpu.SemaphoreType.DMA((NSEG,)), pltpu.SemaphoreType.DMA((NSEG,)), pltpu.SemaphoreType.DMA((2,)),
        ],
        compiler_params=pltpu.CompilerParams(vmem_limit_bytes=64000000),
        name="mlp",
    )(x, cot, ob, wp, w1, w2, vec, counts)


def kernel_c(x_hbm, dx1_hbm, hw_hbm, qkv_hbm, p_hbm, wqkv, wp, vec,
             dx_hbm, dwq_o, vg_o, dtab_o,
             x_v, dx1, hw, qkvb, pb, fs, os_, dq, dxv, dtab, acc, xsem, isem, psem, ysem):
    cps = window_copies(x_hbm, x_v, xsem, True)
    ins = [pltpu.make_async_copy(a, b, isem.at[n]) for n, (a, b) in enumerate([(dx1_hbm, dx1), (hw_hbm, hw), (qkv_hbm, qkvb), (p_hbm, pb)])]
    ins[0].start()
    ins[2].start()
    ins[3].start()
    ins[1].start()
    for c in cps:
        c.start()
    acc[...] = jnp.zeros_like(acc)
    dtab[...] = jnp.zeros_like(dtab)
    ins[0].wait()

    def rows0(t, _):
        r0 = pl.multiple_of(t * BLK, BLK)
        ev = dx1[pl.ds(r0, BLK), :].astype(BF16)
        for g in range(4):
            os_[pl.ds(g * RS + r0, BLK), :] = dot_nt(ev, wp[g * 128:(g + 1) * 128, :])
        return 0
    lax.fori_loop(0, NBLK, rows0, 0)
    ins[2].wait()
    ins[3].wait()
    heads = lane_head()

    def attend(i, _):
        w = lax.shift_right_arithmetic(i, 3)
        b = i & 7
        base = w * WROWS + b
        for g in range(4):
            do = take_rows(os_, g * RS + base).astype(BF16)
            q = qkvb[i, g]
            k = qkvb[i, 4 + g]
            v = qkvb[i, 8 + g]
            pbv = pb[i, g]
            p = pbv.astype(F32)
            dobd = block_diag(do, heads)
            dp = dot_nt(v, dobd)
            t = p * dp
            ds = t - p * jnp.sum(t, 0, keepdims=True)
            dtab[g] += ds
            dsb = ds.astype(BF16)
            put_rows(fs, (8 + g) * RS + base, dot(pbv, dobd))
            put_rows(fs, (4 + g) * RS + base, dot(dsb, block_diag(q, heads)))
            put_rows(fs, g * RS + base, diag_sum(dot_tn(dsb, k), heads) * SCALE)
        return 0
    lax.fori_loop(0, WB, attend, 0)
    for c in cps:
        c.wait()
    gain = vec[0:1, :]

    def rows1(t, _):
        r0 = pl.multiple_of(t * BLK, BLK)
        dn = jnp.zeros((BLK, D), F32)
        for c in range(12):
            v = fs[pl.ds(c * RS + r0, BLK), :]
            if c < 4 or c >= 8:
                i = 2 if c < 4 else 3
                acc[8 * i:8 * i + 8, (c % 4) * 128:(c % 4) * 128 + 128] += jnp.sum(v.reshape(BLK // 8, 8, 128), 0)
            dq[pl.ds(r0, BLK), c * 128:(c + 1) * 128] = v.astype(BF16)
        dn = dot_nt(dq[pl.ds(r0, BLK), :], wqkv[...])
        x = x_v[pl.ds(4 * t, 4)].reshape(BLK, D).astype(F32)
        xhat, r = norm_stats(x)
        acc_rows(acc, 0, dn * xhat)
        acc_rows(acc, 1, dn)
        dg = dn * gain
        dt = r * (dg - jnp.mean(dg, -1, keepdims=True) - xhat * jnp.mean(dg * xhat, -1, keepdims=True))
        dxv[pl.ds(4 * t, 4)] = (dx1[pl.ds(r0, BLK), :] + dt).reshape(4, 7, 8, D)
        return 0
    lax.fori_loop(0, NBLK, rows1, 0)
    ycs = window_copies(dx_hbm, dxv, ysem, False)
    for c in ycs:
        c.start()
    vg_o[...] = jnp.sum(acc[...].reshape(8, 8, D), 1)
    ins[1].wait()

    def wq(t, _):
        c0 = pl.multiple_of(t * 256, 256)
        dwq_o[:, pl.ds(c0, 256)] = dot_tn(hw[...], dq[:, pl.ds(c0, 256)])
        return 0
    lax.fori_loop(0, 6, wq, 0)
    dtab_o[...] = dtab[...]
    for c in ycs:
        c.wait()


def call_c(x, dx1, hw, qkv, p, wqkv, wp, vec):
    any_ = pl.BlockSpec(memory_space=pl.ANY)
    vm = pl.BlockSpec(memory_space=pltpu.VMEM)
    sds = jax.ShapeDtypeStruct
    outs = [sds((14, 14, 8, D), F32), sds((D, 3 * D), F32), sds((8, D), F32), sds((4, 64, 256), F32)]
    return pl.pallas_call(
        kernel_c,
        out_shape=outs,
        in_specs=[any_] * 5 + [vm] * 3,
        out_specs=[any_, vm, vm, vm],
        scratch_shapes=[
            pltpu.VMEM((28, 7, 8, D), BF16), pltpu.VMEM((ROWS, D), F32), pltpu.VMEM((ROWS, D), BF16), pltpu.VMEM((WB, 12, 64, 128), BF16), pltpu.VMEM((WB, 4, 64, 256), BF16),
            pltpu.VMEM((12 * RS, 128), F32), pltpu.VMEM((4 * RS, 128), F32), pltpu.VMEM((ROWS, 3 * D), BF16), pltpu.VMEM((28, 7, 8, D), F32),
            pltpu.VMEM((4, 64, 256), F32), pltpu.VMEM((64, D), F32),
            pltpu.SemaphoreType.DMA((NSEG,)), pltpu.SemaphoreType.DMA((4,)), pltpu.SemaphoreType.DMA, pltpu.SemaphoreType.DMA((NSEG,)),
        ],
        compiler_params=pltpu.CompilerParams(vmem_limit_bytes=64000000),
        name="attend_back",
    )(x, dx1, hw, qkv, p, wqkv, wp, vec)


from jax.sharding import PartitionSpec as P

STEP = 2
HIGH = lax.Precision.HIGHEST
DECAY = [0.0, 0.0, 0.05, 0.0, 0.0, 0.0, 0.05, 0.0, 0.0, 0.0, 0.05, 0.0, 0.05, 0.0, 0.0]


def group_starts():
    lengths = [D, D, 3 * D * D, D, D, TAB * HEADS, D * D, D, D, D, D * HID, HID, HID * D, D]
    starts = [0]
    for length in lengths:
        starts.append(starts[-1] + length)
    return starts


def adam_update(weights, first, second, grad, rates, start):
    index = start + lax.iota(jnp.int32, weights.shape[0])
    starts = group_starts()
    rate = jnp.zeros_like(weights) + rates[0]
    decay = jnp.zeros_like(weights)
    for group in range(1, len(starts)):
        after = index >= starts[group]
        rate = jnp.where(after, rates[group], rate)
        decay = jnp.where(after, DECAY[group], decay)
    first_new = 0.9 * first + 0.1 * grad
    second_new = 0.999 * second + 0.001 * grad * grad
    first_hat = first_new / (1.0 - 0.9**STEP)
    second_hat = second_new / (1.0 - 0.999**STEP)
    weights_new = weights - rate * (first_hat / (jnp.sqrt(second_hat) + 1e-08) + decay * weights)
    return (weights_new, first_new, second_new)


def local(images, cotangent, counts, rel_index, params, moment1, moment2, rates):
    shard_len = params.shape[0]
    total_len = shard_len * lax.axis_size("opt")
    working = lax.all_gather(params.astype(BF16), "opt", axis=0, tiled=True)
    starts = group_starts()
    xt = images.transpose(1, 2, 0, 3)
    ct = cotangent.transpose(1, 2, 0, 3)
    flat = working.reshape(-1, 8, 128)
    wqkv, wp, w1, w2, vec, hw, ob, qkv, p = call_a(xt, flat, rel_lanes(rel_index))
    y, dx1, dwp, dw1, dw2, vgb = call_b(xt, ct, ob, wp, w1, w2, vec, counts)
    dx, dwq, vga, dtab = call_c(xt, dx1, hw, qkv, p, wqkv, wp, vec)
    score = dtab.reshape(4, 64, 4, 64)[:, :SPAN, :, :SPAN].transpose(0, 2, 3, 1).reshape(HEADS, SPAN * SPAN)
    onehot = rel_index.reshape(-1)[:, None] == lax.iota(jnp.int32, TAB)[None, :]
    grad_table = jnp.dot(score, onehot.astype(F32), precision=HIGH).T.reshape(-1)
    local_grad = jnp.concatenate([
        vga[0], vga[1], dwq.reshape(-1), vga[2], vga[3], grad_table, dwp.reshape(-1), vgb[3], vgb[1], vgb[2],
        dw1.reshape(-1), vgb[4:8].reshape(-1), dw2.reshape(-1), vgb[0], jnp.zeros((total_len - starts[-1],), F32)])
    summed = lax.psum(local_grad.astype(BF16), "dp")
    grad_shard = lax.psum_scatter(summed, "opt", scatter_dimension=0, tiled=True).astype(F32)
    start = lax.axis_index("opt") * shard_len
    new_params, new_first, new_second = adam_update(params, moment1, moment2, grad_shard, rates, start)
    return (y.transpose(2, 0, 1, 3), dx.transpose(2, 0, 1, 3), grad_shard, new_params, new_first, new_second)


def solution(mesh):
    split = P(("dp", "opt"), None, None, None)
    return jax.shard_map(
        local, mesh=mesh,
        in_specs=(split, split, P(("dp", "opt")), P(), P("opt"), P("opt"), P("opt"), P()),
        out_specs=(split, split, P("opt"), P("opt"), P("opt"), P("opt")),
        check_vma=False)
```

```python
import functools
import jax
import jax.numpy as jnp
from jax import lax
from jax.experimental import pallas as pl
from jax.experimental.pallas import tpu as pltpu

D = 512
HEADS = 16
HEAD_DIM = 32
HID = 2048
SIDE = 14
WIN = 7
SHIFT = 3
TAB = 169
F32 = jnp.float32
BF16 = jnp.bfloat16

IMGS = 8
SPAN = WIN * WIN
WROWS = SPAN * IMGS
ROWS = 4 * WROWS
RS = ROWS + 64
BLK = 224
NBLK = ROWS // BLK
WB = 4 * IMGS
SCALE = HEAD_DIM ** -0.5

R_G1, R_B1, R_QKV, R_BQ, R_BV, R_TAB = 0, 4, 8, 6152, 6156, 6160
R_PROJ, R_BP, R_G2, R_B2, R_W1, R_C1, R_W2, R_C2, R_END = 6181, 8229, 8233, 8237, 8241, 16433, 16449, 24641, 24645
LANE = 16
BROW = 6176


def segments(w):
    if w == 0:
        return [(SHIFT, WIN, 0)]
    return [(WIN + SHIFT, WIN - SHIFT, 0), (0, SHIFT, WIN - SHIFT)]


def window_copies(hbm, vmem, sem, inward):
    out = []
    n = 0
    for wy in range(2):
        for wx in range(2):
            for ys, yl, yo in segments(wy):
                for xs, xl, xo in segments(wx):
                    a = hbm.at[pl.ds(ys, yl), pl.ds(xs, xl)]
                    b = vmem.at[pl.ds((2 * wy + wx) * WIN + yo, yl), pl.ds(xo, xl)]
                    out.append(pltpu.make_async_copy(a, b, sem.at[n]) if inward else pltpu.make_async_copy(b, a, sem.at[n]))
                    n += 1
    return out


NSEG = 9


def dot(a, b):
    return lax.dot_general(a, b, (((1,), (0,)), ((), ())), preferred_element_type=F32)


def dot_nt(a, b):
    return lax.dot_general(a, b, (((1,), (1,)), ((), ())), preferred_element_type=F32)


def dot_tn(a, b):
    return lax.dot_general(a, b, (((0,), (0,)), ((), ())), preferred_element_type=F32)


def norm_stats(x):
    mean = jnp.mean(x, -1, keepdims=True)
    dev = x - mean
    var = jnp.mean(dev * dev, -1, keepdims=True)
    r = lax.rsqrt(var + 1e-05)
    return dev * r, r


def pieces_to_rows(pn, wb, fs, shard, count, base):
    def body(p, _):
        row = pl.multiple_of((shard * pn.units - base + p * pn.pc) * 8, 8)
        fs[pl.ds(row, pn.pc * 8), :] = wb[shard, p & 1, lax.shift_right_arithmetic(p, 1)].astype(F32).reshape(pn.pc * 8, 128)
        return 0
    lax.fori_loop(0, count, body, 0)


def vec_from(fs, row, width, shift):
    parts = []
    lane = lax.broadcasted_iota(jnp.int32, (1, 128), 1)
    for c in range(width // 128):
        a = fs[pl.ds(row + c, 1), :]
        if shift:
            b = fs[pl.ds(row + c + 1, 1), :]
            a = jnp.where(lane < 128 - LANE, pltpu.roll(a, 128 - LANE, 1), pltpu.roll(b, 128 - LANE, 1))
        parts.append(a)
    return jnp.concatenate(parts, 1)


def take_matrix(fs, row, dst, nrows, ncb, shift, step=128):
    lane = lax.broadcasted_iota(jnp.int32, (step, 128), 1)

    def body(t, _):
        base = row + t * (step * ncb)
        r0 = pl.multiple_of(t * step, step)
        for c in range(ncb):
            a = fs[pl.ds(base + c, step, stride=ncb), :]
            if shift:
                b = fs[pl.ds(base + c + 1, step, stride=ncb), :]
                a = jnp.where(lane < 128 - LANE, pltpu.roll(a, 128 - LANE, 1), pltpu.roll(b, 128 - LANE, 1))
            dst[pl.ds(r0, step), c * 128:(c + 1) * 128] = a.astype(BF16)
        return 0

    lax.fori_loop(0, nrows // step, body, 0)


def lane_head():
    return lax.broadcasted_iota(jnp.int32, (64, 128), 1) // HEAD_DIM


def block_diag(v, heads):
    zero = jnp.zeros_like(v)
    return jnp.concatenate([jnp.where(heads == h, v, zero) for h in range(4)], 0)


def diag_sum(r, heads):
    out = r[0:64]
    for h in range(1, 4):
        out = jnp.where(heads == h, r[64 * h:64 * h + 64], out)
    return out


def take_rows(fs, start):
    v = fs[pl.ds(start, 56, stride=IMGS), :]
    v = jnp.where(lax.broadcasted_iota(jnp.int32, (56, 128), 0) < SPAN, v, 0.0)
    return jnp.concatenate([v, jnp.zeros((8, 128), F32)], 0)


def put_rows(fs, start, v):
    fs[pl.ds(start, 48, stride=IMGS), :] = v[0:48]
    fs[pl.ds(start + 48 * IMGS, 1), :] = v[48:49]


def build_bias(tab3, rel_ref, big, bias):
    rel = rel_ref[...]
    row = lax.shift_right_arithmetic(rel, 3)
    low = rel & 7
    oh = (lax.broadcasted_iota(jnp.int32, (32, 4096), 0) == row).astype(F32).astype(BF16)
    tab = jnp.concatenate([tab3, jnp.zeros((8, 128), F32)], 0).astype(BF16)
    r = dot_tn(tab, oh)
    acc = jnp.zeros((16, 4096), F32)
    for j in range(8):
        acc = acc + jnp.where(low == j, r[16 * j:16 * j + 16], 0.0)
    for kk in range(32):
        big[kk * 16:kk * 16 + 16, :] = acc[:, kk * 128:kk * 128 + 128]
    k = lax.broadcasted_iota(jnp.int32, (64, 256), 0)
    q = lax.broadcasted_iota(jnp.int32, (64, 256), 1) & 63
    ki = lax.shift_right_arithmetic(k * 37, 8)
    kj = k - ki * 7
    qi = lax.shift_right_arithmetic(q * 37, 8)
    qj = q - qi * 7
    cut = WIN - SHIFT
    same_y = (ki < cut) == (qi < cut)
    same_x = (kj < cut) == (qj < cut)
    lane = lax.broadcasted_iota(jnp.int32, (32, 128), 1)
    for g in range(4):
        for pair in range(2):
            h = 4 * g + 2 * pair
            a = big[pl.ds(h, 32, stride=16), :]
            b = big[pl.ds(h + 1, 32, stride=16), :]
            even = jnp.where(lane < 64, a, pltpu.roll(b, 64, 1))
            odd = jnp.where(lane < 64, pltpu.roll(a, 64, 1), b)
            big[pl.ds(1024 + g * 256 + pair * 128, 32, stride=2), :] = even
            big[pl.ds(1024 + g * 256 + pair * 128 + 1, 32, stride=2), :] = odd
    for g in range(4):
        pos = jnp.concatenate([big[1024 + g * 256:1024 + g * 256 + 64, :], big[1024 + g * 256 + 128:1024 + g * 256 + 192, :]], 1)
        for w in range(4):
            keep = None
            if w == 1:
                keep = same_x
            elif w == 2:
                keep = same_y
            elif w == 3:
                keep = same_y & same_x
            val = pos if keep is None else pos + jnp.where(keep, 0.0, -100.0)
            bias[w * 4 + g] = jnp.where(k < SPAN, val, -1e30)


def kernel_a(pn, x_hbm, flat_hbm, rel_ref,
             wqkv_o, wp_o, w1_o, w2_o, vec_o, hw_o, ob_o, qkv_o, p_o,
             x_v, flat_v, fs, os_, bias, wqkv, wp, w1, w2, vec, hw, ob, qkvb, pb, xsem, fsem, osem, wsem):
    cps = window_copies(x_hbm, x_v, xsem, True)
    for c in cps:
        c.start()
    fcp = pltpu.make_async_copy(flat_hbm, flat_v, fsem)
    fcp.start()
    fcp.wait()
    for k in range(pn.ka):
        pieces_to_rows(pn, flat_v, fs, k, pn.ndp, 0)
    pieces_to_rows(pn, flat_v, fs, pn.ka, 1, 0)
    take_matrix(fs, R_QKV, wqkv, D, 12, False)
    vec[0:1, :] = vec_from(fs, R_G1, D, False)
    vec[1:2, :] = vec_from(fs, R_B1, D, False)
    vec[2:3, :] = vec_from(fs, R_BQ, D, False)
    vec[3:4, :] = vec_from(fs, R_BV, D, False)
    build_bias(fs[R_TAB:R_TAB + 24, :], rel_ref, os_, bias)
    for c in cps:
        c.wait()
    gain = vec[0:1, :]
    shift = vec[1:2, :]
    bq = vec[2:3, :]
    bv = vec[3:4, :]

    def rows(t, _):
        r0 = pl.multiple_of(t * BLK, BLK)
        x = x_v[pl.ds(4 * t, 4)].reshape(BLK, D).astype(F32)
        xhat, _r = norm_stats(x)
        h = (xhat * gain + shift).astype(BF16)
        hw[pl.ds(r0, BLK), :] = h
        for c in range(12):
            y = dot(h, wqkv[:, c * 128:(c + 1) * 128])
            if c < 4:
                y = (y + bq[:, c * 128:(c + 1) * 128]) * SCALE
            if c >= 8:
                y = y + bv[:, (c - 8) * 128:(c - 7) * 128]
            fs[pl.ds(c * RS + r0, BLK), :] = y
        return 0
    lax.fori_loop(0, NBLK, rows, 0)

    heads = lane_head()

    def attend(i, _):
        w = lax.shift_right_arithmetic(i, 3)
        b = i & 7
        base = w * WROWS + b
        for g in range(4):
            q = take_rows(fs, g * RS + base).astype(BF16)
            k = take_rows(fs, (4 + g) * RS + base).astype(BF16)
            v = take_rows(fs, (8 + g) * RS + base).astype(BF16)
            qkvb[i, g] = q
            qkvb[i, 4 + g] = k
            qkvb[i, 8 + g] = v
            s = dot_nt(k, block_diag(q, heads)) + bias[w * 4 + g]
            m = jnp.max(s, 0, keepdims=True)
            e = jnp.exp(s - m)
            p = (e * (1.0 / jnp.sum(e, 0, keepdims=True))).astype(BF16)
            pb[i, g] = p
            o = diag_sum(dot_tn(p, v), heads)
            put_rows(os_, g * RS + base, o)
        return 0
    lax.fori_loop(0, WB, attend, 0)

    def outs(t, _):
        r0 = pl.multiple_of(t * BLK, BLK)
        for g in range(4):
            ob[pl.ds(r0, BLK), g * 128:(g + 1) * 128] = os_[pl.ds(g * RS + r0, BLK), :].astype(BF16)
        return 0
    lax.fori_loop(0, NBLK, outs, 0)
    cos = [pltpu.make_async_copy(a, b, osem.at[n]) for n, (a, b) in enumerate([(hw, hw_o), (ob, ob_o), (qkvb, qkv_o), (pb, p_o)])]
    for c in cos:
        c.start()
    for k in range(pn.ka, pn.ns):
        pieces_to_rows(pn, flat_v, fs, k, pn.ndp, pn.base)
    first = pn.base * 8
    take_matrix(fs, R_PROJ - first, wp, D, 4, True)
    take_matrix(fs, R_W1 - first, w1, D, 16, True)
    take_matrix(fs, R_W2 - first, w2, HID, 4, True)
    for n, r in enumerate((R_BP, R_G2, R_B2, R_C2)):
        vec[4 + n:5 + n, :] = vec_from(fs, r - first, D, True)
    for n in range(4):
        vec[8 + n:9 + n, :] = vec_from(fs, R_C1 - first + 4 * n, D, True)
    wos = [pltpu.make_async_copy(a, b, wsem.at[n]) for n, (a, b) in enumerate([(wqkv, wqkv_o), (wp, wp_o), (w1, w1_o), (w2, w2_o), (vec, vec_o)])]
    for c in wos:
        c.start()
    for c in cos + wos:
        c.wait()


def call_a(pn, x, flat, rel):
    any_ = pl.BlockSpec(memory_space=pl.ANY)
    sds = jax.ShapeDtypeStruct
    outs = [sds((D, 3 * D), BF16), sds((D, D), BF16), sds((D, HID), BF16), sds((HID, D), BF16), sds((16, D), F32),
            sds((ROWS, D), BF16), sds((ROWS, D), BF16), sds((WB, 12, 64, 128), BF16), sds((WB, 4, 64, 256), BF16)]
    return pl.pallas_call(
        functools.partial(kernel_a, pn),
        out_shape=outs,
        in_specs=[any_, any_, pl.BlockSpec(memory_space=pltpu.VMEM)],
        out_specs=[any_] * len(outs),
        scratch_shapes=[
            pltpu.VMEM((28, 7, 8, D), BF16), pltpu.VMEM(flat.shape, BF16), pltpu.VMEM((12 * RS, 128), F32), pltpu.VMEM((4 * RS, 128), F32),
            pltpu.VMEM((16, 64, 256), F32), pltpu.VMEM((D, 3 * D), BF16), pltpu.VMEM((D, D), BF16), pltpu.VMEM((D, HID), BF16), pltpu.VMEM((HID, D), BF16),
            pltpu.VMEM((16, D), F32), pltpu.VMEM((ROWS, D), BF16), pltpu.VMEM((ROWS, D), BF16), pltpu.VMEM((WB, 12, 64, 128), BF16), pltpu.VMEM((WB, 4, 64, 256), BF16),
            pltpu.SemaphoreType.DMA((NSEG,)), pltpu.SemaphoreType.DMA, pltpu.SemaphoreType.DMA((4,)), pltpu.SemaphoreType.DMA((5,)),
        ],
        compiler_params=pltpu.CompilerParams(vmem_limit_bytes=64000000),
        name="attend",
    )(x, flat, rel)


def rel_lanes(rel_index):
    t = jnp.full((64, 64), -1, jnp.int32).at[:SPAN, :SPAN].set(rel_index.T)
    return t.reshape(1, 4096)


CH = 512
INV_SQRT2 = 0.7071067811865476
INV_SQRT2PI = 0.3989422804014327


def gelu_parts(u):
    e = jnp.exp(u * u * -0.5)
    t = 1.0 / (1.0 + jnp.abs(u) * (0.3275911 * INV_SQRT2))
    half = t * (0.127414796 + t * (-0.142248368 + t * (0.7107068705 + t * (-0.7265760135 + t * 0.5307027145)))) * e
    cdf = jnp.where(u >= 0, 1.0 - half, half)
    return cdf, e * INV_SQRT2PI


def put_block(fs, start, stride, v):
    n = v.shape[0]
    lane = lax.broadcasted_iota(jnp.int32, (n, 128), 1)
    v = pltpu.roll(v, LANE, 1)
    here = pl.ds(start, n, stride=stride) if n > 1 else pl.ds(start, 1)
    fs[here, :] = jnp.where(lane >= LANE, v, fs[here, :])
    here = pl.ds(start + 1, n, stride=stride) if n > 1 else pl.ds(start + 1, 1)
    fs[here, :] = jnp.where(lane < LANE, v, fs[here, :])


def put_vec(fs, row, v):
    for c in range(v.shape[1] // 128):
        put_block(fs, row + c, 1, v[:, c * 128:(c + 1) * 128])


def acc_rows(ref, i, v):
    ref[8 * i:8 * i + 8, 0:v.shape[1]] += jnp.sum(v.reshape(v.shape[0] // 8, 8, v.shape[1]), 0)


def kernel_b(pn, x_hbm, cot_hbm, ob_hbm, wp, w1, w2, vec, counts,
             y_hbm, dx1_o, gb_o,
             x_v, dy_v, ob, yv, a, du, h2, dx1, e, acc, fs, gflat, xsem, csem, ysem, osem, gsem):
    cps = window_copies(x_hbm, x_v, xsem, True) + window_copies(cot_hbm, dy_v, csem, True)
    cps.append(pltpu.make_async_copy(ob_hbm, ob, osem.at[0]))
    for c in cps:
        c.start()
    acc[...] = jnp.zeros_like(acc)
    for c in cps:
        c.wait()
    bp, g2, b2, c2 = (vec[n:n + 1, :] for n in range(4, 8))
    count = counts[0]

    def rows(t, _):
        r0 = pl.multiple_of(t * BLK, BLK)
        x = x_v[pl.ds(4 * t, 4)].reshape(BLK, D).astype(F32)
        alive = lax.broadcasted_iota(jnp.int32, (4, 7, 8, D), 2) < count
        dy = jnp.where(alive, dy_v[pl.ds(4 * t, 4)].astype(F32), 0.0)
        dyb = dy.astype(BF16)
        dy_v[pl.ds(4 * t, 4)] = dyb
        dy = dy.reshape(BLK, D)
        dyb = dyb.reshape(BLK, D)
        x1 = x + dot(ob[pl.ds(r0, BLK), :], wp[...]) + bp
        xhat, r = norm_stats(x1)
        h = (xhat * g2 + b2).astype(BF16)
        h2[pl.ds(r0, BLK), :] = h
        y = x1 + c2
        dh = jnp.zeros((BLK, D), F32)
        for j in range(HID // CH):
            cs = slice(j * CH, (j + 1) * CH)
            u = dot(h, w1[:, cs]) + vec[8 + j:9 + j, :]
            cdf, pdf = gelu_parts(u)
            av = (u * cdf).astype(BF16)
            a[pl.ds(r0, BLK), cs] = av
            y = y + dot(av, w2[cs, :])
            da = dot_nt(dyb, w2[cs, :])
            duv = da * (cdf + u * pdf)
            acc_rows(acc, 4 + j, duv)
            dub = duv.astype(BF16)
            du[pl.ds(r0, BLK), cs] = dub
            dh = dh + dot_nt(dub, w1[:, cs])
        yv[pl.ds(4 * t, 4)] = y.reshape(4, 7, 8, D).astype(BF16)
        acc_rows(acc, 0, dy)
        acc_rows(acc, 1, dh * xhat)
        acc_rows(acc, 2, dh)
        dg = dh * g2
        dt = r * (dg - jnp.mean(dg, -1, keepdims=True) - xhat * jnp.mean(dg * xhat, -1, keepdims=True))
        dxv = dy + dt
        acc_rows(acc, 3, dxv)
        dx1[pl.ds(r0, BLK), :] = dxv
        e[pl.ds(r0, BLK), :] = dxv.astype(BF16)
        return 0
    lax.fori_loop(0, NBLK, rows, 0)
    ycs = window_copies(y_hbm, yv, ysem, False)
    for c in ycs:
        c.start()
    dcp = pltpu.make_async_copy(dx1, dx1_o, osem.at[1])
    dcp.start()
    vg = jnp.sum(acc[...].reshape(8, 8, D), 1)
    dyf = dy_v[...].reshape(ROWS, D)
    first = pn.base * 8
    nrow = pn.bunits * 8
    lo = (R_PROJ // 8 + 1) * 8 - first
    hi = R_END // 8 * 8 - first
    fs[0:lo, :] = jnp.zeros((lo, 128), F32)
    fs[hi:nrow, :] = jnp.zeros((nrow - hi, 128), F32)

    def w2rows(t, _):
        r0 = pl.multiple_of(t * 256, 256)
        v = dot_tn(a[:, pl.ds(r0, 256)], dyf)
        for c in range(4):
            put_block(fs, R_W2 - first + r0 * 4 + c, 4, v[:, c * 128:(c + 1) * 128])
        return 0
    lax.fori_loop(0, HID // 256, w2rows, 0)

    def w1rows(t, _):
        r0 = pl.multiple_of(t * 256, 256)
        v = dot_tn(h2[...], du[:, pl.ds(r0, 256)])
        for c in range(2):
            put_block(fs, R_W1 - first + 2 * t + c, 16, v[:, c * 128:(c + 1) * 128])
        return 0
    lax.fori_loop(0, HID // 256, w1rows, 0)
    v = dot_tn(ob[...], e[...])
    for c in range(4):
        put_block(fs, R_PROJ - first + c, 4, v[:, c * 128:(c + 1) * 128])
    for row, n in ((R_BP, 3), (R_G2, 1), (R_B2, 2), (R_C2, 0)):
        put_vec(fs, row - first, vg[n:n + 1])
    for j in range(4):
        put_vec(fs, R_C1 - first + 4 * j, vg[4 + j:5 + j])

    def low(t, _):
        gflat[pl.ds(t * 32, 32)] = fs[pl.ds(pl.multiple_of(t * 256, 256), 256), :].reshape(32, 8, 128).astype(BF16)
        return 0
    lax.fori_loop(0, pn.bunits // 32, low, 0)
    n = pn.bunits % 32
    if n:
        gflat[pn.bunits - n:pn.bunits] = fs[nrow - 8 * n:nrow, :].reshape(n, 8, 128).astype(BF16)
    gcs = []
    for k in range(pn.nk):
        for p in range(pn.ndp):
            gcs.append(pltpu.make_async_copy(gflat.at[pl.ds(k * pn.units + p * pn.pc, pn.pc)], gb_o.at[p & 1, p >> 1, pl.ds(k * pn.pc, pn.pc)], gsem.at[k * pn.ndp + p]))
    for cp in gcs:
        cp.start()
    for cp in gcs:
        cp.wait()
    dcp.wait()
    for cp in ycs:
        cp.wait()


def call_b(pn, x, cot, ob, wp, w1, w2, vec, counts):
    any_ = pl.BlockSpec(memory_space=pl.ANY)
    vm = pl.BlockSpec(memory_space=pltpu.VMEM)
    sds = jax.ShapeDtypeStruct
    outs = [sds((14, 14, 8, D), BF16), sds((ROWS, D), F32), sds((2, pn.rest, pn.nk * pn.pc, 8, 128), BF16)]
    big = pltpu.VMEM((28, 7, 8, D), BF16)
    return pl.pallas_call(
        functools.partial(kernel_b, pn),
        out_shape=outs,
        in_specs=[any_, any_, any_, vm, vm, vm, vm, pl.BlockSpec(memory_space=pltpu.SMEM)],
        out_specs=[any_] * 3,
        scratch_shapes=[
            big, big, pltpu.VMEM((ROWS, D), BF16), big, pltpu.VMEM((ROWS, HID), BF16), pltpu.VMEM((ROWS, HID), BF16), pltpu.VMEM((ROWS, D), BF16),
            pltpu.VMEM((ROWS, D), F32), pltpu.VMEM((ROWS, D), BF16), pltpu.VMEM((64, D), F32),
            pltpu.VMEM((pn.bunits * 8, 128), F32), pltpu.VMEM((pn.bunits, 8, 128), BF16),
            pltpu.SemaphoreType.DMA((NSEG,)), pltpu.SemaphoreType.DMA((NSEG,)), pltpu.SemaphoreType.DMA((NSEG,)), pltpu.SemaphoreType.DMA((2,)),
            pltpu.SemaphoreType.DMA((pn.nk * pn.ndp,)),
        ],
        compiler_params=pltpu.CompilerParams(vmem_limit_bytes=64000000),
        name="mlp",
    )(x, cot, ob, wp, w1, w2, vec, counts)


def table_grad(rel_ref, big, dtab):
    lane = lax.broadcasted_iota(jnp.int32, (32, 128), 1)
    for g in range(4):
        for pair in range(2):
            at = 1024 + g * 256 + pair * 128
            big[at:at + 64, :] = dtab[g, :, pair * 128:pair * 128 + 128]
    for g in range(4):
        for pair in range(2):
            at = 1024 + g * 256 + pair * 128
            even = big[pl.ds(at, 32, stride=2), :]
            odd = big[pl.ds(at + 1, 32, stride=2), :]
            h = 4 * g + 2 * pair
            big[pl.ds(h, 32, stride=16), :] = jnp.where(lane < 64, even, pltpu.roll(odd, 64, 1))
            big[pl.ds(h + 1, 32, stride=16), :] = jnp.where(lane < 64, pltpu.roll(even, 64, 1), odd)
    rel = rel_ref[...]
    row = lax.shift_right_arithmetic(rel, 3)
    low = rel & 7
    oh = (lax.broadcasted_iota(jnp.int32, (32, 4096), 0) == row).astype(F32).astype(BF16)
    grad = jnp.concatenate([big[kk * 16:kk * 16 + 16, :] for kk in range(32)], 1)
    out = jnp.zeros((32, 128), F32)
    high = grad.astype(BF16).astype(F32)
    for part in (high, grad - high):
        m = jnp.concatenate([jnp.where(low == j, part, 0.0) for j in range(8)], 0).astype(BF16)
        out = out + dot_nt(oh, m)
    return out


def kernel_c(pn, x_hbm, dx1_hbm, hw_hbm, qkv_hbm, p_hbm, wqkv, wp, vec, rel_ref,
             dx_hbm, gm, gs,
             x_v, dx1, hw, qkvb, pb, fs, os_, dq, dxv, dtab, acc, xsem, isem, psem, ysem):
    cps = window_copies(x_hbm, x_v, xsem, True)
    ins = [pltpu.make_async_copy(a, b, isem.at[n]) for n, (a, b) in enumerate([(dx1_hbm, dx1), (hw_hbm, hw), (qkv_hbm, qkvb), (p_hbm, pb)])]
    ins[0].start()
    ins[2].start()
    ins[3].start()
    ins[1].start()
    for c in cps:
        c.start()
    acc[...] = jnp.zeros_like(acc)
    dtab[...] = jnp.zeros_like(dtab)
    ins[0].wait()

    def rows0(t, _):
        r0 = pl.multiple_of(t * BLK, BLK)
        ev = dx1[pl.ds(r0, BLK), :].astype(BF16)
        for g in range(4):
            os_[pl.ds(g * RS + r0, BLK), :] = dot_nt(ev, wp[g * 128:(g + 1) * 128, :])
        return 0
    lax.fori_loop(0, NBLK, rows0, 0)
    ins[2].wait()
    ins[3].wait()
    heads = lane_head()

    def attend(i, _):
        w = lax.shift_right_arithmetic(i, 3)
        b = i & 7
        base = w * WROWS + b
        for g in range(4):
            do = take_rows(os_, g * RS + base).astype(BF16)
            q = qkvb[i, g]
            k = qkvb[i, 4 + g]
            v = qkvb[i, 8 + g]
            pbv = pb[i, g]
            p = pbv.astype(F32)
            dobd = block_diag(do, heads)
            dp = dot_nt(v, dobd)
            t = p * dp
            ds = t - p * jnp.sum(t, 0, keepdims=True)
            dtab[g] += ds
            dsb = ds.astype(BF16)
            put_rows(fs, (8 + g) * RS + base, dot(pbv, dobd))
            put_rows(fs, (4 + g) * RS + base, dot(dsb, block_diag(q, heads)))
            put_rows(fs, g * RS + base, diag_sum(dot_tn(dsb, k), heads) * SCALE)
        return 0
    lax.fori_loop(0, WB, attend, 0)
    for c in cps:
        c.wait()
    gain = vec[0:1, :]

    def rows1(t, _):
        r0 = pl.multiple_of(t * BLK, BLK)
        dn = jnp.zeros((BLK, D), F32)
        for c in range(12):
            v = fs[pl.ds(c * RS + r0, BLK), :]
            if c < 4 or c >= 8:
                i = 2 if c < 4 else 3
                acc[8 * i:8 * i + 8, (c % 4) * 128:(c % 4) * 128 + 128] += jnp.sum(v.reshape(BLK // 8, 8, 128), 0)
            dq[pl.ds(r0, BLK), c * 128:(c + 1) * 128] = v.astype(BF16)
        dn = dot_nt(dq[pl.ds(r0, BLK), :], wqkv[...])
        x = x_v[pl.ds(4 * t, 4)].reshape(BLK, D).astype(F32)
        xhat, r = norm_stats(x)
        acc_rows(acc, 0, dn * xhat)
        acc_rows(acc, 1, dn)
        dg = dn * gain
        dt = r * (dg - jnp.mean(dg, -1, keepdims=True) - xhat * jnp.mean(dg * xhat, -1, keepdims=True))
        dxv[pl.ds(4 * t, 4)] = (dx1[pl.ds(r0, BLK), :] + dt).reshape(4, 7, 8, D)
        return 0
    lax.fori_loop(0, NBLK, rows1, 0)
    ycs = window_copies(dx_hbm, dxv, ysem, False)
    for c in ycs:
        c.start()
    vg = jnp.sum(acc[...].reshape(8, 8, D), 1)
    tab = table_grad(rel_ref, os_, dtab)
    small = [vg[n:n + 1, c * 128:(c + 1) * 128] for n in range(4) for c in range(4)]
    small = [jnp.concatenate(small[:8], 0), jnp.concatenate(small[8:], 0), tab[0:8], tab[8:16], tab[16:24]]
    gs[...] = jnp.zeros_like(gs)
    for n, v in enumerate(small):
        gs[n & 1, n >> 1, 0] = v.astype(BF16)
    ins[1].wait()

    def wq(t, _):
        c0 = pl.multiple_of(t * 256, 256)
        v = dot_tn(hw[...], dq[:, pl.ds(c0, 256)])
        mu = pn.mrow // 8
        for i in range(2):
            u = v[:, i * 128:(i + 1) * 128].reshape(D // 8, 8, 128).astype(BF16)
            for p in range(pn.ndp):
                gm[p & 1, p >> 1, pl.ds((2 * t + i) * mu, mu)] = u[p * mu:(p + 1) * mu]
        return 0
    lax.fori_loop(0, 6, wq, 0)
    for c in ycs:
        c.wait()


def call_c(pn, x, dx1, hw, qkv, p, wqkv, wp, vec, rel):
    any_ = pl.BlockSpec(memory_space=pl.ANY)
    vm = pl.BlockSpec(memory_space=pltpu.VMEM)
    sds = jax.ShapeDtypeStruct
    outs = [sds((14, 14, 8, D), F32), sds((2, pn.rest, 12 * pn.mrow // 8, 8, 128), BF16), sds((2, pn.rest, 1, 8, 128), BF16)]
    return pl.pallas_call(
        functools.partial(kernel_c, pn),
        out_shape=outs,
        in_specs=[any_] * 5 + [vm] * 4,
        out_specs=[any_, vm, vm],
        scratch_shapes=[
            pltpu.VMEM((28, 7, 8, D), BF16), pltpu.VMEM((ROWS, D), F32), pltpu.VMEM((ROWS, D), BF16), pltpu.VMEM((WB, 12, 64, 128), BF16), pltpu.VMEM((WB, 4, 64, 256), BF16),
            pltpu.VMEM((12 * RS, 128), F32), pltpu.VMEM((4 * RS, 128), F32), pltpu.VMEM((ROWS, 3 * D), BF16), pltpu.VMEM((28, 7, 8, D), F32),
            pltpu.VMEM((4, 64, 256), F32), pltpu.VMEM((64, D), F32),
            pltpu.SemaphoreType.DMA((NSEG,)), pltpu.SemaphoreType.DMA((4,)), pltpu.SemaphoreType.DMA, pltpu.SemaphoreType.DMA((NSEG,)),
        ],
        compiler_params=pltpu.CompilerParams(vmem_limit_bytes=64000000),
        name="attend_back",
    )(x, dx1, hw, qkv, p, wqkv, wp, vec, rel)


import functools

MESH = pl.DeviceIdType.MESH
NMAT = 768


class Plan:
    def __init__(self, mesh, shard_len):
        self.ndp = mesh.shape["dp"]
        self.ns = mesh.shape["opt"]
        self.rest = self.ndp // 2
        self.units = shard_len // 1024
        self.pc = -(-self.units // self.ndp)
        self.ka = (BROW // 8) // self.units
        self.nk = self.ns - self.ka
        self.base = self.ka * self.units
        self.bunits = (self.nk - 1) * self.units + self.ndp * self.pc
        self.mrow = D // self.ndp
        self.gunits = max(BROW // 8 + 1, self.ndp * self.pc)


def place():
    me = lax.axis_index("dp")
    return lax.shift_right_arithmetic(me, 1), me & 1, lax.axis_index("opt")


def peer(r, c):
    return {"dp": 2 * r + c}


def enter(pn):
    r, c, z = place()
    bar = pltpu.get_barrier_semaphore()
    pl.semaphore_signal(bar, inc=1, device_id=peer(r, 1 - c), device_id_type=MESH)
    for j in range(1, pn.rest):
        pl.semaphore_signal(bar, inc=1, device_id=peer(lax.rem(r + j, pn.rest), c), device_id_type=MESH)
    for j in range(1, pn.ns):
        pl.semaphore_signal(bar, inc=1, device_id={"opt": lax.rem(z + j, pn.ns)}, device_id_type=MESH)
    pl.semaphore_wait(bar, pn.rest + pn.ns - 1)


def remote(src, dst, sems, n, where):
    return pltpu.make_async_remote_copy(src_ref=src, dst_ref=dst, send_sem=sems.at[0, n], recv_sem=sems.at[1, n], device_id=where, device_id_type=MESH)


class Chunk:
    def __init__(self, pn, n, scattered, last, src, r1, s1, r2, r3, ag, sems, lsem):
        self.pn, self.n, self.scattered, self.last = pn, n, scattered, last
        self.m = n // pn.nk if scattered else n
        self.src, self.r1, self.s1, self.r2, self.r3, self.ag, self.sems, self.lsem = src, r1, s1, r2, r3, ag, sems, lsem
        self.k2 = 1
        self.k3 = self.k2 + pn.rest - 1
        self.k4 = self.k3 + pn.ns - 1
        self.k5 = self.k4 + pn.rest - 1

    @staticmethod
    def nsems(pn):
        return 2 * pn.rest + pn.ns - 1

    def here(self, z):
        return z >= self.pn.ka if self.scattered else z <= self.last

    def c1(self):
        r, c, z = place()
        return remote(self.src.at[1 - c], self.r1, self.sems, 0, peer(r, 1 - c))

    def local(self):
        r, c, z = place()
        return pltpu.make_async_copy(self.src.at[c], self.s1, self.lsem)

    def start1(self):
        self.c1().start()
        self.local().start()

    def c2(self, j):
        r, c, z = place()
        to = lax.rem(r + j, self.pn.rest)
        return remote(self.s1.at[to], self.r2.at[j - 1], self.sems, self.k2 + j - 1, peer(to, c))

    def start2(self):
        r, c, z = place()
        self.local().wait()
        self.c1().wait()
        step = self.m
        for j in list(range(1, self.pn.rest)) + [0]:
            to = lax.rem(r + j, self.pn.rest)

            def add(t, _):
                u = pl.ds(t * step, step)
                self.s1[to, u] = (self.s1[to, u].astype(F32) + self.r1[to, u].astype(F32)).astype(BF16)
                return 0
            lax.fori_loop(0, self.n // step, add, 0)
            if j:
                self.c2(j).start()

    def c3(self, j):
        r, c, z = place()
        to = lax.rem(z + j, self.pn.ns)
        if self.scattered:
            src = self.s1.at[r, pl.ds(lax.max(to - self.pn.ka, 0) * self.m, self.m)]
        else:
            src = self.s1.at[r]
        return to, remote(src, self.r3.at[j - 1], self.sems, self.k3 + j - 1, {"opt": to})

    def start3(self):
        r, c, z = place()
        for j in range(1, self.pn.rest):
            self.c2(j).wait()
        step = self.m

        def add(t, _):
            u = pl.ds(t * step, step)
            v = self.s1[r, u].astype(F32)
            for j in range(1, self.pn.rest):
                v = v + self.r2[j - 1, u].astype(F32)
            self.s1[r, u] = v.astype(BF16)
            return 0
        lax.fori_loop(0, self.n // step, add, 0)
        for j in range(1, self.pn.ns):
            to, cp = self.c3(j)

            @pl.when(self.here(to))
            def _():
                cp.start()

    def c4(self, j):
        r, c, z = place()
        return remote(self.ag.at[c, r], self.ag.at[c, r], self.sems, self.k4 + j - 1, peer(lax.rem(r + j, self.pn.rest), c))

    def start4(self):
        r, c, z = place()
        for j in range(1, self.pn.ns):
            to, cp = self.c3(j)

            @pl.when(self.here(to))
            def _():
                cp.wait_send()

        @pl.when(self.here(z))
        def _():
            for j in range(1, self.pn.ns):
                self.c3(j)[1].wait_recv()
            if self.scattered:
                own = self.s1[r, pl.ds((z - self.pn.ka) * self.m, self.m)]
            else:
                own = self.s1[r]
            v = own.astype(F32)
            for j in range(1, self.pn.ns):
                v = v + self.r3[j - 1].astype(F32)
            self.ag[c, r] = v.astype(BF16)
            for j in range(1, self.pn.rest):
                self.c4(j).start()

    def c5(self):
        r, c, z = place()
        return remote(self.ag.at[c], self.ag.at[c], self.sems, self.k5, peer(r, 1 - c))

    def start5(self):
        r, c, z = place()

        @pl.when(self.here(z))
        def _():
            for j in range(1, self.pn.rest):
                self.c4(j).wait()
            self.c5().start()

    def finish(self):
        r, c, z = place()

        @pl.when(self.here(z))
        def _():
            self.c5().wait()


def chunk_scratch(pn, n, m):
    return [pltpu.VMEM((pn.rest, n, 8, 128), BF16), pltpu.VMEM((pn.rest, n, 8, 128), BF16), pltpu.VMEM((pn.rest - 1, n, 8, 128), BF16),
            pltpu.VMEM((pn.ns - 1, m, 8, 128), BF16), pltpu.VMEM((2, pn.rest, m, 8, 128), BF16),
            pltpu.SemaphoreType.DMA((2, Chunk.nsems(pn))), pltpu.SemaphoreType.DMA]


GROUP_ROWS = [R_G1, R_B1, R_QKV, R_BQ, R_BV, R_TAB]
STEP = 2
DECAYED = (2, 6, 10, 12)
LENGTHS = [D, D, 3 * D * D, D, D, TAB * HEADS, D * D, D, D, D, D * HID, HID, HID * D, D]


def adam_units(pn, rates, g, p_v, m_v, w_v, g_v, goff, first, u0, n):
    sl = pl.ds(u0, n)
    grad = g[pl.ds((goff + u0) * 8, n * 8), :].reshape(n, 8, 128)
    shape = (n, 8, 128)
    index = ((first + u0 + lax.broadcasted_iota(jnp.int32, shape, 0)) * 8 + lax.broadcasted_iota(jnp.int32, shape, 1)) * 128 + lax.broadcasted_iota(jnp.int32, shape, 2)
    rate = jnp.zeros(shape, F32) + rates[0]
    decay = jnp.zeros(shape, F32)
    at = 0
    for n_, length in enumerate(LENGTHS):
        at += length
        after = index >= at
        rate = jnp.where(after, rates[n_ + 1], rate)
        if n_ in DECAYED or n_ + 1 in DECAYED:
            decay = jnp.where(after, 0.05 if n_ + 1 in DECAYED else 0.0, decay)
    w = p_v[sl]
    m = 0.9 * m_v[sl] + 0.1 * grad
    s = 0.999 * w_v[sl] + 0.001 * grad * grad
    mh = m / (1.0 - 0.9 ** STEP)
    sh = s / (1.0 - 0.999 ** STEP)
    p_v[sl] = w - rate * (mh / (jnp.sqrt(sh) + 1e-08) + decay * w)
    m_v[sl] = m
    w_v[sl] = s
    g_v[sl] = grad


def spread_grad(pn, g, agb, agm, ags):
    r, c, z = place()

    @pl.when(z >= pn.ka)
    def _():
        def piece(p, _):
            g[pl.ds(p * pn.pc * 8, pn.pc * 8), :] = agb[p & 1, lax.shift_right_arithmetic(p, 1)].astype(F32).reshape(pn.pc * 8, 128)
            return 0
        lax.fori_loop(0, pn.ndp, piece, 0)

    @pl.when(z < pn.ka)
    def _():
        def piece(p, _):
            for col in range(12):
                v = agm[p & 1, lax.shift_right_arithmetic(p, 1), col * (pn.mrow // 8):(col + 1) * (pn.mrow // 8)].astype(F32).reshape(pn.mrow, 128)
                g[pl.ds(R_QKV + p * pn.mrow * 12 + col, pn.mrow, stride=12), :] = v
            return 0
        lax.fori_loop(0, pn.ndp, piece, 0)
        for n, u in enumerate((0, 769, 770, 771, 772)):
            g[u * 8:u * 8 + 8, :] = ags[n & 1, n >> 1, 0].astype(F32)

    @pl.when(z == pn.ka)
    def _():
        for n, u in enumerate((0, 769, 770, 771, 772)):
            if u >= pn.base:
                k = (u - pn.base) * 8
                g[k:k + 8, :] += ags[n & 1, n >> 1, 0].astype(F32)


def kernel_d(pn, gb, gm, gs, rates, params, mom1, mom2, *rest):
    (grad_o, p_o, m_o, w_o, rb1, sb1, rb2, rb3, agb, semb, lb, rm1, sm1, rm2, rm3, agm, semm, lm, rs1, ss1, rs2, rs3, ags, sems, ls,
     g, g_v, p_v, m_v, w_v, isem, osem) = rest
    ins = [pltpu.make_async_copy(a, b, isem.at[n]) for n, (a, b) in enumerate([(params, p_v), (mom1, m_v), (mom2, w_v)])]
    for cp in ins:
        cp.start()
    enter(pn)
    chunks = [Chunk(pn, pn.nk * pn.pc, True, 0, gb, rb1, sb1, rb2, rb3, agb, semb, lb),
              Chunk(pn, 12 * pn.mrow // 8, False, pn.ka - 1, gm, rm1, sm1, rm2, rm3, agm, semm, lm),
              Chunk(pn, 1, False, pn.ka, gs, rs1, ss1, rs2, rs3, ags, sems, ls)]
    for step in ("start1", "start2", "start3", "start4", "start5", "finish"):
        for ch in chunks:
            getattr(ch, step)()
    spread_grad(pn, g, agb, agm, ags)
    r, c, z = place()
    goff = lax.select(z < pn.ka, z * pn.units, 0)
    first = z * pn.units
    for cp in ins:
        cp.wait()
    blk = 32
    full = pn.units // blk

    def body(t, _):
        adam_units(pn, rates, g, p_v, m_v, w_v, g_v, goff, first, t * blk, blk)
        return 0
    lax.fori_loop(0, full, body, 0)
    if pn.units % blk:
        adam_units(pn, rates, g, p_v, m_v, w_v, g_v, goff, first, full * blk, pn.units % blk)
    outs = [pltpu.make_async_copy(a, b, osem.at[n]) for n, (a, b) in enumerate([(g_v, grad_o), (p_v, p_o), (m_v, m_o), (w_v, w_o)])]
    for cp in outs:
        cp.start()
    for cp in outs:
        cp.wait()


def call_d(pn, gb, gm, gs, rates, params, mom1, mom2):
    any_ = pl.BlockSpec(memory_space=pl.ANY)
    shard = jax.ShapeDtypeStruct((pn.units, 8, 128), F32)
    sv = pltpu.VMEM((pn.units, 8, 128), F32)
    view = lambda t: t.reshape(pn.units, 8, 128)
    out = pl.pallas_call(
        functools.partial(kernel_d, pn),
        out_shape=[shard] * 4,
        in_specs=[any_] * 3 + [pl.BlockSpec(memory_space=pltpu.SMEM)] + [any_] * 3,
        out_specs=[any_] * 4,
        scratch_shapes=chunk_scratch(pn, pn.nk * pn.pc, pn.pc) + chunk_scratch(pn, 12 * pn.mrow // 8, 12 * pn.mrow // 8) + chunk_scratch(pn, 1, 1)
        + [pltpu.VMEM((pn.gunits * 8, 128), F32), sv, sv, sv, sv, pltpu.SemaphoreType.DMA((3,)), pltpu.SemaphoreType.DMA((4,))],
        compiler_params=pltpu.CompilerParams(vmem_limit_bytes=64000000, collective_id=1, has_side_effects=True),
        name="reduce",
    )(gb, gm, gs, rates, view(params), view(mom1), view(mom2))
    return [t.reshape(-1) for t in out]


def kernel_g(pn, params, w_o, p_v, wb, sems, isem, osem):
    r, c, z = place()
    cp = pltpu.make_async_copy(params, p_v.at[pl.ds(0, pn.units)], isem)
    cp.start()
    enter(pn)
    cp.wait()

    def cast(p, _):
        wb[z, p & 1, lax.shift_right_arithmetic(p, 1)] = p_v[pl.ds(p * pn.pc, pn.pc)].astype(BF16)
        return 0
    lax.fori_loop(0, pn.ndp, cast, 0)

    def o(j):
        to = lax.rem(z + j, pn.ns)
        return remote(wb.at[z, c, r], wb.at[z, c, r], sems, j - 1, {"opt": to})

    def x(k, j):
        to = lax.rem(r + j, pn.rest)
        src = lax.rem(z - k + pn.ns, pn.ns)
        return remote(wb.at[src, c, r], wb.at[src, c, r], sems, pn.ns - 1 + (k - 1) * (pn.rest - 1) + j - 1, peer(to, c))

    def y(k):
        src = lax.rem(z - k + pn.ns, pn.ns)
        return remote(wb.at[src, c], wb.at[src, c], sems, (pn.ns - 1) * pn.rest + k - 1, peer(r, 1 - c))

    for j in range(1, pn.ns):
        o(j).start()
    for k in range(1, pn.ns):
        o(k).wait()
        for j in range(1, pn.rest):
            x(k, j).start()
    for k in range(1, pn.ns):
        for j in range(1, pn.rest):
            x(k, j).wait()
        y(k).start()
    for k in range(1, pn.ns):
        y(k).wait()
    cp = pltpu.make_async_copy(wb, w_o, osem)
    cp.start()
    cp.wait()


def call_g(pn, params):
    any_ = pl.BlockSpec(memory_space=pl.ANY)
    shape = (pn.ns, 2, pn.rest, pn.pc, 8, 128)
    nsem = (pn.ns - 1) * (pn.rest + 1)
    return pl.pallas_call(
        functools.partial(kernel_g, pn),
        out_shape=jax.ShapeDtypeStruct(shape, BF16),
        in_specs=[any_],
        out_specs=any_,
        scratch_shapes=[pltpu.VMEM((pn.ndp * pn.pc, 8, 128), F32), pltpu.VMEM(shape, BF16), pltpu.SemaphoreType.DMA((2, nsem)), pltpu.SemaphoreType.DMA, pltpu.SemaphoreType.DMA],
        compiler_params=pltpu.CompilerParams(vmem_limit_bytes=64000000, collective_id=0, has_side_effects=True),
        name="gather",
    )(params.reshape(pn.units, 8, 128))


from jax.sharding import PartitionSpec as P


def solution(mesh):
    def local(images, cotangent, counts, rel_index, params, moment1, moment2, rates):
        pn = Plan(mesh, params.shape[0])
        xt = images.transpose(1, 2, 0, 3)
        ct = cotangent.transpose(1, 2, 0, 3)
        rel = rel_lanes(rel_index)
        flat = call_g(pn, params)
        wqkv, wp, w1, w2, vec, hw, ob, qkv, p = call_a(pn, xt, flat, rel)
        y, dx1, gb = call_b(pn, xt, ct, ob, wp, w1, w2, vec, counts)
        dx, gm, gs = call_c(pn, xt, dx1, hw, qkv, p, wqkv, wp, vec, rel)
        grad, new_params, new_first, new_second = call_d(pn, gb, gm, gs, rates, params, moment1, moment2)
        return (y.transpose(2, 0, 1, 3), dx.transpose(2, 0, 1, 3), grad, new_params, new_first, new_second)

    split = P(("dp", "opt"), None, None, None)
    return jax.shard_map(
        local, mesh=mesh,
        in_specs=(split, split, P(("dp", "opt")), P(), P("opt"), P("opt"), P("opt"), P()),
        out_specs=(split, split, P("opt"), P("opt"), P("opt"), P("opt")),
        check_vma=False)
```

```python
import functools
import jax
import jax.numpy as jnp
from jax import lax
from jax.experimental import pallas as pl
from jax.experimental.pallas import tpu as pltpu

D = 512
HEADS = 16
HEAD_DIM = 32
HID = 2048
SIDE = 14
WIN = 7
SHIFT = 3
TAB = 169
F32 = jnp.float32
BF16 = jnp.bfloat16

IMGS = 8
SPAN = WIN * WIN
WROWS = SPAN * IMGS
ROWS = 4 * WROWS
RS = ROWS + 64
BLK = 224
NBLK = ROWS // BLK
WB = 4 * IMGS
SCALE = HEAD_DIM ** -0.5

R_G1, R_B1, R_QKV, R_BQ, R_BV, R_TAB = 0, 4, 8, 6152, 6156, 6160
R_PROJ, R_BP, R_G2, R_B2, R_W1, R_C1, R_W2, R_C2, R_END = 6181, 8229, 8233, 8237, 8241, 16433, 16449, 24641, 24645
LANE = 16
BROW = 6176


def segments(w):
    if w == 0:
        return [(SHIFT, WIN, 0)]
    return [(WIN + SHIFT, WIN - SHIFT, 0), (0, SHIFT, WIN - SHIFT)]


def window_copies(hbm, vmem, sem, inward):
    out = []
    n = 0
    for wy in range(2):
        for wx in range(2):
            for ys, yl, yo in segments(wy):
                for xs, xl, xo in segments(wx):
                    a = hbm.at[pl.ds(ys, yl), pl.ds(xs, xl)]
                    b = vmem.at[pl.ds((2 * wy + wx) * WIN + yo, yl), pl.ds(xo, xl)]
                    out.append(pltpu.make_async_copy(a, b, sem.at[n]) if inward else pltpu.make_async_copy(b, a, sem.at[n]))
                    n += 1
    return out


NSEG = 9


def dot(a, b):
    return lax.dot_general(a, b, (((1,), (0,)), ((), ())), preferred_element_type=F32)


def dot_nt(a, b):
    return lax.dot_general(a, b, (((1,), (1,)), ((), ())), preferred_element_type=F32)


def dot_tn(a, b):
    return lax.dot_general(a, b, (((0,), (0,)), ((), ())), preferred_element_type=F32)


def norm_stats(x):
    mean = jnp.mean(x, -1, keepdims=True)
    dev = x - mean
    var = jnp.mean(dev * dev, -1, keepdims=True)
    r = lax.rsqrt(var + 1e-05)
    return dev * r, r


def pieces_to_rows(pn, wb, fs, shard, count, base):
    def body(p, _):
        row = pl.multiple_of((shard * pn.units - base + p * pn.pc) * 8, 8)
        fs[pl.ds(row, pn.pc * 8), :] = wb[shard, p & 1, lax.shift_right_arithmetic(p, 1)].astype(F32).reshape(pn.pc * 8, 128)
        return 0
    lax.fori_loop(0, count, body, 0)


def vec_from(fs, row, width, shift):
    parts = []
    lane = lax.broadcasted_iota(jnp.int32, (1, 128), 1)
    for c in range(width // 128):
        a = fs[pl.ds(row + c, 1), :]
        if shift:
            b = fs[pl.ds(row + c + 1, 1), :]
            a = jnp.where(lane < 128 - LANE, pltpu.roll(a, 128 - LANE, 1), pltpu.roll(b, 128 - LANE, 1))
        parts.append(a)
    return jnp.concatenate(parts, 1)


def take_matrix(fs, row, dst, nrows, ncb, shift, step=128):
    lane = lax.broadcasted_iota(jnp.int32, (step, 128), 1)

    def body(t, _):
        base = row + t * (step * ncb)
        r0 = pl.multiple_of(t * step, step)
        for c in range(ncb):
            a = fs[pl.ds(base + c, step, stride=ncb), :]
            if shift:
                b = fs[pl.ds(base + c + 1, step, stride=ncb), :]
                a = jnp.where(lane < 128 - LANE, pltpu.roll(a, 128 - LANE, 1), pltpu.roll(b, 128 - LANE, 1))
            dst[pl.ds(r0, step), c * 128:(c + 1) * 128] = a.astype(BF16)
        return 0

    lax.fori_loop(0, nrows // step, body, 0)


def transpose_rows(src, dst):
    full = ROWS // 128

    def body(t, _):
        r0 = pl.multiple_of(t * 128, 128)
        dst[:, pl.ds(r0, 128)] = src[pl.ds(r0, 128), :].T
        return 0
    lax.fori_loop(0, full, body, 0)
    if ROWS % 128:
        dst[:, full * 128:ROWS] = src[full * 128:ROWS, :].T


def lane_head():
    return lax.broadcasted_iota(jnp.int32, (64, 128), 1) // HEAD_DIM


def block_diag(v, heads):
    zero = jnp.zeros_like(v)
    return jnp.concatenate([jnp.where(heads == h, v, zero) for h in range(4)], 0)


def diag_sum(r, heads):
    out = r[0:64]
    for h in range(1, 4):
        out = jnp.where(heads == h, r[64 * h:64 * h + 64], out)
    return out


def take_rows(fs, start):
    v = fs[pl.ds(start, 56, stride=IMGS), :]
    v = jnp.where(lax.broadcasted_iota(jnp.int32, (56, 128), 0) < SPAN, v, 0.0)
    return jnp.concatenate([v, jnp.zeros((8, 128), F32)], 0)


def put_rows(fs, start, v):
    fs[pl.ds(start, 48, stride=IMGS), :] = v[0:48]
    fs[pl.ds(start + 48 * IMGS, 1), :] = v[48:49]


def build_bias(tab3, rel_ref, big, bias):
    rel = rel_ref[...]
    row = lax.shift_right_arithmetic(rel, 3)
    low = rel & 7
    oh = (lax.broadcasted_iota(jnp.int32, (32, 4096), 0) == row).astype(F32).astype(BF16)
    tab = jnp.concatenate([tab3, jnp.zeros((8, 128), F32)], 0).astype(BF16)
    r = dot_tn(tab, oh)
    acc = jnp.zeros((16, 4096), F32)
    for j in range(8):
        acc = acc + jnp.where(low == j, r[16 * j:16 * j + 16], 0.0)
    for kk in range(32):
        big[kk * 16:kk * 16 + 16, :] = acc[:, kk * 128:kk * 128 + 128]
    k = lax.broadcasted_iota(jnp.int32, (64, 256), 0)
    q = lax.broadcasted_iota(jnp.int32, (64, 256), 1) & 63
    ki = lax.shift_right_arithmetic(k * 37, 8)
    kj = k - ki * 7
    qi = lax.shift_right_arithmetic(q * 37, 8)
    qj = q - qi * 7
    cut = WIN - SHIFT
    same_y = (ki < cut) == (qi < cut)
    same_x = (kj < cut) == (qj < cut)
    lane = lax.broadcasted_iota(jnp.int32, (32, 128), 1)
    for g in range(4):
        for pair in range(2):
            h = 4 * g + 2 * pair
            a = big[pl.ds(h, 32, stride=16), :]
            b = big[pl.ds(h + 1, 32, stride=16), :]
            even = jnp.where(lane < 64, a, pltpu.roll(b, 64, 1))
            odd = jnp.where(lane < 64, pltpu.roll(a, 64, 1), b)
            big[pl.ds(1024 + g * 256 + pair * 128, 32, stride=2), :] = even
            big[pl.ds(1024 + g * 256 + pair * 128 + 1, 32, stride=2), :] = odd
    for g in range(4):
        pos = jnp.concatenate([big[1024 + g * 256:1024 + g * 256 + 64, :], big[1024 + g * 256 + 128:1024 + g * 256 + 192, :]], 1)
        for w in range(4):
            keep = None
            if w == 1:
                keep = same_x
            elif w == 2:
                keep = same_y
            elif w == 3:
                keep = same_y & same_x
            val = pos if keep is None else pos + jnp.where(keep, 0.0, -100.0)
            bias[w * 4 + g] = jnp.where(k < SPAN, val, -1e30)


def kernel_a(pn, x_hbm, flat_hbm, rel_ref,
             wqkv_o, wp_o, w1_o, w2_o, vec_o, hw_o, ob_o, qkv_o, p_o,
             x_v, flat_v, fs, os_, bias, wqkv, wp, w1, w2, vec, hw, hwt, ob, qkvb, pb, xsem, fsem, osem, wsem):
    cps = window_copies(x_hbm, x_v, xsem, True)
    for c in cps:
        c.start()
    fcp = pltpu.make_async_copy(flat_hbm, flat_v, fsem)
    fcp.start()
    fcp.wait()
    for k in range(pn.ka):
        pieces_to_rows(pn, flat_v, fs, k, pn.ndp, 0)
    pieces_to_rows(pn, flat_v, fs, pn.ka, 1, 0)
    take_matrix(fs, R_QKV, wqkv, D, 12, False)
    vec[0:1, :] = vec_from(fs, R_G1, D, False)
    vec[1:2, :] = vec_from(fs, R_B1, D, False)
    vec[2:3, :] = vec_from(fs, R_BQ, D, False)
    vec[3:4, :] = vec_from(fs, R_BV, D, False)
    build_bias(fs[R_TAB:R_TAB + 24, :], rel_ref, os_, bias)
    for c in cps:
        c.wait()
    gain = vec[0:1, :]
    shift = vec[1:2, :]
    bq = vec[2:3, :]
    bv = vec[3:4, :]

    def rows(t, _):
        r0 = pl.multiple_of(t * BLK, BLK)
        x = x_v[pl.ds(4 * t, 4)].reshape(BLK, D).astype(F32)
        xhat, _r = norm_stats(x)
        h = (xhat * gain + shift).astype(BF16)
        hw[pl.ds(r0, BLK), :] = h
        for c in range(12):
            y = dot(h, wqkv[:, c * 128:(c + 1) * 128])
            if c < 4:
                y = (y + bq[:, c * 128:(c + 1) * 128]) * SCALE
            if c >= 8:
                y = y + bv[:, (c - 8) * 128:(c - 7) * 128]
            fs[pl.ds(c * RS + r0, BLK), :] = y
        return 0
    lax.fori_loop(0, NBLK, rows, 0)

    heads = lane_head()

    def attend(i, _):
        w = lax.shift_right_arithmetic(i, 3)
        b = i & 7
        base = w * WROWS + b
        for g in range(4):
            q = take_rows(fs, g * RS + base).astype(BF16)
            k = take_rows(fs, (4 + g) * RS + base).astype(BF16)
            v = take_rows(fs, (8 + g) * RS + base).astype(BF16)
            qkvb[i, g] = q
            qkvb[i, 4 + g] = k
            qkvb[i, 8 + g] = v
            s = dot_nt(k, block_diag(q, heads)) + bias[w * 4 + g]
            m = jnp.max(s, 0, keepdims=True)
            e = jnp.exp(s - m)
            p = (e * (1.0 / jnp.sum(e, 0, keepdims=True))).astype(BF16)
            pb[i, g] = p
            o = diag_sum(dot_tn(p, v), heads)
            put_rows(os_, g * RS + base, o)
        return 0
    lax.fori_loop(0, WB, attend, 0)

    def outs(t, _):
        r0 = pl.multiple_of(t * BLK, BLK)
        for g in range(4):
            ob[pl.ds(r0, BLK), g * 128:(g + 1) * 128] = os_[pl.ds(g * RS + r0, BLK), :].astype(BF16)
        return 0
    lax.fori_loop(0, NBLK, outs, 0)
    transpose_rows(hw, hwt)
    cos = [pltpu.make_async_copy(a, b, osem.at[n]) for n, (a, b) in enumerate([(hwt, hw_o), (ob, ob_o), (qkvb, qkv_o), (pb, p_o)])]
    for c in cos:
        c.start()
    for k in range(pn.ka, pn.ns):
        pieces_to_rows(pn, flat_v, fs, k, pn.ndp, pn.base)
    first = pn.base * 8
    take_matrix(fs, R_PROJ - first, wp, D, 4, True)
    take_matrix(fs, R_W1 - first, w1, D, 16, True)
    take_matrix(fs, R_W2 - first, w2, HID, 4, True)
    for n, r in enumerate((R_BP, R_G2, R_B2, R_C2)):
        vec[4 + n:5 + n, :] = vec_from(fs, r - first, D, True)
    for n in range(4):
        vec[8 + n:9 + n, :] = vec_from(fs, R_C1 - first + 4 * n, D, True)
    wos = [pltpu.make_async_copy(a, b, wsem.at[n]) for n, (a, b) in enumerate([(wqkv, wqkv_o), (wp, wp_o), (w1, w1_o), (w2, w2_o), (vec, vec_o)])]
    for c in wos:
        c.start()
    for c in cos + wos:
        c.wait()


def call_a(pn, x, flat, rel):
    any_ = pl.BlockSpec(memory_space=pl.ANY)
    sds = jax.ShapeDtypeStruct
    outs = [sds((D, 3 * D), BF16), sds((D, D), BF16), sds((D, HID), BF16), sds((HID, D), BF16), sds((16, D), F32),
            sds((D, ROWS), BF16), sds((ROWS, D), BF16), sds((WB, 12, 64, 128), BF16), sds((WB, 4, 64, 256), BF16)]
    return pl.pallas_call(
        functools.partial(kernel_a, pn),
        out_shape=outs,
        in_specs=[any_, any_, pl.BlockSpec(memory_space=pltpu.VMEM)],
        out_specs=[any_] * len(outs),
        scratch_shapes=[
            pltpu.VMEM((28, 7, 8, D), BF16), pltpu.VMEM(flat.shape, BF16), pltpu.VMEM((12 * RS, 128), F32), pltpu.VMEM((4 * RS, 128), F32),
            pltpu.VMEM((16, 64, 256), F32), pltpu.VMEM((D, 3 * D), BF16), pltpu.VMEM((D, D), BF16), pltpu.VMEM((D, HID), BF16), pltpu.VMEM((HID, D), BF16),
            pltpu.VMEM((16, D), F32), pltpu.VMEM((ROWS, D), BF16), pltpu.VMEM((D, ROWS), BF16), pltpu.VMEM((ROWS, D), BF16), pltpu.VMEM((WB, 12, 64, 128), BF16), pltpu.VMEM((WB, 4, 64, 256), BF16),
            pltpu.SemaphoreType.DMA((NSEG,)), pltpu.SemaphoreType.DMA, pltpu.SemaphoreType.DMA((4,)), pltpu.SemaphoreType.DMA((5,)),
        ],
        compiler_params=pltpu.CompilerParams(vmem_limit_bytes=64000000),
        name="attend",
    )(x, flat, rel)


def rel_lanes(rel_index):
    t = jnp.full((64, 64), -1, jnp.int32).at[:SPAN, :SPAN].set(rel_index.T)
    return t.reshape(1, 4096)


CH = 512
INV_SQRT2 = 0.7071067811865476
INV_SQRT2PI = 0.3989422804014327


def gelu_parts(u):
    e = jnp.exp(u * u * -0.5)
    t = 1.0 / (1.0 + jnp.abs(u) * (0.3275911 * INV_SQRT2))
    half = t * (0.127414796 + t * (-0.142248368 + t * (0.7107068705 + t * (-0.7265760135 + t * 0.5307027145)))) * e
    cdf = jnp.where(u >= 0, 1.0 - half, half)
    return cdf, e * INV_SQRT2PI


def put_block(fs, start, stride, v):
    n = v.shape[0]
    lane = lax.broadcasted_iota(jnp.int32, (n, 128), 1)
    v = pltpu.roll(v, LANE, 1)
    here = pl.ds(start, n, stride=stride) if n > 1 else pl.ds(start, 1)
    fs[here, :] = jnp.where(lane >= LANE, v, fs[here, :])
    here = pl.ds(start + 1, n, stride=stride) if n > 1 else pl.ds(start + 1, 1)
    fs[here, :] = jnp.where(lane < LANE, v, fs[here, :])


def put_vec(fs, row, v):
    for c in range(v.shape[1] // 128):
        put_block(fs, row + c, 1, v[:, c * 128:(c + 1) * 128])


def acc_rows(ref, i, v):
    ref[8 * i:8 * i + 8, 0:v.shape[1]] += jnp.sum(v.reshape(v.shape[0] // 8, 8, v.shape[1]), 0)


def table_grad(rel_ref, big, dtab):
    lane = lax.broadcasted_iota(jnp.int32, (32, 128), 1)
    for g in range(4):
        for pair in range(2):
            at = 1024 + g * 256 + pair * 128
            big[at:at + 64, :] = dtab[g, :, pair * 128:pair * 128 + 128]
    for g in range(4):
        for pair in range(2):
            at = 1024 + g * 256 + pair * 128
            even = big[pl.ds(at, 32, stride=2), :]
            odd = big[pl.ds(at + 1, 32, stride=2), :]
            h = 4 * g + 2 * pair
            big[pl.ds(h, 32, stride=16), :] = jnp.where(lane < 64, even, pltpu.roll(odd, 64, 1))
            big[pl.ds(h + 1, 32, stride=16), :] = jnp.where(lane < 64, pltpu.roll(even, 64, 1), odd)
    rel = rel_ref[...]
    row = lax.shift_right_arithmetic(rel, 3)
    low = rel & 7
    oh = (lax.broadcasted_iota(jnp.int32, (32, 4096), 0) == row).astype(F32).astype(BF16)
    grad = jnp.concatenate([big[kk * 16:kk * 16 + 16, :] for kk in range(32)], 1)
    out = jnp.zeros((32, 128), F32)
    high = grad.astype(BF16).astype(F32)
    for part in (high, grad - high):
        m = jnp.concatenate([jnp.where(low == j, part, 0.0) for j in range(8)], 0).astype(BF16)
        out = out + dot_nt(oh, m)
    return out


MESH = pl.DeviceIdType.MESH
NMAT = 768


class Plan:
    def __init__(self, mesh, shard_len):
        self.ndp = mesh.shape["dp"]
        self.ns = mesh.shape["opt"]
        self.rest = self.ndp // 2
        self.units = shard_len // 1024
        self.pc = -(-self.units // self.ndp)
        self.ka = (BROW // 8) // self.units
        self.base = self.ka * self.units
        self.bunits = (self.ns - self.ka - 1) * self.units + self.ndp * self.pc
        self.kh = -(-(R_W2 // 8 + 1) // self.units)
        self.mrow = D // self.ndp
        self.gunits = max(BROW // 8 + 1, self.ndp * self.pc)


def place():
    me = lax.axis_index("dp")
    return lax.shift_right_arithmetic(me, 1), me & 1, lax.axis_index("opt")


def peer(r, c):
    return {"dp": 2 * r + c}


def enter(pn, all_dp=False):
    r, c, z = place()
    bar = pltpu.get_barrier_semaphore()
    pl.semaphore_signal(bar, inc=1, device_id=peer(r, 1 - c), device_id_type=MESH)
    for j in range(1, pn.rest):
        for to in ((c, 1 - c) if all_dp else (c,)):
            pl.semaphore_signal(bar, inc=1, device_id=peer(lax.rem(r + j, pn.rest), to), device_id_type=MESH)
    for j in range(1, pn.ns):
        pl.semaphore_signal(bar, inc=1, device_id={"opt": lax.rem(z + j, pn.ns)}, device_id_type=MESH)
    pl.semaphore_wait(bar, (pn.ndp - 1 if all_dp else pn.rest) + pn.ns - 1)


def remote(src, dst, sems, n, where):
    return pltpu.make_async_remote_copy(src_ref=src, dst_ref=dst, send_sem=sems.at[0, n], recv_sem=sems.at[1, n], device_id=where, device_id_type=MESH)


class Chunk:
    def __init__(self, pn, k0, k1, scatter, m, src, r1, r2, r3, sems, ag):
        self.pn, self.k0, self.k1, self.scatter, self.m = pn, k0, k1, scatter, m
        self.n = m * (k1 - k0) if scatter else m
        self.src, self.r1, self.r2, self.r3, self.ag, self.sems = src, r1, r2, r3, ag, sems
        self.k2 = 1
        self.k3 = self.k2 + pn.rest - 1
        self.k4 = self.k3 + pn.ns - 1
        self.k5 = self.k4 + pn.rest - 1

    @staticmethod
    def scratch(pn, m, count, shared):
        n = m * count
        return [pltpu.VMEM((2, pn.rest, n, 8, 128), BF16), pltpu.VMEM((pn.rest, n, 8, 128), BF16), pltpu.VMEM((pn.rest - 1, n, 8, 128), BF16),
                pltpu.VMEM((pn.ns - 1, m, 8, 128), BF16),
                pltpu.SemaphoreType.DMA((2, 2 * pn.rest + pn.ns - 1))] + [pltpu.VMEM((2, pn.rest, m, 8, 128), BF16)] * (not shared)

    def here(self, z):
        return (z >= self.k0) & (z < self.k1)

    def c1(self):
        r, c, z = place()
        return remote(self.src.at[1 - c], self.r1, self.sems, 0, peer(r, 1 - c))

    def start1(self):
        self.c1().start()

    def c2(self, j):
        r, c, z = place()
        to = lax.rem(r + j, self.pn.rest)
        return remote(self.src.at[c, to], self.r2.at[j - 1], self.sems, self.k2 + j - 1, peer(to, c))

    def start2(self):
        r, c, z = place()
        self.c1().wait()
        step = self.m
        for j in list(range(1, self.pn.rest)) + [0]:
            to = lax.rem(r + j, self.pn.rest)

            def add(t, _):
                u = pl.ds(t * step, step)
                self.src[c, to, u] = (self.src[c, to, u].astype(F32) + self.r1[to, u].astype(F32)).astype(BF16)
                return 0
            lax.fori_loop(0, self.n // step, add, 0)
            if j:
                self.c2(j).start()

    def c3(self, j):
        r, c, z = place()
        to = lax.rem(z + j, self.pn.ns)
        src = self.src.at[c, r]
        if self.scatter:
            src = src.at[pl.ds(lax.clamp(0, to - self.k0, self.k1 - self.k0 - 1) * self.m, self.m)]
        return to, remote(src, self.r3.at[j - 1], self.sems, self.k3 + j - 1, {"opt": to})

    def start3(self):
        r, c, z = place()
        for j in range(1, self.pn.rest):
            self.c2(j).wait()
        step = self.m

        def add(t, _):
            u = pl.ds(t * step, step)
            v = self.src[c, r, u].astype(F32)
            for j in range(1, self.pn.rest):
                v = v + self.r2[j - 1, u].astype(F32)
            self.src[c, r, u] = v.astype(BF16)
            return 0
        lax.fori_loop(0, self.n // step, add, 0)
        for j in range(1, self.pn.ns):
            to, cp = self.c3(j)

            @pl.when(self.here(to))
            def _():
                cp.start()

    def c4(self, j):
        r, c, z = place()
        return remote(self.ag.at[c, r], self.ag.at[c, r], self.sems, self.k4 + j - 1, peer(lax.rem(r + j, self.pn.rest), c))

    def start4(self):
        r, c, z = place()
        for j in range(1, self.pn.ns):
            to, cp = self.c3(j)

            @pl.when(self.here(to))
            def _():
                cp.wait_send()

        @pl.when(self.here(z))
        def _():
            for j in range(1, self.pn.ns):
                self.c3(j)[1].wait_recv()
            at = lax.clamp(0, z - self.k0, self.k1 - self.k0 - 1) * self.m if self.scatter else 0
            v = self.src[c, r, pl.ds(at, self.m)].astype(F32)
            for j in range(1, self.pn.ns):
                v = v + self.r3[j - 1].astype(F32)
            self.ag[c, r] = v.astype(BF16)
            for j in range(1, self.pn.rest):
                self.c4(j).start()

    def c5(self):
        r, c, z = place()
        return remote(self.ag.at[c], self.ag.at[c], self.sems, self.k5, peer(r, 1 - c))

    def start5(self):
        r, c, z = place()

        @pl.when(self.here(z))
        def _():
            for j in range(1, self.pn.rest):
                self.c4(j).wait()
            self.c5().start()

    def finish(self):
        r, c, z = place()

        @pl.when(self.here(z))
        def _():
            self.c5().wait()


SMALL = (0, 769, 770, 771, 772)


class Small:
    def __init__(self, pn, own, r1, mid, r2, sems):
        self.pn, self.own, self.r1, self.mid, self.r2, self.sems = pn, own, r1, mid, r2, sems

    @staticmethod
    def scratch(pn):
        u = len(SMALL)
        return [pltpu.VMEM((u, 8, 128), BF16), pltpu.VMEM((pn.ndp, u, 8, 128), BF16), pltpu.VMEM((u, 8, 128), BF16), pltpu.VMEM((pn.ns, u, 8, 128), BF16),
                pltpu.SemaphoreType.DMA((2, pn.ndp + pn.ns - 2))]

    def c1(self, j):
        me = lax.axis_index("dp")
        return remote(self.own, self.r1.at[me], self.sems, j - 1, {"dp": lax.rem(me + j, self.pn.ndp)})

    def w1(self, j):
        me = lax.axis_index("dp")
        return remote(self.own, self.r1.at[lax.rem(me - j + self.pn.ndp, self.pn.ndp)], self.sems, j - 1, {"dp": lax.rem(me + j, self.pn.ndp)})

    def start1(self):
        me = lax.axis_index("dp")
        for j in range(1, self.pn.ndp):
            self.c1(j).start()
        self.r1[me] = self.own[...]

    def c2(self, j):
        z = lax.axis_index("opt")
        to = lax.rem(z + j, self.pn.ns)
        return to, remote(self.mid, self.r2.at[z], self.sems, self.pn.ndp - 2 + j, {"opt": to})

    def w2(self, j):
        z = lax.axis_index("opt")
        return remote(self.mid, self.r2.at[lax.rem(z - j + self.pn.ns, self.pn.ns)], self.sems, self.pn.ndp - 2 + j, {"opt": lax.rem(z + j, self.pn.ns)})

    def start2(self):
        z = lax.axis_index("opt")
        for j in range(1, self.pn.ndp):
            self.c1(j).wait_send()
            self.w1(j).wait_recv()
        v = self.r1[0].astype(F32)
        for n in range(1, self.pn.ndp):
            v = v + self.r1[n].astype(F32)
        self.mid[...] = v.astype(BF16)
        for j in range(1, self.pn.ns):
            to, cp = self.c2(j)

            @pl.when(to <= self.pn.ka)
            def _():
                cp.start()
        self.r2[z] = v.astype(BF16)

    def finish(self):
        z = lax.axis_index("opt")
        for j in range(1, self.pn.ns):
            to, cp = self.c2(j)

            @pl.when(to <= self.pn.ka)
            def _():
                cp.wait_send()

            @pl.when(z <= self.pn.ka)
            def _():
                self.w2(j).wait_recv()

    def total(self, n):
        v = self.r2[0, n].astype(F32)
        for k in range(1, self.pn.ns):
            v = v + self.r2[k, n].astype(F32)
        return v.astype(BF16).astype(F32)


BM = 784
NSEMS = 32


def put_rows_grad(fs, start, v):
    put_rows(fs, start, v)


def kernel_bc(pn, x_hbm, cot_hbm, ob_hbm, wp_hbm, w1_hbm, w2_hbm, hwt_hbm, qkv_hbm, p_hbm, wqkv_hbm, vec, rel_ref, counts,
              y_hbm, dx_hbm, g_hbm, *refs):
    refs = list(refs)
    dx1, wp, acc, dsem = refs[:4]
    refs = refs[4:]
    chunks = []
    for n, (k0, k1, scatter, m) in enumerate(part_list(pn)):
        if n == 1:
            refs.insert(5, chunks[0].ag)
        chunks.append(Chunk(pn, k0, k1, scatter, m, *refs[:6]))
        refs = refs[6:]
    hi, lo = chunks[:2]
    ac = chunks[2:]
    small = Small(pn, *refs)
    count = counts[0]

    def local(n, src, dst):
        return pltpu.make_async_copy(src, dst, dsem.at[n])

    def mlp(x_v, dy_v, ob, a, du, h2, w1, w2, fs, xsem, csem):
        ins = [local(n, s, d) for n, (s, d) in enumerate([(ob_hbm, ob), (wp_hbm, wp), (w1_hbm, w1), (w2_hbm, w2)])]
        cps = window_copies(x_hbm, x_v, xsem, True) + window_copies(cot_hbm, dy_v, csem, True)
        for cp in cps + ins:
            cp.start()
        acc[...] = jnp.zeros_like(acc)
        bp, g2, b2, c2 = (vec[n:n + 1, :] for n in range(4, 8))
        enter(pn, True)
        for cp in cps + ins:
            cp.wait()
        nb = BM // 56

        def rows(t, _):
            r0 = pl.multiple_of(t * BM, BM)
            x = x_v[pl.ds(nb * t, nb)].reshape(BM, D).astype(F32)
            alive = lax.broadcasted_iota(jnp.int32, (nb, 7, 8, D), 2) < count
            dy = jnp.where(alive, dy_v[pl.ds(nb * t, nb)].astype(F32), 0.0)
            dyb = dy.astype(BF16)
            dy_v[pl.ds(nb * t, nb)] = dyb
            dy = dy.reshape(BM, D)
            dyb = dyb.reshape(BM, D)
            x1 = x + dot(ob[pl.ds(r0, BM), :], wp[...]) + bp
            xhat, r = norm_stats(x1)
            h = (xhat * g2 + b2).astype(BF16)
            h2[pl.ds(r0, BM), :] = h
            y = x1 + c2
            dh = jnp.zeros((BM, D), F32)
            for j in range(HID // CH):
                cs = slice(j * CH, (j + 1) * CH)
                u = dot(h, w1[:, cs]) + vec[8 + j:9 + j, :]
                cdf, pdf = gelu_parts(u)
                av = (u * cdf).astype(BF16)
                a[pl.ds(r0, BM), cs] = av
                y = y + dot(av, w2[cs, :])
                da = dot_nt(dyb, w2[cs, :])
                duv = da * (cdf + u * pdf)
                acc_rows(acc, 4 + j, duv)
                dub = duv.astype(BF16)
                du[pl.ds(r0, BM), cs] = dub
                dh = dh + dot_nt(dub, w1[:, cs])
            x_v[pl.ds(nb * t, nb)] = y.reshape(nb, 7, 8, D).astype(BF16)
            acc_rows(acc, 0, dy)
            acc_rows(acc, 1, dh * xhat)
            acc_rows(acc, 2, dh)
            dg = dh * g2
            dt = r * (dg - jnp.mean(dg, -1, keepdims=True) - xhat * jnp.mean(dg * xhat, -1, keepdims=True))
            dxv = dy + dt
            acc_rows(acc, 3, dxv)
            dx1[pl.ds(nb * t, nb)] = dxv.reshape(nb, 7, 8, D)
            return 0
        lax.fori_loop(0, ROWS // BM, rows, 0)
        ycs = window_copies(y_hbm, x_v, xsem, False)
        for cp in ycs:
            cp.start()
        vg = jnp.sum(acc[...].reshape(8, 8, D), 1)
        first = pn.base * 8
        nrow = pn.bunits * 8
        lo_row = (R_PROJ // 8 + 1) * 8 - first
        hi_row = R_END // 8 * 8 - first
        fs[0:lo_row, :] = jnp.zeros((lo_row, 128), F32)
        fs[hi_row:nrow, :] = jnp.zeros((nrow - hi_row, 128), F32)
        dyf = dy_v[...].reshape(ROWS, D)

        def w2rows(t, _):
            r0 = pl.multiple_of(t * 512, 512)
            v = dot_tn(a[:, pl.ds(r0, 512)], dyf)
            for c in range(4):
                put_block(fs, R_W2 - first + r0 * 4 + c, 4, v[:, c * 128:(c + 1) * 128])
            return 0
        lax.fori_loop(0, HID // 512, w2rows, 0)
        put_vec(fs, R_C2 - first, vg[0:1])

        def fill(ch):
            for k in range(ch.k0, ch.k1):
                def piece(p, _):
                    row = pl.multiple_of(((k - pn.ka) * pn.units + p * pn.pc) * 8, 8)
                    ch.src[p & 1, lax.shift_right_arithmetic(p, 1), (k - ch.k0) * pn.pc:(k - ch.k0 + 1) * pn.pc] = fs[pl.ds(row, pn.pc * 8), :].reshape(pn.pc, 8, 128).astype(BF16)
                    return 0
                lax.fori_loop(0, pn.ndp, piece, 0)
        fill(hi)
        hi.start1()
        h2t = a.at[0:D, 0:1664]
        transpose_rows(h2, h2t)

        def w1rows(t, _):
            r0 = pl.multiple_of(t * 256, 256)
            v = dot(h2t[:, 0:ROWS], du[:, pl.ds(r0, 256)])
            for c in range(2):
                put_block(fs, R_W1 - first + 2 * t + c, 16, v[:, c * 128:(c + 1) * 128])
            return 0
        lax.fori_loop(0, HID // 256, w1rows, 0)
        hi.start2()
        v = dot_tn(ob[...], dx1[...].reshape(ROWS, D).astype(BF16))
        for c in range(4):
            put_block(fs, R_PROJ - first + c, 4, v[:, c * 128:(c + 1) * 128])
        for row, n in ((R_BP, 3), (R_G2, 1), (R_B2, 2)):
            put_vec(fs, row - first, vg[n:n + 1])
        for j in range(4):
            put_vec(fs, R_C1 - first + 4 * j, vg[4 + j:5 + j])
        fill(lo)
        lo.start1()
        for cp in ycs:
            cp.wait()

    big = pltpu.VMEM((28, 7, 8, D), BF16)
    pl.run_scoped(mlp, big, big, pltpu.VMEM((ROWS, D), BF16), pltpu.VMEM((ROWS, HID), BF16), pltpu.VMEM((ROWS, HID), BF16), pltpu.VMEM((ROWS, D), BF16),
                  pltpu.VMEM((D, HID), BF16), pltpu.VMEM((HID, D), BF16), pltpu.VMEM((pn.bunits * 8, 128), F32),
                  pltpu.SemaphoreType.DMA((NSEG,)), pltpu.SemaphoreType.DMA((NSEG,)))

    def attention(x_v, qkvb, pb, hwt, wqkv, fs, os_, dq, dtab, xsem):
        ins = [local(n, s, d) for n, (s, d) in enumerate([(qkv_hbm, qkvb), (p_hbm, pb), (hwt_hbm, hwt), (wqkv_hbm, wqkv)])]
        for cp in ins:
            cp.start()
        cps = window_copies(x_hbm, x_v, xsem, True)
        for cp in cps:
            cp.start()
        acc[...] = jnp.zeros_like(acc)
        dtab[...] = jnp.zeros_like(dtab)

        def rows0(t, _):
            r0 = pl.multiple_of(t * 392, 8)
            ev = dx1[pl.ds(7 * t, 7)].reshape(392, D).astype(BF16)
            v = dot_nt(ev, wp[...])
            for g in range(4):
                os_[pl.ds(g * RS + r0, 392), :] = v[:, g * 128:(g + 1) * 128]
            return 0
        lax.fori_loop(0, 4, rows0, 0)
        ins[0].wait()
        ins[1].wait()
        lo.start2()
        heads = lane_head()

        def one(g, i):
            base = lax.shift_right_arithmetic(i, 3) * WROWS + (i & 7)
            do = take_rows(os_, g * RS + base).astype(BF16)
            q = qkvb[i, g]
            k = qkvb[i, 4 + g]
            v = qkvb[i, 8 + g]
            pbv = pb[i, g]
            p = pbv.astype(F32)
            dobd = block_diag(do, heads)
            dp = dot_nt(v, dobd)
            t = p * dp
            ds = t - p * jnp.sum(t, 0, keepdims=True)
            dsb = ds.astype(BF16)
            put_rows(fs, 2 * RS + base, dot(pbv, dobd))
            put_rows(fs, RS + base, dot(dsb, block_diag(q, heads)))
            put_rows(fs, base, diag_sum(dot_tn(dsb, k), heads) * SCALE)
            return ds

        mid = {0: (hi.start3,), 1: (ac[0].start2, hi.start4), 2: (hi.start5, ac[1].start2, ac[0].start3), 3: (ac[2].start2, ac[1].start3, ac[0].start4)}
        end = {0: (), 1: (lo.start3,), 2: (lo.start4,), 3: (lo.start5,)}
        for g in range(4):
            def attend(t, _):
                @pl.when(t == 4)
                def _():
                    for f in mid[g]:
                        f()
                total = dtab[g]
                for n in range(4):
                    total = total + one(g, 4 * t + n)
                dtab[g] = total
                return 0
            lax.fori_loop(0, WB // 4, attend, 0)
            for f in end[g]:
                f()
            parts = []
            for n in range(3):
                v = fs[n * RS:n * RS + ROWS, :]
                if n != 1:
                    acc[8 * (2 + n // 2):8 * (3 + n // 2), g * 128:(g + 1) * 128] = jnp.sum(v.reshape(ROWS // 8, 8, 128), 0)
                v = v.astype(BF16)
                dq[:, n * D + g * 128:n * D + (g + 1) * 128] = v
                parts.append(v)
            if g == 0:
                ins[2].wait()
                ins[3].wait()
            v = dot(hwt[...], jnp.concatenate(parts, 1))
            mu = pn.mrow // 8
            for n in range(3):
                u = v[:, n * 128:(n + 1) * 128].reshape(D // 8, 8, 128).astype(BF16)
                for p in range(pn.ndp):
                    ac[g].src[p & 1, p >> 1, n * mu:(n + 1) * mu] = u[p * mu:(p + 1) * mu]
            ac[g].start1()
        for cp in cps:
            cp.wait()
        gain = vec[0:1, :]
        tab = table_grad(rel_ref, os_, dtab)
        for n in range(3):
            small.own[2 + n] = tab[8 * n:8 * n + 8].astype(BF16)
        late = {1: (ac[3].start2, ac[2].start3, ac[1].start4, ac[0].start5), 3: (ac[3].start3, ac[2].start4, ac[1].start5), 5: (ac[3].start4, ac[2].start5)}

        def rows1(t, _):
            for k, fns in late.items():
                @pl.when(t == k)
                def _():
                    for f in fns:
                        f()
            r0 = pl.multiple_of(t * BLK, BLK)
            dn = dot_nt(dq[pl.ds(r0, BLK), :], wqkv[...])
            x = x_v[pl.ds(4 * t, 4)].reshape(BLK, D).astype(F32)
            xhat, r = norm_stats(x)
            acc_rows(acc, 0, dn * xhat)
            acc_rows(acc, 1, dn)
            dg = dn * gain
            dt = r * (dg - jnp.mean(dg, -1, keepdims=True) - xhat * jnp.mean(dg * xhat, -1, keepdims=True))
            dx1[pl.ds(4 * t, 4)] += dt.reshape(4, 7, 8, D)
            return 0
        lax.fori_loop(0, NBLK, rows1, 0)
        vg = jnp.sum(acc[...].reshape(8, 8, D), 1)
        flat = [vg[n:n + 1, c * 128:(c + 1) * 128] for n in range(4) for c in range(4)]
        small.own[0] = jnp.concatenate(flat[:8], 0).astype(BF16)
        small.own[1] = jnp.concatenate(flat[8:], 0).astype(BF16)
        small.start1()
        ycs = window_copies(dx_hbm, dx1, xsem, False)
        for cp in ycs:
            cp.start()
        ac[3].start5()
        for ch in chunks:
            ch.finish()
        small.start2()
        r, c, z = place()
        g = os_

        def scattered(ch):
            @pl.when(ch.here(z))
            def _():
                def piece(p, _):
                    g[pl.ds(pl.multiple_of(p * pn.pc * 8, 8), pn.pc * 8), :] = ch.ag[p & 1, lax.shift_right_arithmetic(p, 1)].astype(F32).reshape(pn.pc * 8, 128)
                    return 0
                lax.fori_loop(0, pn.ndp, piece, 0)
        scattered(hi)
        scattered(lo)
        mu = pn.mrow // 8

        @pl.when(z < pn.ka)
        def _():
            def piece(p, _):
                for h in range(4):
                    for n in range(3):
                        v = ac[h].ag[p & 1, lax.shift_right_arithmetic(p, 1), n * mu:(n + 1) * mu].astype(F32).reshape(pn.mrow, 128)
                        g[pl.ds(R_QKV + p * pn.mrow * 12 + n * 4 + h, pn.mrow, stride=12), :] = v
                return 0
            lax.fori_loop(0, pn.ndp, piece, 0)
        small.finish()

        @pl.when(z < pn.ka)
        def _():
            for n, u in enumerate(SMALL):
                g[u * 8:u * 8 + 8, :] = small.total(n)

        @pl.when(z == pn.ka)
        def _():
            for n, u in enumerate(SMALL):
                if u >= pn.base:
                    k = (u - pn.base) * 8
                    g[k:k + 8, :] += small.total(n)
        out = local(0, g.at[pl.ds(pl.multiple_of(lax.select(z < pn.ka, z * (pn.units * 8), 0), 8), pn.units * 8)], g_hbm)
        out.start()
        out.wait()
        for cp in ycs:
            cp.wait()

    pl.run_scoped(attention, big, pltpu.VMEM((WB, 12, 64, 128), BF16), pltpu.VMEM((WB, 4, 64, 256), BF16), pltpu.VMEM((D, ROWS), BF16), pltpu.VMEM((D, 3 * D), BF16),
                  pltpu.VMEM((3 * RS, 128), F32), pltpu.VMEM((max(4 * RS, pn.gunits * 8), 128), F32), pltpu.VMEM((ROWS, 3 * D), BF16), pltpu.VMEM((4, 64, 256), F32), pltpu.SemaphoreType.DMA((NSEG,)))


def part_list(pn):
    mu = 3 * pn.mrow // 8
    return [(pn.kh, pn.ns, True, pn.pc), (pn.ka, pn.kh, True, pn.pc)] + [(0, pn.ka, False, mu)] * 4


def call_bc(pn, x, cot, ob, wp, w1, w2, hwt, qkv, p, wqkv, vec, rel, counts):
    any_ = pl.BlockSpec(memory_space=pl.ANY)
    vm = pl.BlockSpec(memory_space=pltpu.VMEM)
    sds = jax.ShapeDtypeStruct
    outs = [sds((14, 14, 8, D), BF16), sds((14, 14, 8, D), F32), sds((pn.units * 8, 128), F32)]
    scratch = [pltpu.VMEM((28, 7, 8, D), F32), pltpu.VMEM((D, D), BF16), pltpu.VMEM((64, D), F32), pltpu.SemaphoreType.DMA((4,))]
    for n, (k0, k1, scatter, m) in enumerate(part_list(pn)):
        scratch += Chunk.scratch(pn, m, k1 - k0 if scatter else 1, n == 1)
    scratch += Small.scratch(pn)
    return pl.pallas_call(
        functools.partial(kernel_bc, pn),
        out_shape=outs,
        in_specs=[any_] * 10 + [vm, vm, pl.BlockSpec(memory_space=pltpu.SMEM)],
        out_specs=[any_] * 3,
        scratch_shapes=scratch,
        compiler_params=pltpu.CompilerParams(vmem_limit_bytes=67000000, collective_id=1, has_side_effects=True),
        name="back",
    )(x, cot, ob, wp, w1, w2, hwt, qkv, p, wqkv, vec, rel, counts)


STEP = 2
DECAYED = (2, 6, 10, 12)
LENGTHS = [D, D, 3 * D * D, D, D, TAB * HEADS, D * D, D, D, D, D * HID, HID, HID * D, D]
AU = 64


def kernel_adam(rates, first, g, p, m1, m2, g_o, p_o, m_o, v_o):
    shape = (AU, 8, 128)
    u0 = first[0] + pl.program_id(0) * AU
    index = ((u0 + lax.broadcasted_iota(jnp.int32, shape, 0)) * 8 + lax.broadcasted_iota(jnp.int32, shape, 1)) * 128 + lax.broadcasted_iota(jnp.int32, shape, 2)
    rate = jnp.zeros(shape, F32) + rates[0]
    decay = jnp.zeros(shape, F32)
    at = 0
    for n, length in enumerate(LENGTHS):
        at += length
        after = index >= at
        rate = jnp.where(after, rates[n + 1], rate)
        if n in DECAYED or n + 1 in DECAYED:
            decay = jnp.where(after, 0.05 if n + 1 in DECAYED else 0.0, decay)
    grad = g[...]
    w = p[...]
    m = 0.9 * m1[...] + 0.1 * grad
    v = 0.999 * m2[...] + 0.001 * grad * grad
    mh = m / (1.0 - 0.9 ** STEP)
    vh = v / (1.0 - 0.999 ** STEP)
    p_o[...] = w - rate * (mh / (jnp.sqrt(vh) + 1e-08) + decay * w)
    m_o[...] = m
    v_o[...] = v
    g_o[...] = grad


def call_adam(pn, rates, g, params, mom1, mom2):
    view = lambda t: t.reshape(pn.units, 8, 128)
    spec = pl.BlockSpec((AU, 8, 128), lambda i: (i, 0, 0))
    sm = pl.BlockSpec(memory_space=pltpu.SMEM)
    first = (lax.axis_index("opt") * pn.units).astype(jnp.int32).reshape(1)
    out = pl.pallas_call(
        kernel_adam,
        grid=(pl.cdiv(pn.units, AU),),
        out_shape=[jax.ShapeDtypeStruct((pn.units, 8, 128), F32)] * 4,
        in_specs=[sm, sm] + [spec] * 4,
        out_specs=[spec] * 4,
        compiler_params=pltpu.CompilerParams(vmem_limit_bytes=67043328),
        name="adamw",
    )(rates, first, view(g), view(params), view(mom1), view(mom2))
    return [t.reshape(-1) for t in out]


def kernel_g(pn, params, w_o, p_v, wb, sems, isem, osem):
    r, c, z = place()
    cp = pltpu.make_async_copy(params, p_v.at[pl.ds(0, pn.units)], isem)
    cp.start()
    enter(pn)
    cp.wait()

    def cast(p, _):
        wb[z, p & 1, lax.shift_right_arithmetic(p, 1)] = p_v[pl.ds(p * pn.pc, pn.pc)].astype(BF16)
        return 0
    lax.fori_loop(0, pn.ndp, cast, 0)

    def o(j):
        to = lax.rem(z + j, pn.ns)
        return remote(wb.at[z, c, r], wb.at[z, c, r], sems, j - 1, {"opt": to})

    def x(k, j):
        to = lax.rem(r + j, pn.rest)
        src = lax.rem(z - k + pn.ns, pn.ns)
        return remote(wb.at[src, c, r], wb.at[src, c, r], sems, pn.ns - 1 + (k - 1) * (pn.rest - 1) + j - 1, peer(to, c))

    def y(k):
        src = lax.rem(z - k + pn.ns, pn.ns)
        return remote(wb.at[src, c], wb.at[src, c], sems, (pn.ns - 1) * pn.rest + k - 1, peer(r, 1 - c))

    for j in range(1, pn.ns):
        o(j).start()
    for k in range(1, pn.ns):
        o(k).wait()
        for j in range(1, pn.rest):
            x(k, j).start()
    for k in range(1, pn.ns):
        for j in range(1, pn.rest):
            x(k, j).wait()
        y(k).start()
    for k in range(1, pn.ns):
        y(k).wait()
    cp = pltpu.make_async_copy(wb, w_o, osem)
    cp.start()
    cp.wait()


def call_g(pn, params):
    any_ = pl.BlockSpec(memory_space=pl.ANY)
    shape = (pn.ns, 2, pn.rest, pn.pc, 8, 128)
    nsem = (pn.ns - 1) * (pn.rest + 1)
    return pl.pallas_call(
        functools.partial(kernel_g, pn),
        out_shape=jax.ShapeDtypeStruct(shape, BF16),
        in_specs=[any_],
        out_specs=any_,
        scratch_shapes=[pltpu.VMEM((pn.ndp * pn.pc, 8, 128), F32), pltpu.VMEM(shape, BF16), pltpu.SemaphoreType.DMA((2, nsem)), pltpu.SemaphoreType.DMA, pltpu.SemaphoreType.DMA],
        compiler_params=pltpu.CompilerParams(vmem_limit_bytes=64000000, collective_id=0, has_side_effects=True),
        name="gather",
    )(params.reshape(pn.units, 8, 128))


from jax.sharding import PartitionSpec as P


def solution(mesh):
    def local(images, cotangent, counts, rel_index, params, moment1, moment2, rates):
        pn = Plan(mesh, params.shape[0])
        xt = images.transpose(1, 2, 0, 3)
        ct = cotangent.transpose(1, 2, 0, 3)
        rel = rel_lanes(rel_index)
        flat = call_g(pn, params)
        wqkv, wp, w1, w2, vec, hwt, ob, qkv, p = call_a(pn, xt, flat, rel)
        y, dx, g = call_bc(pn, xt, ct, ob, wp, w1, w2, hwt, qkv, p, wqkv, vec, rel, counts)
        grad, new_params, new_first, new_second = call_adam(pn, rates, g, params, moment1, moment2)
        return (y.transpose(2, 0, 1, 3), dx.transpose(2, 0, 1, 3), grad, new_params, new_first, new_second)

    split = P(("dp", "opt"), None, None, None)
    return jax.shard_map(
        local, mesh=mesh,
        in_specs=(split, split, P(("dp", "opt")), P(), P("opt"), P("opt"), P("opt"), P()),
        out_specs=(split, split, P("opt"), P("opt"), P("opt"), P("opt")),
        check_vma=False)
```

```python
import functools
import jax
import jax.numpy as jnp
from jax import lax
from jax.experimental import pallas as pl
from jax.experimental.pallas import tpu as pltpu

D = 512
HEADS = 16
HEAD_DIM = 32
HID = 2048
SIDE = 14
WIN = 7
SHIFT = 3
TAB = 169
F32 = jnp.float32
BF16 = jnp.bfloat16

IMGS = 8
SPAN = WIN * WIN
WROWS = SPAN * IMGS
ROWS = 4 * WROWS
RS = ROWS + 64
BLK = 224
NBLK = ROWS // BLK
WB = 4 * IMGS
SCALE = HEAD_DIM ** -0.5

R_G1, R_B1, R_QKV, R_BQ, R_BV, R_TAB = 0, 4, 8, 6152, 6156, 6160
R_PROJ, R_BP, R_G2, R_B2, R_W1, R_C1, R_W2, R_C2, R_END = 6181, 8229, 8233, 8237, 8241, 16433, 16449, 24641, 24645
LANE = 16
BROW = 6176


def segments(w):
    if w == 0:
        return [(SHIFT, WIN, 0)]
    return [(WIN + SHIFT, WIN - SHIFT, 0), (0, SHIFT, WIN - SHIFT)]


def window_copies(hbm, vmem, sem, inward):
    out = []
    n = 0
    for wy in range(2):
        for wx in range(2):
            for ys, yl, yo in segments(wy):
                for xs, xl, xo in segments(wx):
                    a = hbm.at[pl.ds(ys, yl), pl.ds(xs, xl)]
                    b = vmem.at[pl.ds((2 * wy + wx) * WIN + yo, yl), pl.ds(xo, xl)]
                    out.append(pltpu.make_async_copy(a, b, sem.at[n]) if inward else pltpu.make_async_copy(b, a, sem.at[n]))
                    n += 1
    return out


NSEG = 9


def dot(a, b):
    return lax.dot_general(a, b, (((1,), (0,)), ((), ())), preferred_element_type=F32)


def dot_nt(a, b):
    return lax.dot_general(a, b, (((1,), (1,)), ((), ())), preferred_element_type=F32)


def dot_tn(a, b):
    return lax.dot_general(a, b, (((0,), (0,)), ((), ())), preferred_element_type=F32)


def norm_stats(x):
    mean = jnp.mean(x, -1, keepdims=True)
    dev = x - mean
    var = jnp.mean(dev * dev, -1, keepdims=True)
    r = lax.rsqrt(var + 1e-05)
    return dev * r, r


def pieces_to_rows(pn, wb, fs, shard, count, base):
    def body(p, _):
        row = pl.multiple_of((shard * pn.units - base + p * pn.pc) * 8, 8)
        fs[pl.ds(row, pn.pc * 8), :] = wb[shard, p & 1, lax.shift_right_arithmetic(p, 1)].astype(F32).reshape(pn.pc * 8, 128)
        return 0
    lax.fori_loop(0, count, body, 0)


def vec_from(fs, row, width, shift):
    parts = []
    lane = lax.broadcasted_iota(jnp.int32, (1, 128), 1)
    for c in range(width // 128):
        a = fs[pl.ds(row + c, 1), :]
        if shift:
            b = fs[pl.ds(row + c + 1, 1), :]
            a = jnp.where(lane < 128 - LANE, pltpu.roll(a, 128 - LANE, 1), pltpu.roll(b, 128 - LANE, 1))
        parts.append(a)
    return jnp.concatenate(parts, 1)


def take_matrix(fs, row, dst, nrows, ncb, shift, step=128):
    lane = lax.broadcasted_iota(jnp.int32, (step, 128), 1)

    def body(t, _):
        base = row + t * (step * ncb)
        r0 = pl.multiple_of(t * step, step)
        for c in range(ncb):
            a = fs[pl.ds(base + c, step, stride=ncb), :]
            if shift:
                b = fs[pl.ds(base + c + 1, step, stride=ncb), :]
                a = jnp.where(lane < 128 - LANE, pltpu.roll(a, 128 - LANE, 1), pltpu.roll(b, 128 - LANE, 1))
            dst[pl.ds(r0, step), c * 128:(c + 1) * 128] = a.astype(BF16)
        return 0

    lax.fori_loop(0, nrows // step, body, 0)


def transpose_rows(src, dst):
    full = ROWS // 128

    def body(t, _):
        r0 = pl.multiple_of(t * 128, 128)
        dst[:, pl.ds(r0, 128)] = src[pl.ds(r0, 128), :].T
        return 0
    lax.fori_loop(0, full, body, 0)
    if ROWS % 128:
        dst[:, full * 128:ROWS] = src[full * 128:ROWS, :].T


def lane_head():
    return lax.broadcasted_iota(jnp.int32, (64, 128), 1) // HEAD_DIM


def block_diag(v, heads):
    zero = jnp.zeros_like(v)
    return jnp.concatenate([jnp.where(heads == h, v, zero) for h in range(4)], 0)


def diag_sum(r, heads):
    out = r[0:64]
    for h in range(1, 4):
        out = jnp.where(heads == h, r[64 * h:64 * h + 64], out)
    return out


def take_rows(fs, start):
    v = fs[pl.ds(start, 56, stride=IMGS), :]
    v = jnp.where(lax.broadcasted_iota(jnp.int32, (56, 128), 0) < SPAN, v, 0.0)
    return jnp.concatenate([v, jnp.zeros((8, 128), F32)], 0)


def put_rows(fs, start, v):
    fs[pl.ds(start, 48, stride=IMGS), :] = v[0:48]
    fs[pl.ds(start + 48 * IMGS, 1), :] = v[48:49]


def build_bias(tab3, rel_ref, big, bias):
    rel = rel_ref[...]
    row = lax.shift_right_arithmetic(rel, 3)
    low = rel & 7
    oh = (lax.broadcasted_iota(jnp.int32, (32, 4096), 0) == row).astype(F32).astype(BF16)
    tab = jnp.concatenate([tab3, jnp.zeros((8, 128), F32)], 0).astype(BF16)
    r = dot_tn(tab, oh)
    acc = jnp.zeros((16, 4096), F32)
    for j in range(8):
        acc = acc + jnp.where(low == j, r[16 * j:16 * j + 16], 0.0)
    for kk in range(32):
        big[kk * 16:kk * 16 + 16, :] = acc[:, kk * 128:kk * 128 + 128]
    k = lax.broadcasted_iota(jnp.int32, (64, 256), 0)
    q = lax.broadcasted_iota(jnp.int32, (64, 256), 1) & 63
    ki = lax.shift_right_arithmetic(k * 37, 8)
    kj = k - ki * 7
    qi = lax.shift_right_arithmetic(q * 37, 8)
    qj = q - qi * 7
    cut = WIN - SHIFT
    same_y = (ki < cut) == (qi < cut)
    same_x = (kj < cut) == (qj < cut)
    lane = lax.broadcasted_iota(jnp.int32, (32, 128), 1)
    for g in range(4):
        for pair in range(2):
            h = 4 * g + 2 * pair
            a = big[pl.ds(h, 32, stride=16), :]
            b = big[pl.ds(h + 1, 32, stride=16), :]
            even = jnp.where(lane < 64, a, pltpu.roll(b, 64, 1))
            odd = jnp.where(lane < 64, pltpu.roll(a, 64, 1), b)
            big[pl.ds(1024 + g * 256 + pair * 128, 32, stride=2), :] = even
            big[pl.ds(1024 + g * 256 + pair * 128 + 1, 32, stride=2), :] = odd
    for g in range(4):
        pos = jnp.concatenate([big[1024 + g * 256:1024 + g * 256 + 64, :], big[1024 + g * 256 + 128:1024 + g * 256 + 192, :]], 1)
        for w in range(4):
            keep = None
            if w == 1:
                keep = same_x
            elif w == 2:
                keep = same_y
            elif w == 3:
                keep = same_y & same_x
            val = pos if keep is None else pos + jnp.where(keep, 0.0, -100.0)
            bias[w * 4 + g] = jnp.where(k < SPAN, val, -1e30)


MESH = pl.DeviceIdType.MESH
NMAT = 768


class Plan:
    def __init__(self, mesh, shard_len):
        self.ndp = mesh.shape["dp"]
        self.ns = mesh.shape["opt"]
        self.rest = self.ndp // 2
        self.units = shard_len // 1024
        self.pc = -(-self.units // self.ndp)
        self.ka = (BROW // 8) // self.units
        self.base = self.ka * self.units
        self.bunits = (self.ns - self.ka - 1) * self.units + self.ndp * self.pc
        self.kh = -(-(R_W2 // 8 + 1) // self.units)
        self.mrow = D // self.ndp
        self.gunits = max(BROW // 8 + 1, self.ndp * self.pc)


def place():
    me = lax.axis_index("dp")
    return lax.shift_right_arithmetic(me, 1), me & 1, lax.axis_index("opt")


def peer(r, c):
    return {"dp": 2 * r + c}


def enter(pn, all_dp=False):
    r, c, z = place()
    bar = pltpu.get_barrier_semaphore()
    pl.semaphore_signal(bar, inc=1, device_id=peer(r, 1 - c), device_id_type=MESH)
    for j in range(1, pn.rest):
        for to in ((c, 1 - c) if all_dp else (c,)):
            pl.semaphore_signal(bar, inc=1, device_id=peer(lax.rem(r + j, pn.rest), to), device_id_type=MESH)
    for j in range(1, pn.ns):
        pl.semaphore_signal(bar, inc=1, device_id={"opt": lax.rem(z + j, pn.ns)}, device_id_type=MESH)
    pl.semaphore_wait(bar, (pn.ndp - 1 if all_dp else pn.rest) + pn.ns - 1)


def remote(src, dst, sems, n, where):
    return pltpu.make_async_remote_copy(src_ref=src, dst_ref=dst, send_sem=sems.at[0, n], recv_sem=sems.at[1, n], device_id=where, device_id_type=MESH)


class Gather:
    def __init__(self, pn, wb, osend, orecv, xsem, ysem):
        self.pn, self.wb, self.osend, self.orecv, self.xsem, self.ysem = pn, wb, osend, orecv, xsem, ysem

    @staticmethod
    def scratch(pn):
        return [pltpu.VMEM((pn.ns, 2, pn.rest, pn.pc, 8, 128), BF16), pltpu.SemaphoreType.DMA((pn.ns,)), pltpu.SemaphoreType.DMA((pn.ns,)),
                pltpu.SemaphoreType.DMA((2, pn.ns * pn.rest)), pltpu.SemaphoreType.DMA((2, pn.ns))]

    def o(self, j):
        r, c, z = place()
        own = self.wb.at[z, c, r]
        return pltpu.make_async_remote_copy(src_ref=own, dst_ref=own, send_sem=self.osend.at[j], recv_sem=self.orecv.at[z],
                                            device_id={"opt": lax.rem(z + j, self.pn.ns)}, device_id_type=MESH)

    def arrived(self, s):
        r, c, z = place()
        own = self.wb.at[s, c, r]
        return pltpu.make_async_remote_copy(src_ref=own, dst_ref=own, send_sem=self.osend.at[0], recv_sem=self.orecv.at[s],
                                            device_id={"opt": lax.rem(z + 1, self.pn.ns)}, device_id_type=MESH)

    def x(self, s, j):
        r, c, z = place()
        own = self.wb.at[s, c, r]
        return remote(own, own, self.xsem, s * self.pn.rest + j, peer(lax.rem(r + j, self.pn.rest), c))

    def y(self, s):
        r, c, z = place()
        return remote(self.wb.at[s, c], self.wb.at[s, c], self.ysem, s, peer(r, 1 - c))

    def start(self):
        for j in range(1, self.pn.ns):
            self.o(j).start()

    def spread(self, s):
        r, c, z = place()

        @pl.when(z != s)
        def _():
            self.arrived(s).wait_recv()
            for j in range(1, self.pn.rest):
                self.x(s, j).start()

    def pair(self, s):
        r, c, z = place()

        @pl.when(z != s)
        def _():
            for j in range(1, self.pn.rest):
                self.x(s, j).wait_recv()
            self.y(s).start()

    def ready(self, s):
        r, c, z = place()

        @pl.when(z != s)
        def _():
            self.y(s).wait_recv()

    def finish(self):
        r, c, z = place()
        for j in range(1, self.pn.ns):
            self.o(j).wait_send()
        for s in range(self.pn.ns):
            @pl.when(z != s)
            def _():
                for j in range(1, self.pn.rest):
                    self.x(s, j).wait_send()
                self.y(s).wait_send()


def kernel_a(pn, x_hbm, params, rel_ref,
             wqkv_o, wp_o, w1_o, w2_o, vec_o, hw_o, ob_o, qkv_o, p_o,
             x_v, fs, os_, bias, wqkv, wp, w1, w2, vec, hw, hwt, ob, qkvb, pb, xsem, fsem, osem, wsem, flat_v, *gsems):
    cps = window_copies(x_hbm, x_v, xsem, True)
    for c in cps:
        c.start()
    r, c, z = place()
    gather = Gather(pn, flat_v, *gsems)
    fcp = pltpu.make_async_copy(params, fs.at[pl.ds(0, pn.units * 8)], fsem)
    fcp.start()
    enter(pn)
    fcp.wait()

    def cast(p):
        flat_v[z, p & 1, lax.shift_right_arithmetic(p, 1)] = fs[pl.ds(pl.multiple_of(p * pn.pc * 8, 8), pn.pc * 8), :].reshape(pn.pc, 8, 128).astype(BF16)
    me = lax.axis_index("dp")
    cast(me)
    gather.start()

    def others(j, _):
        cast(lax.rem(me + j, pn.ndp))
        return 0
    lax.fori_loop(1, pn.ndp, others, 0)
    for k in range(pn.ka + 1):
        gather.spread(k)
    for k in range(pn.ka):
        gather.pair(k)
    for k in range(pn.ka):
        gather.ready(k)
    for k in range(pn.ka):
        pieces_to_rows(pn, flat_v, fs, k, pn.ndp, 0)
    take_matrix(fs, R_QKV, wqkv, D, 12, False)
    vec[0:1, :] = vec_from(fs, R_G1, D, False)
    vec[1:2, :] = vec_from(fs, R_B1, D, False)
    vec[2:3, :] = vec_from(fs, R_BQ, D, False)
    vec[3:4, :] = vec_from(fs, R_BV, D, False)
    wos = [pltpu.make_async_copy(wqkv, wqkv_o, wsem.at[0])]
    wos[0].start()
    for cp in cps:
        cp.wait()
    gain = vec[0:1, :]
    shift = vec[1:2, :]
    bq = vec[2:3, :]
    bv = vec[3:4, :]

    def rows(t, _):
        @pl.when(t == 2)
        def _():
            gather.pair(pn.ka)
            for k in range(pn.ka + 1, pn.ns):
                gather.spread(k)
        r0 = pl.multiple_of(t * BLK, BLK)
        x = x_v[pl.ds(4 * t, 4)].reshape(BLK, D).astype(F32)
        xhat, _r = norm_stats(x)
        h = (xhat * gain + shift).astype(BF16)
        hw[pl.ds(r0, BLK), :] = h
        for c in range(12):
            y = dot(h, wqkv[:, c * 128:(c + 1) * 128])
            if c < 4:
                y = (y + bq[:, c * 128:(c + 1) * 128]) * SCALE
            if c >= 8:
                y = y + bv[:, (c - 8) * 128:(c - 7) * 128]
            fs[pl.ds(c * RS + r0, BLK), :] = y
        return 0
    lax.fori_loop(0, NBLK, rows, 0)
    gather.ready(pn.ka)
    tab = []
    for u in range(R_TAB // 8, R_TAB // 8 + 3):
        k, at = (pn.ka, u - pn.base) if u >= pn.base else (pn.ka - 1, u - pn.base + pn.units)
        p = at // pn.pc
        tab.append(flat_v[k, p & 1, p >> 1, at - p * pn.pc].astype(F32))
    build_bias(jnp.concatenate(tab, 0), rel_ref, os_, bias)
    heads = lane_head()

    def saved(t):
        four = pl.ds(4 * t, 4)
        return [pltpu.make_async_copy(qkvb.at[four], qkv_o.at[four], osem.at[2 + t]), pltpu.make_async_copy(pb.at[four], p_o.at[four], osem.at[2 + WB // 4 + t])]

    def attend(t, _):
        un = 4
        items = [(un * t + n, g) for n in range(un) for g in range(4)]
        ss = []
        vs = []
        for i, g in items:
            w = lax.shift_right_arithmetic(i, 3)
            base = w * WROWS + (i & 7)
            q = take_rows(fs, g * RS + base).astype(BF16)
            k = take_rows(fs, (4 + g) * RS + base).astype(BF16)
            v = take_rows(fs, (8 + g) * RS + base).astype(BF16)
            qkvb[i, g] = q
            qkvb[i, 4 + g] = k
            qkvb[i, 8 + g] = v
            vs.append(v)
            ss.append(dot_nt(k, block_diag(q, heads)) + bias[w * 4 + g])
        ps = []
        for (i, g), s in zip(items, ss):
            m = jnp.max(s, 0, keepdims=True)
            e = jnp.exp(s - m)
            p = (e * (1.0 / jnp.sum(e, 0, keepdims=True))).astype(BF16)
            pb[i, g] = p
            ps.append(p)
        for (i, g), p, v in zip(items, ps, vs):
            w = lax.shift_right_arithmetic(i, 3)
            base = w * WROWS + (i & 7)
            o = diag_sum(dot_tn(p, v), heads)
            put_rows(os_, g * RS + base, o)
        for cp in saved(t):
            cp.start()

        @pl.when(t == 2)
        def _():
            for k in range(pn.ka + 1, pn.ns):
                gather.pair(k)
        return 0
    lax.fori_loop(0, WB // 4, attend, 0)

    def outs(t, _):
        r0 = pl.multiple_of(t * BLK, BLK)
        for g in range(4):
            ob[pl.ds(r0, BLK), g * 128:(g + 1) * 128] = os_[pl.ds(g * RS + r0, BLK), :].astype(BF16)
        return 0
    lax.fori_loop(0, NBLK, outs, 0)
    transpose_rows(hw, hwt)
    cos = [pltpu.make_async_copy(a, b, osem.at[n]) for n, (a, b) in enumerate([(hwt, hw_o), (ob, ob_o)])]
    for cp in cos:
        cp.start()
    for k in range(pn.ka + 1, pn.ns):
        gather.ready(k)
    for k in range(pn.ka, pn.ns):
        pieces_to_rows(pn, flat_v, fs, k, pn.ndp, pn.base)
    first = pn.base * 8
    take_matrix(fs, R_PROJ - first, wp, D, 4, True)
    take_matrix(fs, R_W1 - first, w1, D, 16, True)
    take_matrix(fs, R_W2 - first, w2, HID, 4, True)
    for n, r in enumerate((R_BP, R_G2, R_B2, R_C2)):
        vec[4 + n:5 + n, :] = vec_from(fs, r - first, D, True)
    for n in range(4):
        vec[8 + n:9 + n, :] = vec_from(fs, R_C1 - first + 4 * n, D, True)
    for n, (a, b) in enumerate([(wp, wp_o), (w1, w1_o), (w2, w2_o), (vec, vec_o)]):
        wos.append(pltpu.make_async_copy(a, b, wsem.at[n + 1]))
        wos[-1].start()
    for t in range(WB // 4):
        cos += saved(t)
    for cp in cos + wos:
        cp.wait()
    gather.finish()


def call_a(pn, x, params, rel):
    any_ = pl.BlockSpec(memory_space=pl.ANY)
    sds = jax.ShapeDtypeStruct
    outs = [sds((D, 3 * D), BF16), sds((D, D), BF16), sds((D, HID), BF16), sds((HID, D), BF16), sds((16, D), F32),
            sds((D, ROWS), BF16), sds((ROWS, D), BF16), sds((WB, 12, 64, 128), BF16), sds((WB, 4, 64, 256), BF16)]
    return pl.pallas_call(
        functools.partial(kernel_a, pn),
        out_shape=outs,
        in_specs=[any_, any_, pl.BlockSpec(memory_space=pltpu.VMEM)],
        out_specs=[any_] * len(outs),
        scratch_shapes=[
            pltpu.VMEM((28, 7, 8, D), BF16), pltpu.VMEM((12 * RS, 128), F32), pltpu.VMEM((4 * RS, 128), F32),
            pltpu.VMEM((16, 64, 256), F32), pltpu.VMEM((D, 3 * D), BF16), pltpu.VMEM((D, D), BF16), pltpu.VMEM((D, HID), BF16), pltpu.VMEM((HID, D), BF16),
            pltpu.VMEM((16, D), F32), pltpu.VMEM((ROWS, D), BF16), pltpu.VMEM((D, ROWS), BF16), pltpu.VMEM((ROWS, D), BF16), pltpu.VMEM((WB, 12, 64, 128), BF16), pltpu.VMEM((WB, 4, 64, 256), BF16),
            pltpu.SemaphoreType.DMA((NSEG,)), pltpu.SemaphoreType.DMA, pltpu.SemaphoreType.DMA((2 + WB // 2,)), pltpu.SemaphoreType.DMA((5,)),
        ] + Gather.scratch(pn),
        compiler_params=pltpu.CompilerParams(vmem_limit_bytes=64000000, collective_id=0, has_side_effects=True),
        name="attend",
    )(x, params.reshape(pn.units * 8, 128), rel)


def rel_lanes(rel_index):
    t = jnp.full((64, 64), -1, jnp.int32).at[:SPAN, :SPAN].set(rel_index.T)
    return t.reshape(1, 4096)


CH = 512
INV_SQRT2 = 0.7071067811865476
INV_SQRT2PI = 0.3989422804014327


def gelu_parts(u):
    e = jnp.exp(u * u * -0.5)
    t = 1.0 / (1.0 + jnp.abs(u) * (0.3275911 * INV_SQRT2))
    half = t * (0.127414796 + t * (-0.142248368 + t * (0.7107068705 + t * (-0.7265760135 + t * 0.5307027145)))) * e
    cdf = jnp.where(u >= 0, 1.0 - half, half)
    return cdf, e * INV_SQRT2PI


def put_block(fs, start, stride, v):
    n = v.shape[0]
    lane = lax.broadcasted_iota(jnp.int32, (n, 128), 1)
    v = pltpu.roll(v, LANE, 1)
    here = pl.ds(start, n, stride=stride) if n > 1 else pl.ds(start, 1)
    fs[here, :] = jnp.where(lane >= LANE, v, fs[here, :])
    here = pl.ds(start + 1, n, stride=stride) if n > 1 else pl.ds(start + 1, 1)
    fs[here, :] = jnp.where(lane < LANE, v, fs[here, :])


def put_vec(fs, row, v):
    for c in range(v.shape[1] // 128):
        put_block(fs, row + c, 1, v[:, c * 128:(c + 1) * 128])


def acc_rows(ref, i, v):
    ref[8 * i:8 * i + 8, 0:v.shape[1]] += jnp.sum(v.reshape(v.shape[0] // 8, 8, v.shape[1]), 0)


def table_grad(rel_ref, big, dtab):
    lane = lax.broadcasted_iota(jnp.int32, (32, 128), 1)
    for g in range(4):
        for pair in range(2):
            at = 1024 + g * 256 + pair * 128
            big[at:at + 64, :] = dtab[g, :, pair * 128:pair * 128 + 128]
    for g in range(4):
        for pair in range(2):
            at = 1024 + g * 256 + pair * 128
            even = big[pl.ds(at, 32, stride=2), :]
            odd = big[pl.ds(at + 1, 32, stride=2), :]
            h = 4 * g + 2 * pair
            big[pl.ds(h, 32, stride=16), :] = jnp.where(lane < 64, even, pltpu.roll(odd, 64, 1))
            big[pl.ds(h + 1, 32, stride=16), :] = jnp.where(lane < 64, pltpu.roll(even, 64, 1), odd)
    rel = rel_ref[...]
    row = lax.shift_right_arithmetic(rel, 3)
    low = rel & 7
    oh = (lax.broadcasted_iota(jnp.int32, (32, 4096), 0) == row).astype(F32).astype(BF16)
    grad = jnp.concatenate([big[kk * 16:kk * 16 + 16, :] for kk in range(32)], 1)
    out = jnp.zeros((32, 128), F32)
    high = grad.astype(BF16).astype(F32)
    for part in (high, grad - high):
        m = jnp.concatenate([jnp.where(low == j, part, 0.0) for j in range(8)], 0).astype(BF16)
        out = out + dot_nt(oh, m)
    return out


class Chunk:
    def __init__(self, pn, k0, k1, scatter, m, src, r1, r2, r3, sems, ag):
        self.pn, self.k0, self.k1, self.scatter, self.m = pn, k0, k1, scatter, m
        self.n = m * (k1 - k0) if scatter else m
        self.src, self.r1, self.r2, self.r3, self.ag, self.sems = src, r1, r2, r3, ag, sems
        self.k2 = 1
        self.k3 = self.k2 + pn.rest - 1
        self.k4 = self.k3 + pn.ns - 1
        self.k5 = self.k4 + pn.rest - 1

    @staticmethod
    def scratch(pn, m, count, shared):
        n = m * count
        return [pltpu.VMEM((2, pn.rest, n, 8, 128), BF16), pltpu.VMEM((pn.rest, n, 8, 128), BF16), pltpu.VMEM((pn.rest - 1, n, 8, 128), BF16),
                pltpu.VMEM((pn.ns - 1, m, 8, 128), BF16),
                pltpu.SemaphoreType.DMA((2, 2 * pn.rest + pn.ns - 1))] + [pltpu.VMEM((2, pn.rest, m, 8, 128), BF16)] * (not shared)

    def here(self, z):
        return (z >= self.k0) & (z < self.k1)

    def c1(self):
        r, c, z = place()
        return remote(self.src.at[1 - c], self.r1, self.sems, 0, peer(r, 1 - c))

    def start1(self):
        self.c1().start()

    def c2(self, j):
        r, c, z = place()
        to = lax.rem(r + j, self.pn.rest)
        return remote(self.src.at[c, to], self.r2.at[j - 1], self.sems, self.k2 + j - 1, peer(to, c))

    def start2(self):
        r, c, z = place()
        self.c1().wait()
        step = self.m
        for j in list(range(1, self.pn.rest)) + [0]:
            to = lax.rem(r + j, self.pn.rest)

            def add(t, _):
                u = pl.ds(t * step, step)
                self.src[c, to, u] = (self.src[c, to, u].astype(F32) + self.r1[to, u].astype(F32)).astype(BF16)
                return 0
            lax.fori_loop(0, self.n // step, add, 0)
            if j:
                self.c2(j).start()

    def c3(self, j):
        r, c, z = place()
        to = lax.rem(z + j, self.pn.ns)
        src = self.src.at[c, r]
        if self.scatter:
            src = src.at[pl.ds(lax.clamp(0, to - self.k0, self.k1 - self.k0 - 1) * self.m, self.m)]
        return to, remote(src, self.r3.at[j - 1], self.sems, self.k3 + j - 1, {"opt": to})

    def start3(self):
        r, c, z = place()
        for j in range(1, self.pn.rest):
            self.c2(j).wait()
        step = self.m

        def add(t, _):
            u = pl.ds(t * step, step)
            v = self.src[c, r, u].astype(F32)
            for j in range(1, self.pn.rest):
                v = v + self.r2[j - 1, u].astype(F32)
            self.src[c, r, u] = v.astype(BF16)
            return 0
        lax.fori_loop(0, self.n // step, add, 0)
        for j in range(1, self.pn.ns):
            to, cp = self.c3(j)

            @pl.when(self.here(to))
            def _():
                cp.start()

    def c4(self, j):
        r, c, z = place()
        return remote(self.ag.at[c, r], self.ag.at[c, r], self.sems, self.k4 + j - 1, peer(lax.rem(r + j, self.pn.rest), c))

    def start4(self):
        r, c, z = place()
        for j in range(1, self.pn.ns):
            to, cp = self.c3(j)

            @pl.when(self.here(to))
            def _():
                cp.wait_send()

        @pl.when(self.here(z))
        def _():
            for j in range(1, self.pn.ns):
                self.c3(j)[1].wait_recv()
            at = lax.clamp(0, z - self.k0, self.k1 - self.k0 - 1) * self.m if self.scatter else 0
            v = self.src[c, r, pl.ds(at, self.m)].astype(F32)
            for j in range(1, self.pn.ns):
                v = v + self.r3[j - 1].astype(F32)
            self.ag[c, r] = v.astype(BF16)
            for j in range(1, self.pn.rest):
                self.c4(j).start()

    def c5(self):
        r, c, z = place()
        return remote(self.ag.at[c], self.ag.at[c], self.sems, self.k5, peer(r, 1 - c))

    def start5(self):
        r, c, z = place()

        @pl.when(self.here(z))
        def _():
            for j in range(1, self.pn.rest):
                self.c4(j).wait()
            self.c5().start()

    def finish(self):
        r, c, z = place()

        @pl.when(self.here(z))
        def _():
            self.c5().wait()


SMALL = (0, 769, 770, 771, 772)


class Small:
    def __init__(self, pn, own, r1, mid, r2, sems):
        self.pn, self.own, self.r1, self.mid, self.r2, self.sems = pn, own, r1, mid, r2, sems

    @staticmethod
    def scratch(pn):
        u = len(SMALL)
        return [pltpu.VMEM((u, 8, 128), BF16), pltpu.VMEM((pn.ndp, u, 8, 128), BF16), pltpu.VMEM((u, 8, 128), BF16), pltpu.VMEM((pn.ns, u, 8, 128), BF16),
                pltpu.SemaphoreType.DMA((2, pn.ndp + pn.ns - 2))]

    def c1(self, j):
        me = lax.axis_index("dp")
        return remote(self.own, self.r1.at[me], self.sems, j - 1, {"dp": lax.rem(me + j, self.pn.ndp)})

    def w1(self, j):
        me = lax.axis_index("dp")
        return remote(self.own, self.r1.at[lax.rem(me - j + self.pn.ndp, self.pn.ndp)], self.sems, j - 1, {"dp": lax.rem(me + j, self.pn.ndp)})

    def start1(self):
        me = lax.axis_index("dp")
        for j in range(1, self.pn.ndp):
            self.c1(j).start()
        self.r1[me] = self.own[...]

    def c2(self, j):
        z = lax.axis_index("opt")
        to = lax.rem(z + j, self.pn.ns)
        return to, remote(self.mid, self.r2.at[z], self.sems, self.pn.ndp - 2 + j, {"opt": to})

    def w2(self, j):
        z = lax.axis_index("opt")
        return remote(self.mid, self.r2.at[lax.rem(z - j + self.pn.ns, self.pn.ns)], self.sems, self.pn.ndp - 2 + j, {"opt": lax.rem(z + j, self.pn.ns)})

    def start2(self):
        z = lax.axis_index("opt")
        for j in range(1, self.pn.ndp):
            self.c1(j).wait_send()
            self.w1(j).wait_recv()
        v = self.r1[0].astype(F32)
        for n in range(1, self.pn.ndp):
            v = v + self.r1[n].astype(F32)
        self.mid[...] = v.astype(BF16)
        for j in range(1, self.pn.ns):
            to, cp = self.c2(j)

            @pl.when(to <= self.pn.ka)
            def _():
                cp.start()
        self.r2[z] = v.astype(BF16)

    def finish(self):
        z = lax.axis_index("opt")
        for j in range(1, self.pn.ns):
            to, cp = self.c2(j)

            @pl.when(to <= self.pn.ka)
            def _():
                cp.wait_send()

            @pl.when(z <= self.pn.ka)
            def _():
                self.w2(j).wait_recv()

    def total(self, n):
        v = self.r2[0, n].astype(F32)
        for k in range(1, self.pn.ns):
            v = v + self.r2[k, n].astype(F32)
        return v.astype(BF16).astype(F32)


BM = 784
NSEMS = 32


def put_rows_grad(fs, start, v):
    put_rows(fs, start, v)


def kernel_bc(pn, x_hbm, cot_hbm, ob_hbm, wp_hbm, w1_hbm, w2_hbm, hwt_hbm, qkv_hbm, p_hbm, wqkv_hbm, vec, rel_ref, counts,
              y_hbm, dx_hbm, g_hbm, *refs):
    refs = list(refs)
    dx1, wp, acc, dsem = refs[:4]
    refs = refs[4:]
    chunks = []
    for n, (k0, k1, scatter, m) in enumerate(part_list(pn)):
        if n == 1:
            refs.insert(5, chunks[0].ag)
        chunks.append(Chunk(pn, k0, k1, scatter, m, *refs[:6]))
        refs = refs[6:]
    hi, lo = chunks[:2]
    ac = chunks[2:]
    small = Small(pn, *refs)
    count = counts[0]

    def local(n, src, dst):
        return pltpu.make_async_copy(src, dst, dsem.at[n])

    def mlp(x_v, dy_v, ob, a, du, h2, w1, w2, fs, xsem, csem):
        ins = [local(n, s, d) for n, (s, d) in enumerate([(ob_hbm, ob), (wp_hbm, wp), (w1_hbm, w1), (w2_hbm, w2)])]
        cps = window_copies(x_hbm, x_v, xsem, True) + window_copies(cot_hbm, dy_v, csem, True)
        for cp in cps + ins:
            cp.start()
        acc[...] = jnp.zeros_like(acc)
        bp, g2, b2, c2 = (vec[n:n + 1, :] for n in range(4, 8))
        enter(pn, True)
        for cp in cps + ins:
            cp.wait()
        nb = BM // 56

        def rows(t, _):
            r0 = pl.multiple_of(t * BM, BM)
            x = x_v[pl.ds(nb * t, nb)].reshape(BM, D).astype(F32)
            alive = lax.broadcasted_iota(jnp.int32, (nb, 7, 8, D), 2) < count
            dy = jnp.where(alive, dy_v[pl.ds(nb * t, nb)].astype(F32), 0.0)
            dyb = dy.astype(BF16)
            dy_v[pl.ds(nb * t, nb)] = dyb
            dy = dy.reshape(BM, D)
            dyb = dyb.reshape(BM, D)
            x1 = x + dot(ob[pl.ds(r0, BM), :], wp[...]) + bp
            xhat, r = norm_stats(x1)
            h = (xhat * g2 + b2).astype(BF16)
            h2[pl.ds(r0, BM), :] = h
            y = x1 + c2
            dh = jnp.zeros((BM, D), F32)
            for j in range(HID // CH):
                cs = slice(j * CH, (j + 1) * CH)
                u = dot(h, w1[:, cs]) + vec[8 + j:9 + j, :]
                cdf, pdf = gelu_parts(u)
                av = (u * cdf).astype(BF16)
                a[pl.ds(r0, BM), cs] = av
                y = y + dot(av, w2[cs, :])
                da = dot_nt(dyb, w2[cs, :])
                duv = da * (cdf + u * pdf)
                acc_rows(acc, 4 + j, duv)
                dub = duv.astype(BF16)
                du[pl.ds(r0, BM), cs] = dub
                dh = dh + dot_nt(dub, w1[:, cs])
            x_v[pl.ds(nb * t, nb)] = y.reshape(nb, 7, 8, D).astype(BF16)
            acc_rows(acc, 0, dy)
            acc_rows(acc, 1, dh * xhat)
            acc_rows(acc, 2, dh)
            dg = dh * g2
            dt = r * (dg - jnp.mean(dg, -1, keepdims=True) - xhat * jnp.mean(dg * xhat, -1, keepdims=True))
            dxv = dy + dt
            acc_rows(acc, 3, dxv)
            dx1[pl.ds(nb * t, nb)] = dxv.reshape(nb, 7, 8, D)
            return 0
        lax.fori_loop(0, ROWS // BM, rows, 0)
        ycs = window_copies(y_hbm, x_v, xsem, False)
        for cp in ycs:
            cp.start()
        vg = jnp.sum(acc[...].reshape(8, 8, D), 1)
        first = pn.base * 8
        nrow = pn.bunits * 8
        lo_row = (R_PROJ // 8 + 1) * 8 - first
        hi_row = R_END // 8 * 8 - first
        fs[0:lo_row, :] = jnp.zeros((lo_row, 128), F32)
        fs[hi_row:nrow, :] = jnp.zeros((nrow - hi_row, 128), F32)
        dyf = dy_v[...].reshape(ROWS, D)

        def w2rows(t, _):
            r0 = pl.multiple_of(t * 512, 512)
            v = dot_tn(a[:, pl.ds(r0, 512)], dyf)
            for c in range(4):
                put_block(fs, R_W2 - first + r0 * 4 + c, 4, v[:, c * 128:(c + 1) * 128])
            return 0
        lax.fori_loop(0, HID // 512, w2rows, 0)
        put_vec(fs, R_C2 - first, vg[0:1])

        def fill(ch):
            for k in range(ch.k0, ch.k1):
                def piece(p, _):
                    row = pl.multiple_of(((k - pn.ka) * pn.units + p * pn.pc) * 8, 8)
                    ch.src[p & 1, lax.shift_right_arithmetic(p, 1), (k - ch.k0) * pn.pc:(k - ch.k0 + 1) * pn.pc] = fs[pl.ds(row, pn.pc * 8), :].reshape(pn.pc, 8, 128).astype(BF16)
                    return 0
                lax.fori_loop(0, pn.ndp, piece, 0)
        fill(hi)
        hi.start1()
        h2t = a.at[0:D, 0:1664]
        transpose_rows(h2, h2t)

        def w1rows(t, _):
            r0 = pl.multiple_of(t * 256, 256)
            v = dot(h2t[:, 0:ROWS], du[:, pl.ds(r0, 256)])
            for c in range(2):
                put_block(fs, R_W1 - first + 2 * t + c, 16, v[:, c * 128:(c + 1) * 128])
            return 0
        lax.fori_loop(0, HID // 256, w1rows, 0)
        hi.start2()
        v = dot_tn(ob[...], dx1[...].reshape(ROWS, D).astype(BF16))
        for c in range(4):
            put_block(fs, R_PROJ - first + c, 4, v[:, c * 128:(c + 1) * 128])
        for row, n in ((R_BP, 3), (R_G2, 1), (R_B2, 2)):
            put_vec(fs, row - first, vg[n:n + 1])
        for j in range(4):
            put_vec(fs, R_C1 - first + 4 * j, vg[4 + j:5 + j])
        fill(lo)
        lo.start1()
        for cp in ycs:
            cp.wait()

    big = pltpu.VMEM((28, 7, 8, D), BF16)
    pl.run_scoped(mlp, big, big, pltpu.VMEM((ROWS, D), BF16), pltpu.VMEM((ROWS, HID), BF16), pltpu.VMEM((ROWS, HID), BF16), pltpu.VMEM((ROWS, D), BF16),
                  pltpu.VMEM((D, HID), BF16), pltpu.VMEM((HID, D), BF16), pltpu.VMEM((pn.bunits * 8, 128), F32),
                  pltpu.SemaphoreType.DMA((NSEG,)), pltpu.SemaphoreType.DMA((NSEG,)))

    def attention(x_v, qkvb, pb, hwt, wqkv, fs, os_, dq, dtab, xsem):
        ins = [local(n, s, d) for n, (s, d) in enumerate([(qkv_hbm, qkvb), (p_hbm, pb), (hwt_hbm, hwt), (wqkv_hbm, wqkv)])]
        for cp in ins:
            cp.start()
        cps = window_copies(x_hbm, x_v, xsem, True)
        for cp in cps:
            cp.start()
        acc[...] = jnp.zeros_like(acc)
        dtab[...] = jnp.zeros_like(dtab)

        def rows0(t, _):
            r0 = pl.multiple_of(t * 392, 8)
            ev = dx1[pl.ds(7 * t, 7)].reshape(392, D).astype(BF16)
            v = dot_nt(ev, wp[...])
            for g in range(4):
                os_[pl.ds(g * RS + r0, 392), :] = v[:, g * 128:(g + 1) * 128]
            return 0
        lax.fori_loop(0, 4, rows0, 0)
        ins[0].wait()
        ins[1].wait()
        lo.start2()
        heads = lane_head()

        def several(g, items):
            bases = [lax.shift_right_arithmetic(i, 3) * WROWS + (i & 7) for i in items]
            dobds = [block_diag(take_rows(os_, g * RS + base).astype(BF16), heads) for base in bases]
            dps = [dot_nt(qkvb[i, 8 + g], d) for i, d in zip(items, dobds)]
            total = dtab[g]
            dsbs = []
            for i, dp in zip(items, dps):
                p = pb[i, g].astype(F32)
                t = p * dp
                ds = t - p * jnp.sum(t, 0, keepdims=True)
                total = total + ds
                dsbs.append(ds.astype(BF16))
            dtab[g] = total
            dvs = [dot(pb[i, g], d) for i, d in zip(items, dobds)]
            dks = [dot(d, block_diag(qkvb[i, g], heads)) for i, d in zip(items, dsbs)]
            dqs = [dot_tn(d, qkvb[i, 4 + g]) for i, d in zip(items, dsbs)]
            for base, dv, dk, dqv in zip(bases, dvs, dks, dqs):
                put_rows(fs, 2 * RS + base, dv)
                put_rows(fs, RS + base, dk)
                put_rows(fs, base, diag_sum(dqv, heads) * SCALE)

        mid = {0: (hi.start3,), 1: (ac[0].start2,), 2: (ac[1].start2, hi.start4), 3: (ac[2].start2,)}
        for g in range(4):
            def attend(t, _):
                @pl.when(t == 4)
                def _():
                    for f in mid[g]:
                        f()
                several(g, [4 * t + n for n in range(4)])
                return 0
            lax.fori_loop(0, WB // 4, attend, 0)
            parts = []
            for n in range(3):
                v = fs[n * RS:n * RS + ROWS, :]
                if n != 1:
                    acc[8 * (2 + n // 2):8 * (3 + n // 2), g * 128:(g + 1) * 128] = jnp.sum(v.reshape(ROWS // 8, 8, 128), 0)
                v = v.astype(BF16)
                dq[:, n * D + g * 128:n * D + (g + 1) * 128] = v
                parts.append(v)
            if g == 0:
                ins[2].wait()
                ins[3].wait()
            v = dot(hwt[...], jnp.concatenate(parts, 1))
            mu = pn.mrow // 8
            for n in range(3):
                u = v[:, n * 128:(n + 1) * 128].reshape(D // 8, 8, 128).astype(BF16)
                for p in range(pn.ndp):
                    ac[g].src[p & 1, p >> 1, n * mu:(n + 1) * mu] = u[p * mu:(p + 1) * mu]
            ac[g].start1()
        for cp in cps:
            cp.wait()
        gain = vec[0:1, :]
        tab = table_grad(rel_ref, os_, dtab)
        for n in range(3):
            small.own[2 + n] = tab[8 * n:8 * n + 8].astype(BF16)
        late = {1: (lo.start3, ac[3].start2), 2: (ac[0].start3, hi.start5), 3: (ac[1].start3,), 4: (ac[2].start3,), 5: (ac[3].start3, ac[0].start4), 6: (ac[1].start4,)}

        def rows1(t, _):
            for k, fns in late.items():
                @pl.when(t == k)
                def _():
                    for f in fns:
                        f()
            r0 = pl.multiple_of(t * BLK, BLK)
            dn = dot_nt(dq[pl.ds(r0, BLK), :], wqkv[...])
            x = x_v[pl.ds(4 * t, 4)].reshape(BLK, D).astype(F32)
            xhat, r = norm_stats(x)
            acc_rows(acc, 0, dn * xhat)
            acc_rows(acc, 1, dn)
            dg = dn * gain
            dt = r * (dg - jnp.mean(dg, -1, keepdims=True) - xhat * jnp.mean(dg * xhat, -1, keepdims=True))
            dx1[pl.ds(4 * t, 4)] += dt.reshape(4, 7, 8, D)
            return 0
        lax.fori_loop(0, NBLK, rows1, 0)
        vg = jnp.sum(acc[...].reshape(8, 8, D), 1)
        flat = [vg[n:n + 1, c * 128:(c + 1) * 128] for n in range(4) for c in range(4)]
        small.own[0] = jnp.concatenate(flat[:8], 0).astype(BF16)
        small.own[1] = jnp.concatenate(flat[8:], 0).astype(BF16)
        small.start1()
        ycs = window_copies(dx_hbm, dx1, xsem, False)
        for cp in ycs:
            cp.start()
        for f in (lo.start4, ac[2].start4, ac[3].start4, ac[0].start5, ac[1].start5, small.start2, lo.start5, ac[2].start5, ac[3].start5):
            f()
        for ch in chunks:
            ch.finish()
        r, c, z = place()
        g = os_

        def scattered(ch):
            @pl.when(ch.here(z))
            def _():
                def piece(p, _):
                    g[pl.ds(pl.multiple_of(p * pn.pc * 8, 8), pn.pc * 8), :] = ch.ag[p & 1, lax.shift_right_arithmetic(p, 1)].astype(F32).reshape(pn.pc * 8, 128)
                    return 0
                lax.fori_loop(0, pn.ndp, piece, 0)
        scattered(hi)
        scattered(lo)
        mu = pn.mrow // 8

        @pl.when(z < pn.ka)
        def _():
            def piece(p, _):
                for h in range(4):
                    for n in range(3):
                        v = ac[h].ag[p & 1, lax.shift_right_arithmetic(p, 1), n * mu:(n + 1) * mu].astype(F32).reshape(pn.mrow, 128)
                        g[pl.ds(R_QKV + p * pn.mrow * 12 + n * 4 + h, pn.mrow, stride=12), :] = v
                return 0
            lax.fori_loop(0, pn.ndp, piece, 0)
        small.finish()

        @pl.when(z < pn.ka)
        def _():
            for n, u in enumerate(SMALL):
                g[u * 8:u * 8 + 8, :] = small.total(n)

        @pl.when(z == pn.ka)
        def _():
            for n, u in enumerate(SMALL):
                if u >= pn.base:
                    k = (u - pn.base) * 8
                    g[k:k + 8, :] += small.total(n)
        out = local(0, g.at[pl.ds(pl.multiple_of(lax.select(z < pn.ka, z * (pn.units * 8), 0), 8), pn.units * 8)], g_hbm)
        out.start()
        out.wait()
        for cp in ycs:
            cp.wait()

    pl.run_scoped(attention, big, pltpu.VMEM((WB, 12, 64, 128), BF16), pltpu.VMEM((WB, 4, 64, 256), BF16), pltpu.VMEM((D, ROWS), BF16), pltpu.VMEM((D, 3 * D), BF16),
                  pltpu.VMEM((3 * RS, 128), F32), pltpu.VMEM((max(4 * RS, pn.gunits * 8), 128), F32), pltpu.VMEM((ROWS, 3 * D), BF16), pltpu.VMEM((4, 64, 256), F32), pltpu.SemaphoreType.DMA((NSEG,)))


def part_list(pn):
    mu = 3 * pn.mrow // 8
    return [(pn.kh, pn.ns, True, pn.pc), (pn.ka, pn.kh, True, pn.pc)] + [(0, pn.ka, False, mu)] * 4


def call_bc(pn, x, cot, ob, wp, w1, w2, hwt, qkv, p, wqkv, vec, rel, counts):
    any_ = pl.BlockSpec(memory_space=pl.ANY)
    vm = pl.BlockSpec(memory_space=pltpu.VMEM)
    sds = jax.ShapeDtypeStruct
    outs = [sds((14, 14, 8, D), BF16), sds((14, 14, 8, D), F32), sds((pn.units * 8, 128), F32)]
    scratch = [pltpu.VMEM((28, 7, 8, D), F32), pltpu.VMEM((D, D), BF16), pltpu.VMEM((64, D), F32), pltpu.SemaphoreType.DMA((4,))]
    for n, (k0, k1, scatter, m) in enumerate(part_list(pn)):
        scratch += Chunk.scratch(pn, m, k1 - k0 if scatter else 1, n == 1)
    scratch += Small.scratch(pn)
    return pl.pallas_call(
        functools.partial(kernel_bc, pn),
        out_shape=outs,
        in_specs=[any_] * 10 + [vm, vm, pl.BlockSpec(memory_space=pltpu.SMEM)],
        out_specs=[any_] * 3,
        scratch_shapes=scratch,
        compiler_params=pltpu.CompilerParams(vmem_limit_bytes=67000000, collective_id=1, has_side_effects=True),
        name="back",
    )(x, cot, ob, wp, w1, w2, hwt, qkv, p, wqkv, vec, rel, counts)


STEP = 2
DECAYED = (2, 6, 10, 12)
LENGTHS = [D, D, 3 * D * D, D, D, TAB * HEADS, D * D, D, D, D, D * HID, HID, HID * D, D]
AU = 64


def kernel_adam(rates, first, g, p, m1, m2, g_o, p_o, m_o, v_o):
    shape = (AU, 8, 128)
    u0 = first[0] + pl.program_id(0) * AU
    starts = [sum(LENGTHS[:n + 1]) for n in range(len(LENGTHS))]

    def group(at):
        k = jnp.int32(0)
        for s in starts:
            k = k + (at >= s).astype(jnp.int32)
        return k

    def update(rate, decay):
        grad = g[...]
        w = p[...]
        m = 0.9 * m1[...] + 0.1 * grad
        v = 0.999 * m2[...] + 0.001 * grad * grad
        mh = m / (1.0 - 0.9 ** STEP)
        vh = v / (1.0 - 0.999 ** STEP)
        p_o[...] = w - rate * (mh / (jnp.sqrt(vh) + 1e-08) + decay * w)
        m_o[...] = m
        v_o[...] = v
        g_o[...] = grad
    k0 = group(u0 * 1024)
    k1 = group((u0 + AU) * 1024 - 1)

    @pl.when(k0 == k1)
    def _():
        decay = jnp.float32(0.0)
        for n in DECAYED:
            decay = jnp.where(k0 == n, jnp.float32(0.05), decay)
        update(rates[k0], decay)

    @pl.when(k0 != k1)
    def _():
        index = ((u0 + lax.broadcasted_iota(jnp.int32, shape, 0)) * 8 + lax.broadcasted_iota(jnp.int32, shape, 1)) * 128 + lax.broadcasted_iota(jnp.int32, shape, 2)
        rate = jnp.zeros(shape, F32) + rates[0]
        decay = jnp.zeros(shape, F32)
        for n, s in enumerate(starts):
            after = index >= s
            rate = jnp.where(after, rates[n + 1], rate)
            if n in DECAYED or n + 1 in DECAYED:
                decay = jnp.where(after, 0.05 if n + 1 in DECAYED else 0.0, decay)
        update(rate, decay)


def call_adam(pn, rates, g, params, mom1, mom2):
    view = lambda t: t.reshape(pn.units, 8, 128)
    spec = pl.BlockSpec((AU, 8, 128), lambda i: (i, 0, 0))
    sm = pl.BlockSpec(memory_space=pltpu.SMEM)
    first = (lax.axis_index("opt") * pn.units).astype(jnp.int32).reshape(1)
    out = pl.pallas_call(
        kernel_adam,
        grid=(pl.cdiv(pn.units, AU),),
        out_shape=[jax.ShapeDtypeStruct((pn.units, 8, 128), F32)] * 4,
        in_specs=[sm, sm] + [spec] * 4,
        out_specs=[spec] * 4,
        compiler_params=pltpu.CompilerParams(vmem_limit_bytes=67043328),
        name="adamw",
    )(rates, first, view(g), view(params), view(mom1), view(mom2))
    return [t.reshape(-1) for t in out]


from jax.sharding import PartitionSpec as P


def solution(mesh):
    def local(images, cotangent, counts, rel_index, params, moment1, moment2, rates):
        pn = Plan(mesh, params.shape[0])
        xt = images.transpose(1, 2, 0, 3)
        ct = cotangent.transpose(1, 2, 0, 3)
        rel = rel_lanes(rel_index)
        wqkv, wp, w1, w2, vec, hwt, ob, qkv, p = call_a(pn, xt, params, rel)
        y, dx, g = call_bc(pn, xt, ct, ob, wp, w1, w2, hwt, qkv, p, wqkv, vec, rel, counts)
        grad, new_params, new_first, new_second = call_adam(pn, rates, g, params, moment1, moment2)
        return (y.transpose(2, 0, 1, 3), dx.transpose(2, 0, 1, 3), grad, new_params, new_first, new_second)

    split = P(("dp", "opt"), None, None, None)
    return jax.shard_map(
        local, mesh=mesh,
        in_specs=(split, split, P(("dp", "opt")), P(), P("opt"), P("opt"), P("opt"), P()),
        out_specs=(split, split, P("opt"), P("opt"), P("opt"), P("opt")),
        check_vma=False)
```

```python
import functools
import jax
import jax.numpy as jnp
from jax import lax
from jax.experimental import pallas as pl
from jax.experimental.pallas import tpu as pltpu

D = 512
HEADS = 16
HEAD_DIM = 32
HID = 2048
SIDE = 14
WIN = 7
SHIFT = 3
TAB = 169
F32 = jnp.float32
BF16 = jnp.bfloat16

IMGS = 8
SPAN = WIN * WIN
WROWS = SPAN * IMGS
ROWS = 4 * WROWS
RS = ROWS + 64
BLK = 224
NBLK = ROWS // BLK
WB = 4 * IMGS
SCALE = HEAD_DIM ** -0.5

R_G1, R_B1, R_QKV, R_BQ, R_BV, R_TAB = 0, 4, 8, 6152, 6156, 6160
R_PROJ, R_BP, R_G2, R_B2, R_W1, R_C1, R_W2, R_C2, R_END = 6181, 8229, 8233, 8237, 8241, 16433, 16449, 24641, 24645
LANE = 16
BROW = 6176


def segments(w):
    if w == 0:
        return [(SHIFT, WIN, 0)]
    return [(WIN + SHIFT, WIN - SHIFT, 0), (0, SHIFT, WIN - SHIFT)]


def window_copies(hbm, vmem, sem, inward):
    out = []
    n = 0
    for wy in range(2):
        for wx in range(2):
            for ys, yl, yo in segments(wy):
                for xs, xl, xo in segments(wx):
                    a = hbm.at[pl.ds(ys, yl), pl.ds(xs, xl)]
                    b = vmem.at[pl.ds((2 * wy + wx) * WIN + yo, yl), pl.ds(xo, xl)]
                    out.append(pltpu.make_async_copy(a, b, sem.at[n]) if inward else pltpu.make_async_copy(b, a, sem.at[n]))
                    n += 1
    return out


NSEG = 9


def dot(a, b):
    return lax.dot_general(a, b, (((1,), (0,)), ((), ())), preferred_element_type=F32)


def dot_nt(a, b):
    return lax.dot_general(a, b, (((1,), (1,)), ((), ())), preferred_element_type=F32)


def dot_tn(a, b):
    return lax.dot_general(a, b, (((0,), (0,)), ((), ())), preferred_element_type=F32)


def norm_stats(x):
    mean = jnp.mean(x, -1, keepdims=True)
    dev = x - mean
    var = jnp.mean(dev * dev, -1, keepdims=True)
    r = lax.rsqrt(var + 1e-05)
    return dev * r, r


def pieces_to_rows(pn, wb, fs, shard, count, base):
    def body(p, _):
        row = pl.multiple_of((shard * pn.units - base + p * pn.pc) * 8, 8)
        fs[pl.ds(row, pn.pc * 8), :] = wb[shard, p & 1, lax.shift_right_arithmetic(p, 1)].astype(F32).reshape(pn.pc * 8, 128)
        return 0
    lax.fori_loop(0, count, body, 0)


def vec_from(fs, row, width, shift):
    parts = []
    lane = lax.broadcasted_iota(jnp.int32, (1, 128), 1)
    for c in range(width // 128):
        a = fs[pl.ds(row + c, 1), :]
        if shift:
            b = fs[pl.ds(row + c + 1, 1), :]
            a = jnp.where(lane < 128 - LANE, pltpu.roll(a, 128 - LANE, 1), pltpu.roll(b, 128 - LANE, 1))
        parts.append(a)
    return jnp.concatenate(parts, 1)


def take_matrix(fs, row, dst, nrows, ncb, shift, step=128):
    lane = lax.broadcasted_iota(jnp.int32, (step, 128), 1)

    def body(t, _):
        base = row + t * (step * ncb)
        r0 = pl.multiple_of(t * step, step)
        for c in range(ncb):
            a = fs[pl.ds(base + c, step, stride=ncb), :]
            if shift:
                b = fs[pl.ds(base + c + 1, step, stride=ncb), :]
                a = jnp.where(lane < 128 - LANE, pltpu.roll(a, 128 - LANE, 1), pltpu.roll(b, 128 - LANE, 1))
            dst[pl.ds(r0, step), c * 128:(c + 1) * 128] = a.astype(BF16)
        return 0

    lax.fori_loop(0, nrows // step, body, 0)


def transpose_rows(src, dst):
    full = ROWS // 128

    def body(t, _):
        r0 = pl.multiple_of(t * 128, 128)
        dst[:, pl.ds(r0, 128)] = src[pl.ds(r0, 128), :].T
        return 0
    lax.fori_loop(0, full, body, 0)
    if ROWS % 128:
        dst[:, full * 128:ROWS] = src[full * 128:ROWS, :].T


def lane_head():
    return lax.broadcasted_iota(jnp.int32, (64, 128), 1) // HEAD_DIM


def block_diag(v, heads):
    zero = jnp.zeros_like(v)
    return jnp.concatenate([jnp.where(heads == h, v, zero) for h in range(4)], 0)


def diag_sum(r, heads):
    out = r[0:64]
    for h in range(1, 4):
        out = jnp.where(heads == h, r[64 * h:64 * h + 64], out)
    return out


def take_rows(fs, start):
    v = fs[pl.ds(start, 56, stride=IMGS), :]
    v = jnp.where(lax.broadcasted_iota(jnp.int32, (56, 128), 0) < SPAN, v, 0.0)
    return jnp.concatenate([v, jnp.zeros((8, 128), F32)], 0)


def put_rows(fs, start, v):
    fs[pl.ds(start, 48, stride=IMGS), :] = v[0:48]
    fs[pl.ds(start + 48 * IMGS, 1), :] = v[48:49]


def build_bias(tab3, rel_ref, big, bias):
    rel = rel_ref[...]
    row = lax.shift_right_arithmetic(rel, 3)
    low = rel & 7
    oh = (lax.broadcasted_iota(jnp.int32, (32, 4096), 0) == row).astype(F32).astype(BF16)
    tab = jnp.concatenate([tab3, jnp.zeros((8, 128), F32)], 0).astype(BF16)
    r = dot_tn(tab, oh)
    acc = jnp.zeros((16, 4096), F32)
    for j in range(8):
        acc = acc + jnp.where(low == j, r[16 * j:16 * j + 16], 0.0)
    for kk in range(32):
        big[kk * 16:kk * 16 + 16, :] = acc[:, kk * 128:kk * 128 + 128]
    k = lax.broadcasted_iota(jnp.int32, (64, 256), 0)
    q = lax.broadcasted_iota(jnp.int32, (64, 256), 1) & 63
    ki = lax.shift_right_arithmetic(k * 37, 8)
    kj = k - ki * 7
    qi = lax.shift_right_arithmetic(q * 37, 8)
    qj = q - qi * 7
    cut = WIN - SHIFT
    same_y = (ki < cut) == (qi < cut)
    same_x = (kj < cut) == (qj < cut)
    lane = lax.broadcasted_iota(jnp.int32, (32, 128), 1)
    for g in range(4):
        for pair in range(2):
            h = 4 * g + 2 * pair
            a = big[pl.ds(h, 32, stride=16), :]
            b = big[pl.ds(h + 1, 32, stride=16), :]
            even = jnp.where(lane < 64, a, pltpu.roll(b, 64, 1))
            odd = jnp.where(lane < 64, pltpu.roll(a, 64, 1), b)
            big[pl.ds(1024 + g * 256 + pair * 128, 32, stride=2), :] = even
            big[pl.ds(1024 + g * 256 + pair * 128 + 1, 32, stride=2), :] = odd
    for g in range(4):
        pos = jnp.concatenate([big[1024 + g * 256:1024 + g * 256 + 64, :], big[1024 + g * 256 + 128:1024 + g * 256 + 192, :]], 1)
        for w in range(4):
            keep = None
            if w == 1:
                keep = same_x
            elif w == 2:
                keep = same_y
            elif w == 3:
                keep = same_y & same_x
            val = pos if keep is None else pos + jnp.where(keep, 0.0, -100.0)
            bias[w * 4 + g] = jnp.where(k < SPAN, val, -1e30)


MESH = pl.DeviceIdType.MESH
NMAT = 768


class Plan:
    def __init__(self, mesh, shard_len):
        self.ndp = mesh.shape["dp"]
        self.ns = mesh.shape["opt"]
        self.rest = self.ndp // 2
        self.units = shard_len // 1024
        self.pc = -(-self.units // self.ndp)
        self.ka = (BROW // 8) // self.units
        self.base = self.ka * self.units
        self.bunits = (self.ns - self.ka - 1) * self.units + self.ndp * self.pc
        self.kh = -(-(R_W2 // 8 + 1) // self.units)
        self.mrow = D // self.ndp
        self.gunits = max(BROW // 8 + 1, self.ndp * self.pc)


def place():
    me = lax.axis_index("dp")
    return lax.shift_right_arithmetic(me, 1), me & 1, lax.axis_index("opt")


def peer(r, c):
    return {"dp": 2 * r + c}


def enter(pn, all_dp=False):
    r, c, z = place()
    bar = pltpu.get_barrier_semaphore()
    pl.semaphore_signal(bar, inc=1, device_id=peer(r, 1 - c), device_id_type=MESH)
    for j in range(1, pn.rest):
        for to in ((c, 1 - c) if all_dp else (c,)):
            pl.semaphore_signal(bar, inc=1, device_id=peer(lax.rem(r + j, pn.rest), to), device_id_type=MESH)
    for j in range(1, pn.ns):
        pl.semaphore_signal(bar, inc=1, device_id={"opt": lax.rem(z + j, pn.ns)}, device_id_type=MESH)
    pl.semaphore_wait(bar, (pn.ndp - 1 if all_dp else pn.rest) + pn.ns - 1)


def remote(src, dst, sems, n, where):
    return pltpu.make_async_remote_copy(src_ref=src, dst_ref=dst, send_sem=sems.at[0, n], recv_sem=sems.at[1, n], device_id=where, device_id_type=MESH)


class Gather:
    def __init__(self, pn, wb, osem, xsem, ysem):
        self.pn, self.wb, self.osem, self.xsem, self.ysem = pn, wb, osem, xsem, ysem
        h = (pn.pc + 1) // 2
        self.parts = [pl.ds(0, h), pl.ds(h, pn.pc - h)]

    @staticmethod
    def scratch(pn):
        return [pltpu.VMEM((pn.ns, 2, pn.rest, pn.pc, 8, 128), BF16), pltpu.SemaphoreType.DMA((2, 2 * pn.ns)),
                pltpu.SemaphoreType.DMA((2, 2 * pn.ns * pn.rest)), pltpu.SemaphoreType.DMA((2, 2 * pn.ns))]

    def o(self, j, h):
        r, c, z = place()
        own = self.wb.at[z, c, r, self.parts[h]]
        return pltpu.make_async_remote_copy(src_ref=own, dst_ref=own, send_sem=self.osem.at[0, 2 * j + h], recv_sem=self.osem.at[1, 2 * z + h],
                                            device_id={"opt": lax.rem(z + j, self.pn.ns)}, device_id_type=MESH)

    def arrived(self, s, h):
        r, c, z = place()
        own = self.wb.at[s, c, r, self.parts[h]]
        return pltpu.make_async_remote_copy(src_ref=own, dst_ref=own, send_sem=self.osem.at[0, h], recv_sem=self.osem.at[1, 2 * s + h],
                                            device_id={"opt": lax.rem(z + 1, self.pn.ns)}, device_id_type=MESH)

    def x(self, s, h, j):
        r, c, z = place()
        own = self.wb.at[s, c, r, self.parts[h]]
        return remote(own, own, self.xsem, (2 * s + h) * self.pn.rest + j, peer(lax.rem(r + j, self.pn.rest), c))

    def y(self, s, h):
        r, c, z = place()
        own = self.wb.at[s, c, :, self.parts[h]]
        return remote(own, own, self.ysem, 2 * s + h, peer(r, 1 - c))

    def start(self, first):
        r, c, z = place()
        for h in range(2):
            for j in range(1, self.pn.ns):
                soon = (z < self.pn.ka) | (z + j >= self.pn.ns)

                @pl.when(soon if first else jnp.logical_not(soon))
                def _():
                    self.o(j, h).start()

    def spread(self, s, h):
        r, c, z = place()

        @pl.when(z != s)
        def _():
            self.arrived(s, h).wait_recv()
            for j in range(1, self.pn.rest):
                self.x(s, h, j).start()

    def pair(self, s, h):
        r, c, z = place()

        @pl.when(z != s)
        def _():
            for j in range(1, self.pn.rest):
                self.x(s, h, j).wait_recv()
            self.y(s, h).start()

    def ready(self, s):
        r, c, z = place()

        @pl.when(z != s)
        def _():
            for h in range(2):
                self.y(s, h).wait_recv()

    def finish(self):
        r, c, z = place()
        for h in range(2):
            for j in range(1, self.pn.ns):
                self.o(j, h).wait_send()
            for s in range(self.pn.ns):
                @pl.when(z != s)
                def _():
                    for j in range(1, self.pn.rest):
                        self.x(s, h, j).wait_send()
                    self.y(s, h).wait_send()


def kernel_a(pn, x_hbm, params, rel_ref,
             wqkv_o, wp_o, w1_o, w2_o, vec_o, hw_o, ob_o, qkv_o, p_o,
             x_v, fs, os_, bias, wqkv, wp, w1, w2, vec, hw, hwt, ob, qkvb, pb, xsem, fsem, osem, wsem, flat_v, *gsems):
    cps = window_copies(x_hbm, x_v, xsem, True)
    for c in cps:
        c.start()
    r, c, z = place()
    gather = Gather(pn, flat_v, *gsems)
    fcp = pltpu.make_async_copy(params, fs.at[pl.ds(0, pn.units * 8)], fsem)
    fcp.start()
    enter(pn)
    fcp.wait()

    def cast(p):
        flat_v[z, p & 1, lax.shift_right_arithmetic(p, 1)] = fs[pl.ds(pl.multiple_of(p * pn.pc * 8, 8), pn.pc * 8), :].reshape(pn.pc, 8, 128).astype(BF16)
    me = lax.axis_index("dp")
    cast(me)
    gather.start(True)

    def others(j, _):
        cast(lax.rem(me + j, pn.ndp))
        return 0
    lax.fori_loop(1, pn.ndp, others, 0)
    for h in range(2):
        for k in range(pn.ka):
            gather.spread(k, h)
    gather.start(False)
    for h in range(2):
        for k in range(pn.ka):
            gather.pair(k, h)
        gather.spread(pn.ka, h)
    for k in range(pn.ka):
        gather.ready(k)
    for k in range(pn.ka):
        pieces_to_rows(pn, flat_v, fs, k, pn.ndp, 0)
    take_matrix(fs, R_QKV, wqkv, D, 12, False)
    vec[0:1, :] = vec_from(fs, R_G1, D, False)
    vec[1:2, :] = vec_from(fs, R_B1, D, False)
    vec[2:3, :] = vec_from(fs, R_BQ, D, False)
    vec[3:4, :] = vec_from(fs, R_BV, D, False)
    wos = [pltpu.make_async_copy(wqkv, wqkv_o, wsem.at[0])]
    wos[0].start()
    for cp in cps:
        cp.wait()
    gain = vec[0:1, :]
    shift = vec[1:2, :]
    bq = vec[2:3, :]
    bv = vec[3:4, :]

    def rows(t, _):
        @pl.when(t == 2)
        def _():
            for h in range(2):
                gather.pair(pn.ka, h)
            for k in range(pn.ka + 1, pn.ns):
                for h in range(2):
                    gather.spread(k, h)
        r0 = pl.multiple_of(t * BLK, BLK)
        x = x_v[pl.ds(4 * t, 4)].reshape(BLK, D).astype(F32)
        xhat, _r = norm_stats(x)
        h = (xhat * gain + shift).astype(BF16)
        hw[pl.ds(r0, BLK), :] = h
        for c in range(12):
            y = dot(h, wqkv[:, c * 128:(c + 1) * 128])
            if c < 4:
                y = (y + bq[:, c * 128:(c + 1) * 128]) * SCALE
            if c >= 8:
                y = y + bv[:, (c - 8) * 128:(c - 7) * 128]
            fs[pl.ds(c * RS + r0, BLK), :] = y
        return 0
    lax.fori_loop(0, NBLK, rows, 0)
    gather.ready(pn.ka)
    tab = []
    for u in range(R_TAB // 8, R_TAB // 8 + 3):
        k, at = (pn.ka, u - pn.base) if u >= pn.base else (pn.ka - 1, u - pn.base + pn.units)
        p = at // pn.pc
        tab.append(flat_v[k, p & 1, p >> 1, at - p * pn.pc].astype(F32))
    build_bias(jnp.concatenate(tab, 0), rel_ref, os_, bias)
    heads = lane_head()

    def saved(t):
        four = pl.ds(4 * t, 4)
        return [pltpu.make_async_copy(qkvb.at[four], qkv_o.at[four], osem.at[2 + t]), pltpu.make_async_copy(pb.at[four], p_o.at[four], osem.at[2 + WB // 4 + t])]

    def attend(t, _):
        un = 4
        items = [(un * t + n, g) for n in range(un) for g in range(4)]
        ss = []
        vs = []
        for i, g in items:
            w = lax.shift_right_arithmetic(i, 3)
            base = w * WROWS + (i & 7)
            q = take_rows(fs, g * RS + base).astype(BF16)
            k = take_rows(fs, (4 + g) * RS + base).astype(BF16)
            v = take_rows(fs, (8 + g) * RS + base).astype(BF16)
            qkvb[i, g] = q
            qkvb[i, 4 + g] = k
            qkvb[i, 8 + g] = v
            vs.append(v)
            ss.append(dot_nt(k, block_diag(q, heads)) + bias[w * 4 + g])
        ps = []
        for (i, g), s in zip(items, ss):
            m = jnp.max(s, 0, keepdims=True)
            e = jnp.exp(s - m)
            p = (e * (1.0 / jnp.sum(e, 0, keepdims=True))).astype(BF16)
            pb[i, g] = p
            ps.append(p)
        for (i, g), p, v in zip(items, ps, vs):
            w = lax.shift_right_arithmetic(i, 3)
            base = w * WROWS + (i & 7)
            o = diag_sum(dot_tn(p, v), heads)
            put_rows(os_, g * RS + base, o)
        for cp in saved(t):
            cp.start()

        @pl.when(t == 2)
        def _():
            for k in range(pn.ka + 1, pn.ns):
                for h in range(2):
                    gather.pair(k, h)
        return 0
    lax.fori_loop(0, WB // 4, attend, 0)

    def outs(t, _):
        r0 = pl.multiple_of(t * BLK, BLK)
        for g in range(4):
            ob[pl.ds(r0, BLK), g * 128:(g + 1) * 128] = os_[pl.ds(g * RS + r0, BLK), :].astype(BF16)
        return 0
    lax.fori_loop(0, NBLK, outs, 0)
    transpose_rows(hw, hwt)
    cos = [pltpu.make_async_copy(a, b, osem.at[n]) for n, (a, b) in enumerate([(hwt, hw_o), (ob, ob_o)])]
    for cp in cos:
        cp.start()
    for k in range(pn.ka + 1, pn.ns):
        gather.ready(k)
    for k in range(pn.ka, pn.ns):
        pieces_to_rows(pn, flat_v, fs, k, pn.ndp, pn.base)
    first = pn.base * 8
    take_matrix(fs, R_PROJ - first, wp, D, 4, True)
    take_matrix(fs, R_W1 - first, w1, D, 16, True)
    take_matrix(fs, R_W2 - first, w2, HID, 4, True)
    for n, r in enumerate((R_BP, R_G2, R_B2, R_C2)):
        vec[4 + n:5 + n, :] = vec_from(fs, r - first, D, True)
    for n in range(4):
        vec[8 + n:9 + n, :] = vec_from(fs, R_C1 - first + 4 * n, D, True)
    for n, (a, b) in enumerate([(wp, wp_o), (w1, w1_o), (w2, w2_o), (vec, vec_o)]):
        wos.append(pltpu.make_async_copy(a, b, wsem.at[n + 1]))
        wos[-1].start()
    for t in range(WB // 4):
        cos += saved(t)
    for cp in cos + wos:
        cp.wait()
    gather.finish()


def call_a(pn, x, params, rel):
    any_ = pl.BlockSpec(memory_space=pl.ANY)
    sds = jax.ShapeDtypeStruct
    outs = [sds((D, 3 * D), BF16), sds((D, D), BF16), sds((D, HID), BF16), sds((HID, D), BF16), sds((16, D), F32),
            sds((D, ROWS), BF16), sds((ROWS, D), BF16), sds((WB, 12, 64, 128), BF16), sds((WB, 4, 64, 256), BF16)]
    return pl.pallas_call(
        functools.partial(kernel_a, pn),
        out_shape=outs,
        in_specs=[any_, any_, pl.BlockSpec(memory_space=pltpu.VMEM)],
        out_specs=[any_] * len(outs),
        scratch_shapes=[
            pltpu.VMEM((28, 7, 8, D), BF16), pltpu.VMEM((12 * RS, 128), F32), pltpu.VMEM((4 * RS, 128), F32),
            pltpu.VMEM((16, 64, 256), F32), pltpu.VMEM((D, 3 * D), BF16), pltpu.VMEM((D, D), BF16), pltpu.VMEM((D, HID), BF16), pltpu.VMEM((HID, D), BF16),
            pltpu.VMEM((16, D), F32), pltpu.VMEM((ROWS, D), BF16), pltpu.VMEM((D, ROWS), BF16), pltpu.VMEM((ROWS, D), BF16), pltpu.VMEM((WB, 12, 64, 128), BF16), pltpu.VMEM((WB, 4, 64, 256), BF16),
            pltpu.SemaphoreType.DMA((NSEG,)), pltpu.SemaphoreType.DMA, pltpu.SemaphoreType.DMA((2 + WB // 2,)), pltpu.SemaphoreType.DMA((5,)),
        ] + Gather.scratch(pn),
        compiler_params=pltpu.CompilerParams(vmem_limit_bytes=64000000, collective_id=0, has_side_effects=True),
        name="attend",
    )(x, params.reshape(pn.units * 8, 128), rel)


def rel_lanes(rel_index):
    t = jnp.full((64, 64), -1, jnp.int32).at[:SPAN, :SPAN].set(rel_index.T)
    return t.reshape(1, 4096)


CH = 512
INV_SQRT2 = 0.7071067811865476
INV_SQRT2PI = 0.3989422804014327


def gelu_parts(u):
    e = jnp.exp(u * u * -0.5)
    t = 1.0 / (1.0 + jnp.abs(u) * (0.3275911 * INV_SQRT2))
    half = t * (0.127414796 + t * (-0.142248368 + t * (0.7107068705 + t * (-0.7265760135 + t * 0.5307027145)))) * e
    cdf = jnp.where(u >= 0, 1.0 - half, half)
    return cdf, e * INV_SQRT2PI


def put_block(fs, start, stride, v):
    n = v.shape[0]
    lane = lax.broadcasted_iota(jnp.int32, (n, 128), 1)
    v = pltpu.roll(v, LANE, 1)
    here = pl.ds(start, n, stride=stride) if n > 1 else pl.ds(start, 1)
    fs[here, :] = jnp.where(lane >= LANE, v, fs[here, :])
    here = pl.ds(start + 1, n, stride=stride) if n > 1 else pl.ds(start + 1, 1)
    fs[here, :] = jnp.where(lane < LANE, v, fs[here, :])


def shifted(blocks):
    return [pltpu.roll(v, LANE, 1) for v in blocks]


def put_tile(fs, base, stride, blocks):
    n = blocks[0].shape[0]
    lane = lax.broadcasted_iota(jnp.int32, (n, 128), 1)
    head = lax.broadcasted_iota(jnp.int32, (n, 128), 0) == 0
    one = lax.broadcasted_iota(jnp.int32, (1, 128), 1)
    v = shifted(blocks)
    first = fs[pl.ds(base, 1), :]
    last = fs[pl.ds(base + n * stride, 1), :]
    before = jnp.where(head, first, pltpu.roll(v[-1], 1, 0))
    for c in range(len(blocks)):
        fs[pl.ds(base + c, n, stride=stride), :] = jnp.where(lane >= LANE, v[c], before if c == 0 else v[c - 1])
    fs[pl.ds(base + n * stride, 1), :] = jnp.where(one < LANE, v[-1][n - 1:n], last)


def put_vec(fs, row, v):
    for c in range(v.shape[1] // 128):
        put_block(fs, row + c, 1, v[:, c * 128:(c + 1) * 128])


def acc_rows(ref, i, v):
    ref[8 * i:8 * i + 8, 0:v.shape[1]] += jnp.sum(v.reshape(v.shape[0] // 8, 8, v.shape[1]), 0)


def table_grad(rel_ref, big, dtab):
    lane = lax.broadcasted_iota(jnp.int32, (32, 128), 1)
    for g in range(4):
        for pair in range(2):
            at = 1024 + g * 256 + pair * 128
            big[at:at + 64, :] = dtab[g, :, pair * 128:pair * 128 + 128]
    for g in range(4):
        for pair in range(2):
            at = 1024 + g * 256 + pair * 128
            even = big[pl.ds(at, 32, stride=2), :]
            odd = big[pl.ds(at + 1, 32, stride=2), :]
            h = 4 * g + 2 * pair
            big[pl.ds(h, 32, stride=16), :] = jnp.where(lane < 64, even, pltpu.roll(odd, 64, 1))
            big[pl.ds(h + 1, 32, stride=16), :] = jnp.where(lane < 64, pltpu.roll(even, 64, 1), odd)
    rel = rel_ref[...]
    row = lax.shift_right_arithmetic(rel, 3)
    low = rel & 7
    oh = (lax.broadcasted_iota(jnp.int32, (32, 4096), 0) == row).astype(F32).astype(BF16)
    grad = jnp.concatenate([big[kk * 16:kk * 16 + 16, :] for kk in range(32)], 1)
    out = jnp.zeros((32, 128), F32)
    high = grad.astype(BF16).astype(F32)
    for part in (high, grad - high):
        m = jnp.concatenate([jnp.where(low == j, part, 0.0) for j in range(8)], 0).astype(BF16)
        out = out + dot_nt(oh, m)
    return out


class Chunk:
    def __init__(self, pn, k0, k1, n, at, flip, src, r1, r2, sems, r3, ag):
        self.pn, self.k0, self.k1, self.n, self.at = pn, k0, k1, n, at
        self.steps = list(range(pn.rest.bit_length() - 1))
        if flip:
            self.steps.reverse()
        self.src, self.r1, self.r2, self.r3, self.ag, self.sems = src, r1, r2, r3, ag, sems
        self.k2 = 1
        self.k3 = self.k2 + pn.rest - 1
        self.k4 = self.k3 + pn.ns - 1
        self.k5 = self.k4 + pn.rest - 1

    @staticmethod
    def scratch(pn, n, shared):
        return [pltpu.VMEM((2, pn.rest, n, 8, 128), BF16), pltpu.VMEM((pn.rest, n, 8, 128), BF16), pltpu.VMEM((pn.rest - 1, n, 8, 128), BF16),
                pltpu.SemaphoreType.DMA((2, 2 * pn.rest + pn.ns - 1))] + (
            [] if shared else [pltpu.VMEM((pn.ns - 1, n, 8, 128), BF16), pltpu.VMEM((2, pn.rest, n, 8, 128), BF16)])

    def here(self, z):
        return (z >= self.k0) & (z < self.k1)

    def c1(self):
        r, c, z = place()
        return remote(self.src.at[1 - c], self.r1, self.sems, 0, peer(r, 1 - c))

    def start1(self):
        self.c1().start()

    def owners(self, i, other):
        r, c, z = place()
        bits = [lax.shift_right_arithmetic(r, b) & 1 for b in range(len(self.steps))]
        done, b, free = self.steps[:i], self.steps[i], self.steps[i + 1:]
        base = sum((bits[d] * (1 << d) for d in done), jnp.int32(0))
        base = base + (1 - bits[b] if other else bits[b]) * (1 << b)
        out = [base + sum(((q >> n) & 1) << f for n, f in enumerate(free)) for q in range(1 << len(free))]
        slot = sum(self.pn.rest >> (k + 1) for k in range(i))
        return out, slot

    def c2(self, i, q):
        r, c, z = place()
        own, slot = self.owners(i, True)
        b = self.steps[i]
        bit = lax.shift_right_arithmetic(r, b) & 1
        to = r + (1 - 2 * bit) * (1 << b)
        return remote(self.src.at[c, own[q]], self.r2.at[slot + q], self.sems, self.k2 + slot + q, peer(to, c))

    def add(self, owner, term):
        r, c, z = place()
        self.src[c, owner] = (self.src[c, owner].astype(F32) + term.astype(F32)).astype(BF16)

    def start2(self):
        self.c1().wait()
        for q, owner in enumerate(self.owners(0, True)[0]):
            self.add(owner, self.r1[owner])
            self.c2(0, q).start()
        for owner in self.owners(0, False)[0]:
            self.add(owner, self.r1[owner])

    def landed(self, i):
        own, slot = self.owners(i, False)
        for q in range(len(own)):
            self.c2(i, q).wait()
        for q, owner in enumerate(own):
            self.add(owner, self.r2[slot + q])

    def halve(self):
        for i in range(1, len(self.steps)):
            self.landed(i - 1)
            for q in range(len(self.owners(i, True)[0])):
                self.c2(i, q).start()

    def c3(self, j):
        r, c, z = place()
        to = lax.rem(z + j, self.pn.ns)
        return to, remote(self.src.at[c, r], self.r3.at[j - 1], self.sems, self.k3 + j - 1, {"opt": to})

    def start3(self):
        r, c, z = place()
        self.landed(len(self.steps) - 1)
        for j in range(1, self.pn.ns):
            to, cp = self.c3(j)

            @pl.when(self.here(to))
            def _():
                cp.start()

    def c4(self, j):
        r, c, z = place()
        return remote(self.ag.at[c, r], self.ag.at[c, r], self.sems, self.k4 + j - 1, peer(lax.rem(r + j, self.pn.rest), c))

    def start4(self):
        r, c, z = place()
        for j in range(1, self.pn.ns):
            to, cp = self.c3(j)

            @pl.when(self.here(to))
            def _():
                cp.wait_send()

        @pl.when(self.here(z))
        def _():
            for j in range(1, self.pn.ns):
                self.c3(j)[1].wait_recv()
            v = self.src[c, r].astype(F32)
            for j in range(1, self.pn.ns):
                v = v + self.r3[j - 1].astype(F32)
            self.ag[c, r] = v.astype(BF16)
            for j in range(1, self.pn.rest):
                self.c4(j).start()

    def c5(self):
        r, c, z = place()
        return remote(self.ag.at[c], self.ag.at[c], self.sems, self.k5, peer(r, 1 - c))

    def start5(self):
        r, c, z = place()

        @pl.when(self.here(z))
        def _():
            for j in range(1, self.pn.rest):
                self.c4(j).wait()
            self.c5().start()

    def finish(self):
        r, c, z = place()

        @pl.when(self.here(z))
        def _():
            self.c5().wait()


SMALL = (0, 769, 770, 771, 772)


class Small:
    def __init__(self, pn, own, r1, mid, r2, sems):
        self.pn, self.own, self.r1, self.mid, self.r2, self.sems = pn, own, r1, mid, r2, sems

    @staticmethod
    def scratch(pn):
        u = len(SMALL)
        return [pltpu.VMEM((u, 8, 128), BF16), pltpu.VMEM((pn.ndp, u, 8, 128), BF16), pltpu.VMEM((u, 8, 128), BF16), pltpu.VMEM((pn.ns, u, 8, 128), BF16),
                pltpu.SemaphoreType.DMA((2, pn.ndp + pn.ns - 2))]

    def c1(self, j):
        me = lax.axis_index("dp")
        return remote(self.own, self.r1.at[me], self.sems, j - 1, {"dp": lax.rem(me + j, self.pn.ndp)})

    def w1(self, j):
        me = lax.axis_index("dp")
        return remote(self.own, self.r1.at[lax.rem(me - j + self.pn.ndp, self.pn.ndp)], self.sems, j - 1, {"dp": lax.rem(me + j, self.pn.ndp)})

    def start1(self):
        me = lax.axis_index("dp")
        for j in range(1, self.pn.ndp):
            self.c1(j).start()
        self.r1[me] = self.own[...]

    def c2(self, j):
        z = lax.axis_index("opt")
        to = lax.rem(z + j, self.pn.ns)
        return to, remote(self.mid, self.r2.at[z], self.sems, self.pn.ndp - 2 + j, {"opt": to})

    def w2(self, j):
        z = lax.axis_index("opt")
        return remote(self.mid, self.r2.at[lax.rem(z - j + self.pn.ns, self.pn.ns)], self.sems, self.pn.ndp - 2 + j, {"opt": lax.rem(z + j, self.pn.ns)})

    def start2(self):
        z = lax.axis_index("opt")
        for j in range(1, self.pn.ndp):
            self.c1(j).wait_send()
            self.w1(j).wait_recv()
        v = self.r1[0].astype(F32)
        for n in range(1, self.pn.ndp):
            v = v + self.r1[n].astype(F32)
        self.mid[...] = v.astype(BF16)
        for j in range(1, self.pn.ns):
            to, cp = self.c2(j)

            @pl.when(to <= self.pn.ka)
            def _():
                cp.start()
        self.r2[z] = v.astype(BF16)

    def finish(self):
        z = lax.axis_index("opt")
        for j in range(1, self.pn.ns):
            to, cp = self.c2(j)

            @pl.when(to <= self.pn.ka)
            def _():
                cp.wait_send()

            @pl.when(z <= self.pn.ka)
            def _():
                self.w2(j).wait_recv()

    def total(self, n):
        v = self.r2[0, n].astype(F32)
        for k in range(1, self.pn.ns):
            v = v + self.r2[k, n].astype(F32)
        return v.astype(BF16).astype(F32)


BM = 784
NSEMS = 32


def put_rows_grad(fs, start, v):
    put_rows(fs, start, v)


def kernel_bc(pn, x_hbm, cot_hbm, ob_hbm, wp_hbm, w1_hbm, w2_hbm, hwt_hbm, qkv_hbm, p_hbm, wqkv_hbm, vec, rel_ref, counts,
              y_hbm, dx_hbm, g_hbm, *refs):
    refs = list(refs)
    dx1, wp, acc, dsem = refs[:4]
    refs = refs[4:]
    chunks = []
    nb = 2 * (pn.ns - pn.ka)
    for n, (k0, k1, m, at, flip) in enumerate(part_list(pn)):
        if 1 < n < nb:
            refs[4:4] = [chunks[n % 2].r3, chunks[n % 2].ag]
        chunks.append(Chunk(pn, k0, k1, m, at, flip, *refs[:6]))
        refs = refs[6:]
    shards, ac = chunks[:nb], chunks[nb:]
    his = [ch for ch in shards if ch.k0 >= pn.kh]
    los = [ch for ch in shards if ch.k0 < pn.kh]
    mids, last = los[:-2], los[-2:]

    def each(chs, name):
        return tuple(getattr(ch, name) for ch in chs)

    def run(fns):
        for f in fns:
            f()
    small = Small(pn, *refs)
    count = counts[0]

    def local(n, src, dst):
        return pltpu.make_async_copy(src, dst, dsem.at[n])

    def mlp(x_v, dy_v, ob, a, du, h2, w1, w2, fs, xsem, csem):
        ins = [local(n, s, d) for n, (s, d) in enumerate([(ob_hbm, ob), (wp_hbm, wp), (w1_hbm, w1), (w2_hbm, w2)])]
        cps = window_copies(x_hbm, x_v, xsem, True) + window_copies(cot_hbm, dy_v, csem, True)
        for cp in cps + ins:
            cp.start()
        acc[...] = jnp.zeros_like(acc)
        bp, g2, b2, c2 = (vec[n:n + 1, :] for n in range(4, 8))
        enter(pn, True)
        for cp in cps + ins:
            cp.wait()
        nb = BM // 56

        def rows(t, _):
            r0 = pl.multiple_of(t * BM, BM)
            x = x_v[pl.ds(nb * t, nb)].reshape(BM, D).astype(F32)
            alive = lax.broadcasted_iota(jnp.int32, (nb, 7, 8, D), 2) < count
            dy = jnp.where(alive, dy_v[pl.ds(nb * t, nb)].astype(F32), 0.0)
            dyb = dy.astype(BF16)
            dy_v[pl.ds(nb * t, nb)] = dyb
            dy = dy.reshape(BM, D)
            dyb = dyb.reshape(BM, D)
            x1 = x + dot(ob[pl.ds(r0, BM), :], wp[...]) + bp
            xhat, r = norm_stats(x1)
            h = (xhat * g2 + b2).astype(BF16)
            h2[pl.ds(r0, BM), :] = h
            y = x1 + c2
            dh = jnp.zeros((BM, D), F32)
            for j in range(HID // CH):
                cs = slice(j * CH, (j + 1) * CH)
                u = dot(h, w1[:, cs]) + vec[8 + j:9 + j, :]
                cdf, pdf = gelu_parts(u)
                av = (u * cdf).astype(BF16)
                a[pl.ds(r0, BM), cs] = av
                y = y + dot(av, w2[cs, :])
                da = dot_nt(dyb, w2[cs, :])
                duv = da * (cdf + u * pdf)
                acc_rows(acc, 4 + j, duv)
                dub = duv.astype(BF16)
                du[pl.ds(r0, BM), cs] = dub
                dh = dh + dot_nt(dub, w1[:, cs])
            x_v[pl.ds(nb * t, nb)] = y.reshape(nb, 7, 8, D).astype(BF16)
            acc_rows(acc, 0, dy)
            acc_rows(acc, 1, dh * xhat)
            acc_rows(acc, 2, dh)
            dg = dh * g2
            dt = r * (dg - jnp.mean(dg, -1, keepdims=True) - xhat * jnp.mean(dg * xhat, -1, keepdims=True))
            dxv = dy + dt
            acc_rows(acc, 3, dxv)
            dx1[pl.ds(nb * t, nb)] = dxv.reshape(nb, 7, 8, D)
            return 0
        lax.fori_loop(0, ROWS // BM, rows, 0)
        ycs = window_copies(y_hbm, x_v, xsem, False)
        for cp in ycs:
            cp.start()
        vg = jnp.sum(acc[...].reshape(8, 8, D), 1)
        first = pn.base * 8
        nrow = pn.bunits * 8
        lo_row = (R_PROJ // 8 + 1) * 8 - first
        hi_row = R_END // 8 * 8 - first
        fs[0:lo_row, :] = jnp.zeros((lo_row, 128), F32)
        fs[hi_row:nrow, :] = jnp.zeros((nrow - hi_row, 128), F32)
        dyf = dy_v[...].reshape(ROWS, D)

        def w2rows(t, _):
            r0 = pl.multiple_of(t * 512, 512)
            v = dot_tn(a[:, pl.ds(r0, 512)], dyf)
            put_tile(fs, R_W2 - first + r0 * 4, 4, [v[:, c * 128:(c + 1) * 128] for c in range(4)])
            return 0
        lax.fori_loop(0, HID // 512, w2rows, 0)
        put_vec(fs, R_C2 - first, vg[0:1])

        def fill(ch):
            def piece(p, _):
                row = pl.multiple_of(((ch.k0 - pn.ka) * pn.units + p * pn.pc + ch.at) * 8, 8)
                ch.src[p & 1, lax.shift_right_arithmetic(p, 1)] = fs[pl.ds(row, ch.n * 8), :].reshape(ch.n, 8, 128).astype(BF16)
                return 0
            lax.fori_loop(0, pn.ndp, piece, 0)
            ch.start1()
        for ch in his:
            fill(ch)
        h2t = a.at[0:D, 0:1664]
        transpose_rows(h2, h2t)

        lane = lax.broadcasted_iota(jnp.int32, (D, 128), 1)
        at = R_W1 - first
        keep = fs[pl.ds(at, 1), :]

        def w1rows(t, before):
            r0 = pl.multiple_of(t * 512, 512)
            u = dot(h2t[:, 0:ROWS], du[:, pl.ds(r0, 512)])
            v = shifted([u[:, c * 128:(c + 1) * 128] for c in range(4)])
            for c in range(4):
                fs[pl.ds(at + 4 * t + c, D, stride=16), :] = jnp.where(lane >= LANE, v[c], before if c == 0 else v[c - 1])
            return v[3]
        v = lax.fori_loop(0, HID // 512, w1rows, jnp.zeros((D, 128), F32))
        one = lax.broadcasted_iota(jnp.int32, (1, 128), 1)
        v = jnp.where(lax.broadcasted_iota(jnp.int32, (D, 128), 0) == 0, keep, pltpu.roll(v, 1, 0)), v[D - 1:D]
        fs[pl.ds(at, D, stride=16), :] = jnp.where(lane < LANE, v[0], fs[pl.ds(at, D, stride=16), :])
        fs[pl.ds(at + D * 16, 1), :] = jnp.where(one < LANE, v[1], fs[pl.ds(at + D * 16, 1), :])
        run(each(his, 'start2'))
        v = dot_tn(ob[...], dx1[...].reshape(ROWS, D).astype(BF16))
        put_tile(fs, R_PROJ - first, 4, [v[:, c * 128:(c + 1) * 128] for c in range(4)])
        for row, n in ((R_BP, 3), (R_G2, 1), (R_B2, 2)):
            put_vec(fs, row - first, vg[n:n + 1])
        for j in range(4):
            put_vec(fs, R_C1 - first + 4 * j, vg[4 + j:5 + j])
        for ch in los:
            fill(ch)
        for cp in ycs:
            cp.wait()

    big = pltpu.VMEM((28, 7, 8, D), BF16)
    pl.run_scoped(mlp, big, big, pltpu.VMEM((ROWS, D), BF16), pltpu.VMEM((ROWS, HID), BF16), pltpu.VMEM((ROWS, HID), BF16), pltpu.VMEM((ROWS, D), BF16),
                  pltpu.VMEM((D, HID), BF16), pltpu.VMEM((HID, D), BF16), pltpu.VMEM((pn.bunits * 8, 128), F32),
                  pltpu.SemaphoreType.DMA((NSEG,)), pltpu.SemaphoreType.DMA((NSEG,)))

    def attention(x_v, qkvb, pb, hwt, wqkv, fs, os_, dq, dtab, xsem):
        ins = [local(n, s, d) for n, (s, d) in enumerate([(qkv_hbm, qkvb), (p_hbm, pb), (hwt_hbm, hwt), (wqkv_hbm, wqkv)])]
        for cp in ins:
            cp.start()
        cps = window_copies(x_hbm, x_v, xsem, True)
        for cp in cps:
            cp.start()
        acc[...] = jnp.zeros_like(acc)
        dtab[...] = jnp.zeros_like(dtab)

        def rows0(t, _):
            r0 = pl.multiple_of(t * 392, 8)
            ev = dx1[pl.ds(7 * t, 7)].reshape(392, D).astype(BF16)
            v = dot_nt(ev, wp[...])
            for g in range(4):
                os_[pl.ds(g * RS + r0, 392), :] = v[:, g * 128:(g + 1) * 128]
            return 0
        lax.fori_loop(0, 4, rows0, 0)
        ins[0].wait()
        ins[1].wait()
        run(each(his, 'halve') + each(los, 'start2'))
        heads = lane_head()

        def several(g, items):
            bases = [lax.shift_right_arithmetic(i, 3) * WROWS + (i & 7) for i in items]
            dobds = [block_diag(take_rows(os_, g * RS + base).astype(BF16), heads) for base in bases]
            dps = [dot_nt(qkvb[i, 8 + g], d) for i, d in zip(items, dobds)]
            total = dtab[g]
            dsbs = []
            for i, dp in zip(items, dps):
                p = pb[i, g].astype(F32)
                t = p * dp
                ds = t - p * jnp.sum(t, 0, keepdims=True)
                total = total + ds
                dsbs.append(ds.astype(BF16))
            dtab[g] = total
            dvs = [dot(pb[i, g], d) for i, d in zip(items, dobds)]
            dks = [dot(d, block_diag(qkvb[i, g], heads)) for i, d in zip(items, dsbs)]
            dqs = [dot_tn(d, qkvb[i, 4 + g]) for i, d in zip(items, dsbs)]
            for base, dv, dk, dqv in zip(bases, dvs, dks, dqs):
                put_rows(fs, 2 * RS + base, dv)
                put_rows(fs, RS + base, dk)
                put_rows(fs, base, diag_sum(dqv, heads) * SCALE)

        mid = {0: each(his, 'start3'), 1: each(mids, 'halve') + (ac[0].start2,), 2: each(last, 'halve') + (ac[1].start2,) + each(his, 'start4'),
               3: each(mids, 'start3') + (ac[0].halve, ac[2].start2)}
        for g in range(4):
            def attend(t, _):
                @pl.when(t == 1)
                def _():
                    for f in mid[g]:
                        f()
                several(g, [16 * t + n for n in range(16)])
                return 0
            lax.fori_loop(0, WB // 16, attend, 0)
            parts = []
            for n in range(3):
                v = fs[n * RS:n * RS + ROWS, :]
                if n != 1:
                    acc[8 * (2 + n // 2):8 * (3 + n // 2), g * 128:(g + 1) * 128] = jnp.sum(v.reshape(ROWS // 8, 8, 128), 0)
                v = v.astype(BF16)
                dq[:, n * D + g * 128:n * D + (g + 1) * 128] = v
                parts.append(v)
            if g == 0:
                ins[2].wait()
                ins[3].wait()
            v = dot(hwt[...], jnp.concatenate(parts, 1))
            mu = pn.mrow // 8
            for n in range(3):
                u = v[:, n * 128:(n + 1) * 128].reshape(D // 8, 8, 128).astype(BF16)
                for p in range(pn.ndp):
                    ac[g].src[p & 1, p >> 1, n * mu:(n + 1) * mu] = u[p * mu:(p + 1) * mu]
            ac[g].start1()
        run(each(last, 'start3'))
        for cp in cps:
            cp.wait()
        gain = vec[0:1, :]
        tab = table_grad(rel_ref, os_, dtab)
        for n in range(3):
            small.own[2 + n] = tab[8 * n:8 * n + 8].astype(BF16)
        late = {0: (ac[0].start3,), 1: (ac[3].start2, ac[1].halve), 2: (ac[1].start3, ac[2].halve) + each(his, 'start5'), 3: each(mids, 'start4') + (ac[3].halve,),
                4: (ac[2].start3,), 5: (ac[3].start3, ac[0].start4), 6: (ac[1].start4,) + each(mids, 'start5')}

        def rows1(t, _):
            for k, fns in late.items():
                @pl.when(t == k)
                def _():
                    for f in fns:
                        f()
            r0 = pl.multiple_of(t * BLK, BLK)
            dn = dot_nt(dq[pl.ds(r0, BLK), :], wqkv[...])
            x = x_v[pl.ds(4 * t, 4)].reshape(BLK, D).astype(F32)
            xhat, r = norm_stats(x)
            acc_rows(acc, 0, dn * xhat)
            acc_rows(acc, 1, dn)
            dg = dn * gain
            dt = r * (dg - jnp.mean(dg, -1, keepdims=True) - xhat * jnp.mean(dg * xhat, -1, keepdims=True))
            dx1[pl.ds(4 * t, 4)] += dt.reshape(4, 7, 8, D)
            return 0
        lax.fori_loop(0, NBLK, rows1, 0)
        vg = jnp.sum(acc[...].reshape(8, 8, D), 1)
        flat = [vg[n:n + 1, c * 128:(c + 1) * 128] for n in range(4) for c in range(4)]
        small.own[0] = jnp.concatenate(flat[:8], 0).astype(BF16)
        small.own[1] = jnp.concatenate(flat[8:], 0).astype(BF16)
        small.start1()
        ycs = window_copies(dx_hbm, dx1, xsem, False)
        for cp in ycs:
            cp.start()
        run(each(last, 'start4') + (ac[2].start4, ac[3].start4, ac[0].start5, ac[1].start5, small.start2) + each(last, 'start5') + (ac[2].start5, ac[3].start5))
        for ch in chunks:
            ch.finish()
        r, c, z = place()
        g = os_

        @pl.when(z >= pn.ka)
        def _():
            def piece(p, _):
                for ch in shards[:2]:
                    g[pl.ds(pl.multiple_of((p * pn.pc + ch.at) * 8, 8), ch.n * 8), :] = ch.ag[p & 1, lax.shift_right_arithmetic(p, 1)].astype(F32).reshape(ch.n * 8, 128)
                return 0
            lax.fori_loop(0, pn.ndp, piece, 0)
        mu = pn.mrow // 8

        @pl.when(z < pn.ka)
        def _():
            def piece(p, _):
                for h in range(4):
                    for n in range(3):
                        v = ac[h].ag[p & 1, lax.shift_right_arithmetic(p, 1), n * mu:(n + 1) * mu].astype(F32).reshape(pn.mrow, 128)
                        g[pl.ds(R_QKV + p * pn.mrow * 12 + n * 4 + h, pn.mrow, stride=12), :] = v
                return 0
            lax.fori_loop(0, pn.ndp, piece, 0)
        small.finish()

        @pl.when(z < pn.ka)
        def _():
            for n, u in enumerate(SMALL):
                g[u * 8:u * 8 + 8, :] = small.total(n)

        @pl.when(z == pn.ka)
        def _():
            for n, u in enumerate(SMALL):
                if u >= pn.base:
                    k = (u - pn.base) * 8
                    g[k:k + 8, :] += small.total(n)
        out = local(0, g.at[pl.ds(pl.multiple_of(lax.select(z < pn.ka, z * (pn.units * 8), 0), 8), pn.units * 8)], g_hbm)
        out.start()
        out.wait()
        for cp in ycs:
            cp.wait()

    pl.run_scoped(attention, big, pltpu.VMEM((WB, 12, 64, 128), BF16), pltpu.VMEM((WB, 4, 64, 256), BF16), pltpu.VMEM((D, ROWS), BF16), pltpu.VMEM((D, 3 * D), BF16),
                  pltpu.VMEM((3 * RS, 128), F32), pltpu.VMEM((max(4 * RS, pn.gunits * 8), 128), F32), pltpu.VMEM((ROWS, 3 * D), BF16), pltpu.VMEM((4, 64, 256), F32), pltpu.SemaphoreType.DMA((NSEG,)))


def part_list(pn):
    mu = 3 * pn.mrow // 8
    h = (pn.pc + 1) // 2
    out = []
    for k in range(pn.ns - 1, pn.ka - 1, -1):
        out += [(k, k + 1, h, 0, False), (k, k + 1, pn.pc - h, h, True)]
    return out + [(0, pn.ka, mu, 0, g % 2 == 1) for g in range(4)]


def call_bc(pn, x, cot, ob, wp, w1, w2, hwt, qkv, p, wqkv, vec, rel, counts):
    any_ = pl.BlockSpec(memory_space=pl.ANY)
    vm = pl.BlockSpec(memory_space=pltpu.VMEM)
    sds = jax.ShapeDtypeStruct
    outs = [sds((14, 14, 8, D), BF16), sds((14, 14, 8, D), F32), sds((pn.units * 8, 128), F32)]
    scratch = [pltpu.VMEM((28, 7, 8, D), F32), pltpu.VMEM((D, D), BF16), pltpu.VMEM((64, D), F32), pltpu.SemaphoreType.DMA((4,))]
    for n, (k0, k1, m, at, flip) in enumerate(part_list(pn)):
        scratch += Chunk.scratch(pn, m, 1 < n < 2 * (pn.ns - pn.ka))
    scratch += Small.scratch(pn)
    return pl.pallas_call(
        functools.partial(kernel_bc, pn),
        out_shape=outs,
        in_specs=[any_] * 10 + [vm, vm, pl.BlockSpec(memory_space=pltpu.SMEM)],
        out_specs=[any_] * 3,
        scratch_shapes=scratch,
        compiler_params=pltpu.CompilerParams(vmem_limit_bytes=67000000, collective_id=1, has_side_effects=True),
        name="back",
    )(x, cot, ob, wp, w1, w2, hwt, qkv, p, wqkv, vec, rel, counts)


STEP = 2
DECAYED = (2, 6, 10, 12)
LENGTHS = [D, D, 3 * D * D, D, D, TAB * HEADS, D * D, D, D, D, D * HID, HID, HID * D, D]
AU = 128


def kernel_adam(rates, first, g, p, m1, m2, g_o, p_o, m_o, v_o):
    shape = (AU, 8, 128)
    u0 = first[0] + pl.program_id(0) * AU
    starts = [sum(LENGTHS[:n + 1]) for n in range(len(LENGTHS))]

    def group(at):
        k = jnp.int32(0)
        for s in starts:
            k = k + (at >= s).astype(jnp.int32)
        return k

    def update(rate, decay):
        grad = g[...]
        w = p[...]
        m = 0.9 * m1[...] + 0.1 * grad
        v = 0.999 * m2[...] + 0.001 * grad * grad
        mh = m / (1.0 - 0.9 ** STEP)
        vh = v / (1.0 - 0.999 ** STEP)
        p_o[...] = w - rate * (mh / (jnp.sqrt(vh) + 1e-08) + decay * w)
        m_o[...] = m
        v_o[...] = v
        g_o[...] = grad
    k0 = group(u0 * 1024)
    k1 = group((u0 + AU) * 1024 - 1)

    @pl.when(k0 == k1)
    def _():
        decay = jnp.float32(0.0)
        for n in DECAYED:
            decay = jnp.where(k0 == n, jnp.float32(0.05), decay)
        update(rates[k0], decay)

    @pl.when(k0 != k1)
    def _():
        index = ((u0 + lax.broadcasted_iota(jnp.int32, shape, 0)) * 8 + lax.broadcasted_iota(jnp.int32, shape, 1)) * 128 + lax.broadcasted_iota(jnp.int32, shape, 2)
        rate = jnp.zeros(shape, F32) + rates[0]
        decay = jnp.zeros(shape, F32)
        for n, s in enumerate(starts):
            after = index >= s
            rate = jnp.where(after, rates[n + 1], rate)
            if n in DECAYED or n + 1 in DECAYED:
                decay = jnp.where(after, 0.05 if n + 1 in DECAYED else 0.0, decay)
        update(rate, decay)


def call_adam(pn, rates, g, params, mom1, mom2):
    view = lambda t: t.reshape(pn.units, 8, 128)
    spec = pl.BlockSpec((AU, 8, 128), lambda i: (i, 0, 0))
    sm = pl.BlockSpec(memory_space=pltpu.SMEM)
    first = (lax.axis_index("opt") * pn.units).astype(jnp.int32).reshape(1)
    out = pl.pallas_call(
        kernel_adam,
        grid=(pl.cdiv(pn.units, AU),),
        out_shape=[jax.ShapeDtypeStruct((pn.units, 8, 128), F32)] * 4,
        in_specs=[sm, sm] + [spec] * 4,
        out_specs=[spec] * 4,
        compiler_params=pltpu.CompilerParams(vmem_limit_bytes=67043328),
        name="adamw",
    )(rates, first, view(g), view(params), view(mom1), view(mom2))
    return [t.reshape(-1) for t in out]


from jax.sharding import PartitionSpec as P


def solution(mesh):
    def local(images, cotangent, counts, rel_index, params, moment1, moment2, rates):
        pn = Plan(mesh, params.shape[0])
        xt = images.transpose(1, 2, 0, 3)
        ct = cotangent.transpose(1, 2, 0, 3)
        rel = rel_lanes(rel_index)
        wqkv, wp, w1, w2, vec, hwt, ob, qkv, p = call_a(pn, xt, params, rel)
        y, dx, g = call_bc(pn, xt, ct, ob, wp, w1, w2, hwt, qkv, p, wqkv, vec, rel, counts)
        grad, new_params, new_first, new_second = call_adam(pn, rates, g, params, moment1, moment2)
        return (y.transpose(2, 0, 1, 3), dx.transpose(2, 0, 1, 3), grad, new_params, new_first, new_second)

    split = P(("dp", "opt"), None, None, None)
    return jax.shard_map(
        local, mesh=mesh,
        in_specs=(split, split, P(("dp", "opt")), P(), P("opt"), P("opt"), P("opt"), P()),
        out_specs=(split, split, P("opt"), P("opt"), P("opt"), P("opt")),
        check_vma=False)
```

```python
import functools
import jax
import jax.numpy as jnp
from jax import lax
from jax.experimental import pallas as pl
from jax.experimental.pallas import tpu as pltpu

D = 512
HEADS = 16
HEAD_DIM = 32
HID = 2048
SIDE = 14
WIN = 7
SHIFT = 3
TAB = 169
F32 = jnp.float32
BF16 = jnp.bfloat16

IMGS = 8
SPAN = WIN * WIN
WROWS = SPAN * IMGS
ROWS = 4 * WROWS
RS = ROWS + 64
BLK = 224
NBLK = ROWS // BLK
BM = 784
WB = 4 * IMGS
SCALE = HEAD_DIM ** -0.5

R_G1, R_B1, R_QKV, R_BQ, R_BV, R_TAB = 0, 4, 8, 6152, 6156, 6160
R_PROJ, R_BP, R_G2, R_B2, R_W1, R_C1, R_W2, R_C2, R_END = 6181, 8229, 8233, 8237, 8241, 16433, 16449, 24641, 24645
LANE = 16
BROW = 6176


def segments(w):
    if w == 0:
        return [(SHIFT, WIN, 0)]
    return [(WIN + SHIFT, WIN - SHIFT, 0), (0, SHIFT, WIN - SHIFT)]


def window_copies(hbm, vmem, sem, inward):
    out = []
    n = 0
    for wy in range(2):
        for wx in range(2):
            for ys, yl, yo in segments(wy):
                for xs, xl, xo in segments(wx):
                    a = hbm.at[pl.ds(ys, yl), pl.ds(xs, xl)]
                    b = vmem.at[pl.ds((2 * wy + wx) * WIN + yo, yl), pl.ds(xo, xl)]
                    out.append(pltpu.make_async_copy(a, b, sem.at[n]) if inward else pltpu.make_async_copy(b, a, sem.at[n]))
                    n += 1
    return out


NSEG = 9


def dot(a, b):
    return lax.dot_general(a, b, (((1,), (0,)), ((), ())), preferred_element_type=F32)


def dot_nt(a, b):
    return lax.dot_general(a, b, (((1,), (1,)), ((), ())), preferred_element_type=F32)


def dot_tn(a, b):
    return lax.dot_general(a, b, (((0,), (0,)), ((), ())), preferred_element_type=F32)


def norm_stats(x):
    mean = jnp.mean(x, -1, keepdims=True)
    dev = x - mean
    var = jnp.mean(dev * dev, -1, keepdims=True)
    r = lax.rsqrt(var + 1e-05)
    return dev * r, r


def pieces_to_rows(pn, wb, fs, shard, count, base):
    def body(p, _):
        row = pl.multiple_of((shard * pn.units - base + p * pn.pc) * 8, 8)
        fs[pl.ds(row, pn.pc * 8), :] = wb[shard, p & 1, lax.shift_right_arithmetic(p, 1)].astype(F32).reshape(pn.pc * 8, 128)
        return 0
    lax.fori_loop(0, count, body, 0)


def vec_from(fs, row, width, shift):
    parts = []
    lane = lax.broadcasted_iota(jnp.int32, (1, 128), 1)
    for c in range(width // 128):
        a = fs[pl.ds(row + c, 1), :]
        if shift:
            b = fs[pl.ds(row + c + 1, 1), :]
            a = jnp.where(lane < 128 - LANE, pltpu.roll(a, 128 - LANE, 1), pltpu.roll(b, 128 - LANE, 1))
        parts.append(a)
    return jnp.concatenate(parts, 1)


def take_matrix(fs, row, dst, nrows, ncb, shift, step=128):
    lane = lax.broadcasted_iota(jnp.int32, (step, 128), 1)

    def body(t, _):
        base = row + t * (step * ncb)
        r0 = pl.multiple_of(t * step, step)
        for c in range(ncb):
            a = fs[pl.ds(base + c, step, stride=ncb), :]
            if shift:
                b = fs[pl.ds(base + c + 1, step, stride=ncb), :]
                a = jnp.where(lane < 128 - LANE, pltpu.roll(a, 128 - LANE, 1), pltpu.roll(b, 128 - LANE, 1))
            dst[pl.ds(r0, step), c * 128:(c + 1) * 128] = a.astype(BF16)
        return 0

    lax.fori_loop(0, nrows // step, body, 0)


def transpose_rows(src, dst):
    full = ROWS // 128

    def body(t, _):
        r0 = pl.multiple_of(t * 128, 128)
        dst[:, pl.ds(r0, 128)] = src[pl.ds(r0, 128), :].T
        return 0
    lax.fori_loop(0, full, body, 0)
    if ROWS % 128:
        dst[:, full * 128:ROWS] = src[full * 128:ROWS, :].T


def lane_head():
    return lax.broadcasted_iota(jnp.int32, (64, 128), 1) // HEAD_DIM


def block_diag(v, heads):
    zero = jnp.zeros_like(v)
    return jnp.concatenate([jnp.where(heads == h, v, zero) for h in range(4)], 0)


def diag_sum(r, heads):
    out = r[0:64]
    for h in range(1, 4):
        out = jnp.where(heads == h, r[64 * h:64 * h + 64], out)
    return out


def take_rows(fs, start):
    v = fs[pl.ds(start, 56, stride=IMGS), :]
    v = jnp.where(lax.broadcasted_iota(jnp.int32, (56, 128), 0) < SPAN, v, 0.0)
    return jnp.concatenate([v, jnp.zeros((8, 128), F32)], 0)


def put_rows(fs, start, v):
    fs[pl.ds(start, 48, stride=IMGS), :] = v[0:48]
    fs[pl.ds(start + 48 * IMGS, 1), :] = v[48:49]


def build_bias(tab3, rel_ref, big, bias):
    rel = rel_ref[...]
    row = lax.shift_right_arithmetic(rel, 3)
    low = rel & 7
    oh = (lax.broadcasted_iota(jnp.int32, (32, 4096), 0) == row).astype(F32).astype(BF16)
    tab = jnp.concatenate([tab3, jnp.zeros((8, 128), F32)], 0).astype(BF16)
    r = dot_tn(tab, oh)
    acc = jnp.zeros((16, 4096), F32)
    for j in range(8):
        acc = acc + jnp.where(low == j, r[16 * j:16 * j + 16], 0.0)
    for kk in range(32):
        big[kk * 16:kk * 16 + 16, :] = acc[:, kk * 128:kk * 128 + 128]
    k = lax.broadcasted_iota(jnp.int32, (64, 256), 0)
    q = lax.broadcasted_iota(jnp.int32, (64, 256), 1) & 63
    ki = lax.shift_right_arithmetic(k * 37, 8)
    kj = k - ki * 7
    qi = lax.shift_right_arithmetic(q * 37, 8)
    qj = q - qi * 7
    cut = WIN - SHIFT
    same_y = (ki < cut) == (qi < cut)
    same_x = (kj < cut) == (qj < cut)
    lane = lax.broadcasted_iota(jnp.int32, (32, 128), 1)
    for g in range(4):
        for pair in range(2):
            h = 4 * g + 2 * pair
            a = big[pl.ds(h, 32, stride=16), :]
            b = big[pl.ds(h + 1, 32, stride=16), :]
            even = jnp.where(lane < 64, a, pltpu.roll(b, 64, 1))
            odd = jnp.where(lane < 64, pltpu.roll(a, 64, 1), b)
            big[pl.ds(1024 + g * 256 + pair * 128, 32, stride=2), :] = even
            big[pl.ds(1024 + g * 256 + pair * 128 + 1, 32, stride=2), :] = odd
    for g in range(4):
        pos = jnp.concatenate([big[1024 + g * 256:1024 + g * 256 + 64, :], big[1024 + g * 256 + 128:1024 + g * 256 + 192, :]], 1)
        for w in range(4):
            keep = None
            if w == 1:
                keep = same_x
            elif w == 2:
                keep = same_y
            elif w == 3:
                keep = same_y & same_x
            val = pos if keep is None else pos + jnp.where(keep, 0.0, -100.0)
            bias[w * 4 + g] = jnp.where(k < SPAN, val, -1e30)


MESH = pl.DeviceIdType.MESH
NMAT = 768


class Plan:
    def __init__(self, mesh, shard_len):
        self.ndp = mesh.shape["dp"]
        self.ns = mesh.shape["opt"]
        self.rest = self.ndp // 2
        self.units = shard_len // 1024
        self.pc = -(-self.units // self.ndp)
        self.ka = (BROW // 8) // self.units
        self.base = self.ka * self.units
        self.bunits = (self.ns - self.ka - 1) * self.units + self.ndp * self.pc
        self.kh = -(-(R_W2 // 8 + 1) // self.units)
        self.mrow = D // self.ndp
        self.gunits = max(BROW // 8 + 1, self.ndp * self.pc)


def place():
    me = lax.axis_index("dp")
    return lax.shift_right_arithmetic(me, 1), me & 1, lax.axis_index("opt")


def peer(r, c):
    return {"dp": 2 * r + c}


def enter(pn, all_dp=False):
    r, c, z = place()
    bar = pltpu.get_barrier_semaphore()
    pl.semaphore_signal(bar, inc=1, device_id=peer(r, 1 - c), device_id_type=MESH)
    for j in range(1, pn.rest):
        for to in ((c, 1 - c) if all_dp else (c,)):
            pl.semaphore_signal(bar, inc=1, device_id=peer(lax.rem(r + j, pn.rest), to), device_id_type=MESH)
    for j in range(1, pn.ns):
        pl.semaphore_signal(bar, inc=1, device_id={"opt": lax.rem(z + j, pn.ns)}, device_id_type=MESH)
    pl.semaphore_wait(bar, (pn.ndp - 1 if all_dp else pn.rest) + pn.ns - 1)


def remote(src, dst, sems, n, where):
    return pltpu.make_async_remote_copy(src_ref=src, dst_ref=dst, send_sem=sems.at[0, n], recv_sem=sems.at[1, n], device_id=where, device_id_type=MESH)


class Gather:
    def __init__(self, pn, wb, osem, xsem, ysem):
        self.pn, self.wb, self.osem, self.xsem, self.ysem = pn, wb, osem, xsem, ysem
        h = (pn.pc + 1) // 2
        self.parts = [pl.ds(0, h), pl.ds(h, pn.pc - h)]

    @staticmethod
    def scratch(pn):
        return [pltpu.VMEM((pn.ns, 2, pn.rest, pn.pc, 8, 128), BF16), pltpu.SemaphoreType.DMA((2, 2 * pn.ns)),
                pltpu.SemaphoreType.DMA((2, 2 * pn.ns * pn.rest)), pltpu.SemaphoreType.DMA((2, 2 * pn.ns))]

    def o(self, j, h):
        r, c, z = place()
        own = self.wb.at[z, c, r, self.parts[h]]
        return pltpu.make_async_remote_copy(src_ref=own, dst_ref=own, send_sem=self.osem.at[0, 2 * j + h], recv_sem=self.osem.at[1, 2 * z + h],
                                            device_id={"opt": lax.rem(z + j, self.pn.ns)}, device_id_type=MESH)

    def arrived(self, s, h):
        r, c, z = place()
        own = self.wb.at[s, c, r, self.parts[h]]
        return pltpu.make_async_remote_copy(src_ref=own, dst_ref=own, send_sem=self.osem.at[0, h], recv_sem=self.osem.at[1, 2 * s + h],
                                            device_id={"opt": lax.rem(z + 1, self.pn.ns)}, device_id_type=MESH)

    def x(self, s, h, j):
        r, c, z = place()
        own = self.wb.at[s, c, r, self.parts[h]]
        return remote(own, own, self.xsem, (2 * s + h) * self.pn.rest + j, peer(lax.rem(r + j, self.pn.rest), c))

    def y(self, s, h):
        r, c, z = place()
        own = self.wb.at[s, c, :, self.parts[h]]
        return remote(own, own, self.ysem, 2 * s + h, peer(r, 1 - c))

    def start(self):
        for h in range(2):
            for j in range(1, self.pn.ns):
                self.o(j, h).start()

    def spread(self, s, h):
        r, c, z = place()

        @pl.when(z != s)
        def _():
            self.arrived(s, h).wait_recv()
            for j in range(1, self.pn.rest):
                self.x(s, h, j).start()

    def pair(self, s, h):
        r, c, z = place()

        @pl.when(z != s)
        def _():
            for j in range(1, self.pn.rest):
                self.x(s, h, j).wait_recv()
            self.y(s, h).start()

    def ready(self, s):
        r, c, z = place()

        @pl.when(z != s)
        def _():
            for h in range(2):
                self.y(s, h).wait_recv()

    def finish(self):
        r, c, z = place()
        for h in range(2):
            for j in range(1, self.pn.ns):
                self.o(j, h).wait_send()
            for s in range(self.pn.ns):
                @pl.when(z != s)
                def _():
                    for j in range(1, self.pn.rest):
                        self.x(s, h, j).wait_send()
                    self.y(s, h).wait_send()


def kernel_a(pn, x_hbm, params, rel_ref,
             wqkv_o, wp_o, w1_o, w2_o, vec_o, hw_o, ob_o, qkv_o, p_o,
             x_v, fs, os_, bias, wqkv, wp, w1, w2, vec, hw, hwt, ob, qkvb, pb, xsem, fsem, osem, wsem, flat_v, *gsems):
    cps = window_copies(x_hbm, x_v, xsem, True)
    for c in cps:
        c.start()
    r, c, z = place()
    gather = Gather(pn, flat_v, *gsems)
    fcp = pltpu.make_async_copy(params, fs.at[pl.ds(0, pn.units * 8)], fsem)
    fcp.start()
    enter(pn)
    fcp.wait()

    def cast(p):
        flat_v[z, p & 1, lax.shift_right_arithmetic(p, 1)] = fs[pl.ds(pl.multiple_of(p * pn.pc * 8, 8), pn.pc * 8), :].reshape(pn.pc, 8, 128).astype(BF16)
    me = lax.axis_index("dp")
    cast(me)
    gather.start()

    def others(j, _):
        cast(lax.rem(me + j, pn.ndp))
        return 0
    lax.fori_loop(1, pn.ndp, others, 0)
    for h in range(2):
        for k in range(pn.ka):
            gather.spread(k, h)
    for h in range(2):
        for k in range(pn.ka):
            gather.pair(k, h)
        gather.spread(pn.ka, h)
    for k in range(pn.ka):
        gather.ready(k)
    for k in range(pn.ka):
        pieces_to_rows(pn, flat_v, fs, k, pn.ndp, 0)
    take_matrix(fs, R_QKV, wqkv, D, 12, False)
    vec[0:1, :] = vec_from(fs, R_G1, D, False)
    vec[1:2, :] = vec_from(fs, R_B1, D, False)
    vec[2:3, :] = vec_from(fs, R_BQ, D, False)
    vec[3:4, :] = vec_from(fs, R_BV, D, False)
    wos = [pltpu.make_async_copy(wqkv, wqkv_o, wsem.at[0])]
    wos[0].start()
    for cp in cps:
        cp.wait()
    gain = vec[0:1, :]
    shift = vec[1:2, :]
    bq = vec[2:3, :]
    bv = vec[3:4, :]

    def rows(t, _):
        @pl.when(t == 0)
        def _():
            for k in range(pn.ka + 1, pn.ns):
                for h in range(2):
                    gather.spread(k, h)

        @pl.when(t == 1)
        def _():
            for h in range(2):
                gather.pair(pn.ka, h)
        r0 = pl.multiple_of(t * BM, BM)
        x = x_v[pl.ds(BM // 56 * t, BM // 56)].reshape(BM, D).astype(F32)
        xhat, _r = norm_stats(x)
        h = (xhat * gain + shift).astype(BF16)
        hw[pl.ds(r0, BM), :] = h
        for n in range(3):
            y = dot(h, wqkv[:, n * D:(n + 1) * D])
            if n == 0:
                y = (y + bq) * SCALE
            if n == 2:
                y = y + bv
            for c in range(4):
                fs[pl.ds((4 * n + c) * RS + r0, BM), :] = y[:, c * 128:(c + 1) * 128]
        return 0
    lax.fori_loop(0, ROWS // BM, rows, 0)
    gather.ready(pn.ka)
    tab = []
    for u in range(R_TAB // 8, R_TAB // 8 + 3):
        k, at = (pn.ka, u - pn.base) if u >= pn.base else (pn.ka - 1, u - pn.base + pn.units)
        p = at // pn.pc
        tab.append(flat_v[k, p & 1, p >> 1, at - p * pn.pc].astype(F32))
    build_bias(jnp.concatenate(tab, 0), rel_ref, os_, bias)
    heads = lane_head()

    def saved(t):
        four = pl.ds(4 * t, 4)
        return [pltpu.make_async_copy(qkvb.at[four], qkv_o.at[four], osem.at[2 + t]), pltpu.make_async_copy(pb.at[four], p_o.at[four], osem.at[2 + WB // 4 + t])]

    def attend(t, _):
        un = 4
        items = [(un * t + n, g) for n in range(un) for g in range(4)]
        ss = []
        vs = []
        for i, g in items:
            w = lax.shift_right_arithmetic(i, 3)
            base = w * WROWS + (i & 7)
            q = take_rows(fs, g * RS + base).astype(BF16)
            k = take_rows(fs, (4 + g) * RS + base).astype(BF16)
            v = take_rows(fs, (8 + g) * RS + base).astype(BF16)
            qkvb[i, g] = q
            qkvb[i, 4 + g] = k
            qkvb[i, 8 + g] = v
            vs.append(v)
            ss.append(dot_nt(k, block_diag(q, heads)) + bias[w * 4 + g])
        ps = []
        for (i, g), s in zip(items, ss):
            m = jnp.max(s, 0, keepdims=True)
            e = jnp.exp(s - m)
            p = (e * (1.0 / jnp.sum(e, 0, keepdims=True))).astype(BF16)
            pb[i, g] = p
            ps.append(p)
        for (i, g), p, v in zip(items, ps, vs):
            w = lax.shift_right_arithmetic(i, 3)
            base = w * WROWS + (i & 7)
            o = diag_sum(dot_tn(p, v), heads)
            put_rows(os_, g * RS + base, o)
        for cp in saved(t):
            cp.start()

        @pl.when(t == 2)
        def _():
            for k in range(pn.ka + 1, pn.ns):
                for h in range(2):
                    gather.pair(k, h)
        return 0
    lax.fori_loop(0, WB // 4, attend, 0)

    def outs(t, _):
        r0 = pl.multiple_of(t * BLK, BLK)
        for g in range(4):
            ob[pl.ds(r0, BLK), g * 128:(g + 1) * 128] = os_[pl.ds(g * RS + r0, BLK), :].astype(BF16)
        return 0
    lax.fori_loop(0, NBLK, outs, 0)
    transpose_rows(hw, hwt)
    cos = [pltpu.make_async_copy(a, b, osem.at[n]) for n, (a, b) in enumerate([(hwt, hw_o), (ob, ob_o)])]
    for cp in cos:
        cp.start()
    for k in range(pn.ka + 1, pn.ns):
        gather.ready(k)
    for k in range(pn.ka, pn.ns):
        pieces_to_rows(pn, flat_v, fs, k, pn.ndp, pn.base)
    first = pn.base * 8
    take_matrix(fs, R_PROJ - first, wp, D, 4, True)
    take_matrix(fs, R_W1 - first, w1, D, 16, True)
    take_matrix(fs, R_W2 - first, w2, HID, 4, True)
    for n, r in enumerate((R_BP, R_G2, R_B2, R_C2)):
        vec[4 + n:5 + n, :] = vec_from(fs, r - first, D, True)
    for n in range(4):
        vec[8 + n:9 + n, :] = vec_from(fs, R_C1 - first + 4 * n, D, True)
    for n, (a, b) in enumerate([(wp, wp_o), (w1, w1_o), (w2, w2_o), (vec, vec_o)]):
        wos.append(pltpu.make_async_copy(a, b, wsem.at[n + 1]))
        wos[-1].start()
    for t in range(WB // 4):
        cos += saved(t)
    for cp in cos + wos:
        cp.wait()
    gather.finish()


def call_a(pn, x, params, rel):
    any_ = pl.BlockSpec(memory_space=pl.ANY)
    sds = jax.ShapeDtypeStruct
    outs = [sds((D, 3 * D), BF16), sds((D, D), BF16), sds((D, HID), BF16), sds((HID, D), BF16), sds((16, D), F32),
            sds((D, ROWS), BF16), sds((ROWS, D), BF16), sds((WB, 12, 64, 128), BF16), sds((WB, 4, 64, 256), BF16)]
    return pl.pallas_call(
        functools.partial(kernel_a, pn),
        out_shape=outs,
        in_specs=[any_, any_, pl.BlockSpec(memory_space=pltpu.VMEM)],
        out_specs=[any_] * len(outs),
        scratch_shapes=[
            pltpu.VMEM((28, 7, 8, D), BF16), pltpu.VMEM((12 * RS, 128), F32), pltpu.VMEM((4 * RS, 128), F32),
            pltpu.VMEM((16, 64, 256), F32), pltpu.VMEM((D, 3 * D), BF16), pltpu.VMEM((D, D), BF16), pltpu.VMEM((D, HID), BF16), pltpu.VMEM((HID, D), BF16),
            pltpu.VMEM((16, D), F32), pltpu.VMEM((ROWS, D), BF16), pltpu.VMEM((D, ROWS), BF16), pltpu.VMEM((ROWS, D), BF16), pltpu.VMEM((WB, 12, 64, 128), BF16), pltpu.VMEM((WB, 4, 64, 256), BF16),
            pltpu.SemaphoreType.DMA((NSEG,)), pltpu.SemaphoreType.DMA, pltpu.SemaphoreType.DMA((2 + WB // 2,)), pltpu.SemaphoreType.DMA((5,)),
        ] + Gather.scratch(pn),
        compiler_params=pltpu.CompilerParams(vmem_limit_bytes=64000000, collective_id=0, has_side_effects=True),
        name="attend",
    )(x, params.reshape(pn.units * 8, 128), rel)


def rel_lanes(rel_index):
    t = jnp.full((64, 64), -1, jnp.int32).at[:SPAN, :SPAN].set(rel_index.T)
    return t.reshape(1, 4096)


CH = 512
INV_SQRT2 = 0.7071067811865476
INV_SQRT2PI = 0.3989422804014327


def gelu_parts(u):
    e = jnp.exp(u * u * -0.5)
    t = 1.0 / (1.0 + jnp.abs(u) * (0.3275911 * INV_SQRT2))
    half = t * (0.127414796 + t * (-0.142248368 + t * (0.7107068705 + t * (-0.7265760135 + t * 0.5307027145)))) * e
    cdf = jnp.where(u >= 0, 1.0 - half, half)
    return cdf, e * INV_SQRT2PI


def put_block(fs, start, stride, v):
    n = v.shape[0]
    lane = lax.broadcasted_iota(jnp.int32, (n, 128), 1)
    v = pltpu.roll(v, LANE, 1)
    here = pl.ds(start, n, stride=stride) if n > 1 else pl.ds(start, 1)
    fs[here, :] = jnp.where(lane >= LANE, v, fs[here, :])
    here = pl.ds(start + 1, n, stride=stride) if n > 1 else pl.ds(start + 1, 1)
    fs[here, :] = jnp.where(lane < LANE, v, fs[here, :])


def shifted(blocks):
    return [pltpu.roll(v, LANE, 1) for v in blocks]


def put_tile(fs, base, stride, blocks):
    n = blocks[0].shape[0]
    lane = lax.broadcasted_iota(jnp.int32, (n, 128), 1)
    head = lax.broadcasted_iota(jnp.int32, (n, 128), 0) == 0
    one = lax.broadcasted_iota(jnp.int32, (1, 128), 1)
    v = shifted(blocks)
    first = fs[pl.ds(base, 1), :]
    last = fs[pl.ds(base + n * stride, 1), :]
    before = jnp.where(head, first, pltpu.roll(v[-1], 1, 0))
    for c in range(len(blocks)):
        fs[pl.ds(base + c, n, stride=stride), :] = jnp.where(lane >= LANE, v[c], before if c == 0 else v[c - 1])
    fs[pl.ds(base + n * stride, 1), :] = jnp.where(one < LANE, v[-1][n - 1:n], last)


def put_vec(fs, row, v):
    for c in range(v.shape[1] // 128):
        put_block(fs, row + c, 1, v[:, c * 128:(c + 1) * 128])


def acc_rows(ref, i, v):
    ref[8 * i:8 * i + 8, 0:v.shape[1]] += jnp.sum(v.reshape(v.shape[0] // 8, 8, v.shape[1]), 0)


def table_grad(rel_ref, big, dtab):
    lane = lax.broadcasted_iota(jnp.int32, (32, 128), 1)
    for g in range(4):
        for pair in range(2):
            at = 1024 + g * 256 + pair * 128
            big[at:at + 64, :] = dtab[g, :, pair * 128:pair * 128 + 128]
    for g in range(4):
        for pair in range(2):
            at = 1024 + g * 256 + pair * 128
            even = big[pl.ds(at, 32, stride=2), :]
            odd = big[pl.ds(at + 1, 32, stride=2), :]
            h = 4 * g + 2 * pair
            big[pl.ds(h, 32, stride=16), :] = jnp.where(lane < 64, even, pltpu.roll(odd, 64, 1))
            big[pl.ds(h + 1, 32, stride=16), :] = jnp.where(lane < 64, pltpu.roll(even, 64, 1), odd)
    rel = rel_ref[...]
    row = lax.shift_right_arithmetic(rel, 3)
    low = rel & 7
    oh = (lax.broadcasted_iota(jnp.int32, (32, 4096), 0) == row).astype(F32).astype(BF16)
    grad = jnp.concatenate([big[kk * 16:kk * 16 + 16, :] for kk in range(32)], 1)
    out = jnp.zeros((32, 128), F32)
    high = grad.astype(BF16).astype(F32)
    for part in (high, grad - high):
        m = jnp.concatenate([jnp.where(low == j, part, 0.0) for j in range(8)], 0).astype(BF16)
        out = out + dot_nt(oh, m)
    return out


class Chunk:
    def __init__(self, pn, k0, k1, n, at, flip, src, r1, r2, sems, r3, ag):
        self.pn, self.k0, self.k1, self.n, self.at = pn, k0, k1, n, at
        self.steps = list(range(pn.rest.bit_length() - 1))
        if flip:
            self.steps.reverse()
        self.src, self.r1, self.r2, self.r3, self.ag, self.sems = src, r1, r2, r3, ag, sems
        self.k2 = 1
        self.k3 = self.k2 + pn.rest - 1
        self.k4 = self.k3 + pn.ns - 1
        self.k5 = self.k4 + pn.rest - 1

    @staticmethod
    def scratch(pn, n, shared):
        return [pltpu.VMEM((2, pn.rest, n, 8, 128), BF16), pltpu.VMEM((pn.rest, n, 8, 128), BF16), pltpu.VMEM((pn.rest - 1, n, 8, 128), BF16),
                pltpu.SemaphoreType.DMA((2, 2 * pn.rest + pn.ns - 1))] + (
            [] if shared else [pltpu.VMEM((pn.ns - 1, n, 8, 128), BF16), pltpu.VMEM((2, pn.rest, n, 8, 128), BF16)])

    def here(self, z):
        return (z >= self.k0) & (z < self.k1)

    def c1(self):
        r, c, z = place()
        return remote(self.src.at[1 - c], self.r1, self.sems, 0, peer(r, 1 - c))

    def start1(self):
        self.c1().start()

    def owners(self, i, other):
        r, c, z = place()
        bits = [lax.shift_right_arithmetic(r, b) & 1 for b in range(len(self.steps))]
        done, b, free = self.steps[:i], self.steps[i], self.steps[i + 1:]
        base = sum((bits[d] * (1 << d) for d in done), jnp.int32(0))
        base = base + (1 - bits[b] if other else bits[b]) * (1 << b)
        out = [base + sum(((q >> n) & 1) << f for n, f in enumerate(free)) for q in range(1 << len(free))]
        slot = sum(self.pn.rest >> (k + 1) for k in range(i))
        return out, slot

    def c2(self, i, q):
        r, c, z = place()
        own, slot = self.owners(i, True)
        b = self.steps[i]
        bit = lax.shift_right_arithmetic(r, b) & 1
        to = r + (1 - 2 * bit) * (1 << b)
        return remote(self.src.at[c, own[q]], self.r2.at[slot + q], self.sems, self.k2 + slot + q, peer(to, c))

    def add(self, owner, term):
        r, c, z = place()
        self.src[c, owner] = (self.src[c, owner].astype(F32) + term.astype(F32)).astype(BF16)

    def start2(self):
        self.c1().wait()
        for q, owner in enumerate(self.owners(0, True)[0]):
            self.add(owner, self.r1[owner])
            self.c2(0, q).start()
        for owner in self.owners(0, False)[0]:
            self.add(owner, self.r1[owner])

    def landed(self, i):
        own, slot = self.owners(i, False)
        for q in range(len(own)):
            self.c2(i, q).wait()
        for q, owner in enumerate(own):
            self.add(owner, self.r2[slot + q])

    def halve(self):
        for i in range(1, len(self.steps)):
            self.landed(i - 1)
            for q in range(len(self.owners(i, True)[0])):
                self.c2(i, q).start()

    def c3(self, j):
        r, c, z = place()
        to = lax.rem(z + j, self.pn.ns)
        return to, remote(self.src.at[c, r], self.r3.at[j - 1], self.sems, self.k3 + j - 1, {"opt": to})

    def start3(self):
        r, c, z = place()
        self.landed(len(self.steps) - 1)
        for j in range(1, self.pn.ns):
            to, cp = self.c3(j)

            @pl.when(self.here(to))
            def _():
                cp.start()

    def c4(self, j):
        r, c, z = place()
        return remote(self.ag.at[c, r], self.ag.at[c, r], self.sems, self.k4 + j - 1, peer(lax.rem(r + j, self.pn.rest), c))

    def start4(self):
        r, c, z = place()
        for j in range(1, self.pn.ns):
            to, cp = self.c3(j)

            @pl.when(self.here(to))
            def _():
                cp.wait_send()

        @pl.when(self.here(z))
        def _():
            for j in range(1, self.pn.ns):
                self.c3(j)[1].wait_recv()
            v = self.src[c, r].astype(F32)
            for j in range(1, self.pn.ns):
                v = v + self.r3[j - 1].astype(F32)
            self.ag[c, r] = v.astype(BF16)
            for j in range(1, self.pn.rest):
                self.c4(j).start()

    def c5(self):
        r, c, z = place()
        return remote(self.ag.at[c], self.ag.at[c], self.sems, self.k5, peer(r, 1 - c))

    def start5(self):
        r, c, z = place()

        @pl.when(self.here(z))
        def _():
            for j in range(1, self.pn.rest):
                self.c4(j).wait()
            self.c5().start()

    def finish(self):
        r, c, z = place()

        @pl.when(self.here(z))
        def _():
            self.c5().wait()


SMALL = (0, 769, 770, 771, 772)


class Small:
    def __init__(self, pn, own, r1, mid, r2, sems):
        self.pn, self.own, self.r1, self.mid, self.r2, self.sems = pn, own, r1, mid, r2, sems

    @staticmethod
    def scratch(pn):
        u = len(SMALL)
        return [pltpu.VMEM((u, 8, 128), BF16), pltpu.VMEM((pn.ndp, u, 8, 128), BF16), pltpu.VMEM((u, 8, 128), BF16), pltpu.VMEM((pn.ns, u, 8, 128), BF16),
                pltpu.SemaphoreType.DMA((2, pn.ndp + pn.ns - 2))]

    def c1(self, j):
        me = lax.axis_index("dp")
        return remote(self.own, self.r1.at[me], self.sems, j - 1, {"dp": lax.rem(me + j, self.pn.ndp)})

    def w1(self, j):
        me = lax.axis_index("dp")
        return remote(self.own, self.r1.at[lax.rem(me - j + self.pn.ndp, self.pn.ndp)], self.sems, j - 1, {"dp": lax.rem(me + j, self.pn.ndp)})

    def start1(self):
        me = lax.axis_index("dp")
        for j in range(1, self.pn.ndp):
            self.c1(j).start()
        self.r1[me] = self.own[...]

    def c2(self, j):
        z = lax.axis_index("opt")
        to = lax.rem(z + j, self.pn.ns)
        return to, remote(self.mid, self.r2.at[z], self.sems, self.pn.ndp - 2 + j, {"opt": to})

    def w2(self, j):
        z = lax.axis_index("opt")
        return remote(self.mid, self.r2.at[lax.rem(z - j + self.pn.ns, self.pn.ns)], self.sems, self.pn.ndp - 2 + j, {"opt": lax.rem(z + j, self.pn.ns)})

    def start2(self):
        z = lax.axis_index("opt")
        for j in range(1, self.pn.ndp):
            self.c1(j).wait_send()
            self.w1(j).wait_recv()
        v = self.r1[0].astype(F32)
        for n in range(1, self.pn.ndp):
            v = v + self.r1[n].astype(F32)
        self.mid[...] = v.astype(BF16)
        for j in range(1, self.pn.ns):
            to, cp = self.c2(j)

            @pl.when(to <= self.pn.ka)
            def _():
                cp.start()
        self.r2[z] = v.astype(BF16)

    def finish(self):
        z = lax.axis_index("opt")
        for j in range(1, self.pn.ns):
            to, cp = self.c2(j)

            @pl.when(to <= self.pn.ka)
            def _():
                cp.wait_send()

            @pl.when(z <= self.pn.ka)
            def _():
                self.w2(j).wait_recv()

    def total(self, n):
        v = self.r2[0, n].astype(F32)
        for k in range(1, self.pn.ns):
            v = v + self.r2[k, n].astype(F32)
        return v.astype(BF16).astype(F32)


NSEMS = 32


def put_rows_grad(fs, start, v):
    put_rows(fs, start, v)


def kernel_bc(pn, x_hbm, cot_hbm, ob_hbm, wp_hbm, w1_hbm, w2_hbm, hwt_hbm, qkv_hbm, p_hbm, wqkv_hbm, vec, rel_ref, counts,
              y_hbm, dx_hbm, g_hbm, *refs):
    refs = list(refs)
    dx1, wp, acc, dsem = refs[:4]
    refs = refs[4:]
    chunks = []
    nb = 2 * (pn.ns - pn.ka)
    for n, (k0, k1, m, at, flip) in enumerate(part_list(pn)):
        if 1 < n < nb:
            refs[4:4] = [chunks[n % 2].r3, chunks[n % 2].ag]
        chunks.append(Chunk(pn, k0, k1, m, at, flip, *refs[:6]))
        refs = refs[6:]
    shards, ac = chunks[:nb], chunks[nb:]
    his = [ch for ch in shards if ch.k0 >= pn.kh]
    los = [ch for ch in shards if ch.k0 < pn.kh]
    mids, last = los[:-2], los[-2:]

    def each(chs, name):
        return tuple(getattr(ch, name) for ch in chs)

    def run(fns):
        for f in fns:
            f()
    small = Small(pn, *refs)
    count = counts[0]

    def local(n, src, dst):
        return pltpu.make_async_copy(src, dst, dsem.at[n])

    def mlp(x_v, dy_v, ob, a, du, h2, w1, w2, fs, xsem, csem):
        ins = [local(n, s, d) for n, (s, d) in enumerate([(ob_hbm, ob), (wp_hbm, wp), (w1_hbm, w1), (w2_hbm, w2)])]
        cps = window_copies(x_hbm, x_v, xsem, True) + window_copies(cot_hbm, dy_v, csem, True)
        for cp in cps + ins:
            cp.start()
        acc[...] = jnp.zeros_like(acc)
        bp, g2, b2, c2 = (vec[n:n + 1, :] for n in range(4, 8))
        enter(pn, True)
        for cp in cps + ins:
            cp.wait()
        nb = BM // 56

        def rows(t, _):
            r0 = pl.multiple_of(t * BM, BM)
            x = x_v[pl.ds(nb * t, nb)].reshape(BM, D).astype(F32)
            alive = lax.broadcasted_iota(jnp.int32, (nb, 7, 8, D), 2) < count
            dy = jnp.where(alive, dy_v[pl.ds(nb * t, nb)].astype(F32), 0.0)
            dyb = dy.astype(BF16)
            dy_v[pl.ds(nb * t, nb)] = dyb
            dy = dy.reshape(BM, D)
            dyb = dyb.reshape(BM, D)
            x1 = x + dot(ob[pl.ds(r0, BM), :], wp[...]) + bp
            xhat, r = norm_stats(x1)
            h = (xhat * g2 + b2).astype(BF16)
            h2[pl.ds(r0, BM), :] = h
            y = x1 + c2
            dh = jnp.zeros((BM, D), F32)
            for j in range(HID // CH):
                cs = slice(j * CH, (j + 1) * CH)
                u = dot(h, w1[:, cs]) + vec[8 + j:9 + j, :]
                cdf, pdf = gelu_parts(u)
                av = (u * cdf).astype(BF16)
                a[pl.ds(r0, BM), cs] = av
                y = y + dot(av, w2[cs, :])
                da = dot_nt(dyb, w2[cs, :])
                duv = da * (cdf + u * pdf)
                acc_rows(acc, 4 + j, duv)
                dub = duv.astype(BF16)
                du[pl.ds(r0, BM), cs] = dub
                dh = dh + dot_nt(dub, w1[:, cs])
            x_v[pl.ds(nb * t, nb)] = y.reshape(nb, 7, 8, D).astype(BF16)
            acc_rows(acc, 0, dy)
            acc_rows(acc, 1, dh * xhat)
            acc_rows(acc, 2, dh)
            dg = dh * g2
            dt = r * (dg - jnp.mean(dg, -1, keepdims=True) - xhat * jnp.mean(dg * xhat, -1, keepdims=True))
            dxv = dy + dt
            acc_rows(acc, 3, dxv)
            dx1[pl.ds(nb * t, nb)] = dxv.reshape(nb, 7, 8, D)
            return 0
        lax.fori_loop(0, ROWS // BM, rows, 0)
        ycs = window_copies(y_hbm, x_v, xsem, False)
        for cp in ycs:
            cp.start()
        vg = jnp.sum(acc[...].reshape(8, 8, D), 1)
        first = pn.base * 8
        nrow = pn.bunits * 8
        lo_row = (R_PROJ // 8 + 1) * 8 - first
        hi_row = R_END // 8 * 8 - first
        fs[0:lo_row, :] = jnp.zeros((lo_row, 128), F32)
        fs[hi_row:nrow, :] = jnp.zeros((nrow - hi_row, 128), F32)
        dyf = dy_v[...].reshape(ROWS, D)

        def w2rows(t, _):
            r0 = pl.multiple_of(t * 512, 512)
            v = dot_tn(a[:, pl.ds(r0, 512)], dyf)
            put_tile(fs, R_W2 - first + r0 * 4, 4, [v[:, c * 128:(c + 1) * 128] for c in range(4)])
            return 0
        lax.fori_loop(0, HID // 512, w2rows, 0)
        put_vec(fs, R_C2 - first, vg[0:1])

        def fill(ch):
            def piece(p, _):
                row = pl.multiple_of(((ch.k0 - pn.ka) * pn.units + p * pn.pc + ch.at) * 8, 8)
                ch.src[p & 1, lax.shift_right_arithmetic(p, 1)] = fs[pl.ds(row, ch.n * 8), :].reshape(ch.n, 8, 128).astype(BF16)
                return 0
            lax.fori_loop(0, pn.ndp, piece, 0)
            ch.start1()
        for ch in his:
            fill(ch)
        h2t = a.at[0:D, 0:1664]
        transpose_rows(h2, h2t)

        lane = lax.broadcasted_iota(jnp.int32, (D, 128), 1)
        at = R_W1 - first
        keep = fs[pl.ds(at, 1), :]

        def w1rows(t, before):
            r0 = pl.multiple_of(t * 512, 512)
            u = dot(h2t[:, 0:ROWS], du[:, pl.ds(r0, 512)])
            v = shifted([u[:, c * 128:(c + 1) * 128] for c in range(4)])
            for c in range(4):
                fs[pl.ds(at + 4 * t + c, D, stride=16), :] = jnp.where(lane >= LANE, v[c], before if c == 0 else v[c - 1])
            return v[3]
        v = lax.fori_loop(0, HID // 512, w1rows, jnp.zeros((D, 128), F32))
        one = lax.broadcasted_iota(jnp.int32, (1, 128), 1)
        v = jnp.where(lax.broadcasted_iota(jnp.int32, (D, 128), 0) == 0, keep, pltpu.roll(v, 1, 0)), v[D - 1:D]
        fs[pl.ds(at, D, stride=16), :] = jnp.where(lane < LANE, v[0], fs[pl.ds(at, D, stride=16), :])
        fs[pl.ds(at + D * 16, 1), :] = jnp.where(one < LANE, v[1], fs[pl.ds(at + D * 16, 1), :])
        run(each(his, 'start2'))
        v = dot_tn(ob[...], dx1[...].reshape(ROWS, D).astype(BF16))
        put_tile(fs, R_PROJ - first, 4, [v[:, c * 128:(c + 1) * 128] for c in range(4)])
        for row, n in ((R_BP, 3), (R_G2, 1), (R_B2, 2)):
            put_vec(fs, row - first, vg[n:n + 1])
        for j in range(4):
            put_vec(fs, R_C1 - first + 4 * j, vg[4 + j:5 + j])
        for ch in los:
            fill(ch)
        for cp in ycs:
            cp.wait()

    big = pltpu.VMEM((28, 7, 8, D), BF16)
    pl.run_scoped(mlp, big, big, pltpu.VMEM((ROWS, D), BF16), pltpu.VMEM((ROWS, HID), BF16), pltpu.VMEM((ROWS, HID), BF16), pltpu.VMEM((ROWS, D), BF16),
                  pltpu.VMEM((D, HID), BF16), pltpu.VMEM((HID, D), BF16), pltpu.VMEM((pn.bunits * 8, 128), F32),
                  pltpu.SemaphoreType.DMA((NSEG,)), pltpu.SemaphoreType.DMA((NSEG,)))

    def attention(x_v, qkvb, pb, hwt, wqkv, fs, os_, dq, dtab, xsem):
        ins = [local(n, s, d) for n, (s, d) in enumerate([(qkv_hbm, qkvb), (p_hbm, pb), (hwt_hbm, hwt), (wqkv_hbm, wqkv)])]
        for cp in ins:
            cp.start()
        cps = window_copies(x_hbm, x_v, xsem, True)
        for cp in cps:
            cp.start()
        acc[...] = jnp.zeros_like(acc)
        dtab[...] = jnp.zeros_like(dtab)

        def rows0(t, _):
            r0 = pl.multiple_of(t * 392, 8)
            ev = dx1[pl.ds(7 * t, 7)].reshape(392, D).astype(BF16)
            v = dot_nt(ev, wp[...])
            for g in range(4):
                os_[pl.ds(g * RS + r0, 392), :] = v[:, g * 128:(g + 1) * 128]
            return 0
        lax.fori_loop(0, 4, rows0, 0)
        ins[0].wait()
        ins[1].wait()
        run(each(his, 'halve') + each(los, 'start2'))
        heads = lane_head()

        def several(g, items):
            bases = [lax.shift_right_arithmetic(i, 3) * WROWS + (i & 7) for i in items]
            dobds = [block_diag(take_rows(os_, g * RS + base).astype(BF16), heads) for base in bases]
            dps = [dot_nt(qkvb[i, 8 + g], d) for i, d in zip(items, dobds)]
            total = dtab[g]
            dsbs = []
            for i, dp in zip(items, dps):
                p = pb[i, g].astype(F32)
                t = p * dp
                ds = t - p * jnp.sum(t, 0, keepdims=True)
                total = total + ds
                dsbs.append(ds.astype(BF16))
            dtab[g] = total
            dvs = [dot(pb[i, g], d) for i, d in zip(items, dobds)]
            dks = [dot(d, block_diag(qkvb[i, g], heads)) for i, d in zip(items, dsbs)]
            dqs = [dot_tn(d, qkvb[i, 4 + g]) for i, d in zip(items, dsbs)]
            for base, dv, dk, dqv in zip(bases, dvs, dks, dqs):
                put_rows(fs, 2 * RS + base, dv)
                put_rows(fs, RS + base, dk)
                put_rows(fs, base, diag_sum(dqv, heads) * SCALE)

        mid = {0: each(his, 'start3'), 1: each(mids, 'halve') + (ac[0].start2,), 2: each(last, 'halve') + (ac[1].start2,) + each(his, 'start4'),
               3: each(mids, 'start3') + (ac[0].halve, ac[2].start2)}
        for g in range(4):
            def attend(t, _):
                @pl.when(t == 1)
                def _():
                    for f in mid[g]:
                        f()
                several(g, [16 * t + n for n in range(16)])
                return 0
            lax.fori_loop(0, WB // 16, attend, 0)
            parts = []
            for n in range(3):
                v = fs[n * RS:n * RS + ROWS, :]
                if n != 1:
                    acc[8 * (2 + n // 2):8 * (3 + n // 2), g * 128:(g + 1) * 128] = jnp.sum(v.reshape(ROWS // 8, 8, 128), 0)
                v = v.astype(BF16)
                dq[:, n * D + g * 128:n * D + (g + 1) * 128] = v
                parts.append(v)
            if g == 0:
                ins[2].wait()
                ins[3].wait()
            v = dot(hwt[...], jnp.concatenate(parts, 1))
            mu = pn.mrow // 8
            for n in range(3):
                u = v[:, n * 128:(n + 1) * 128].reshape(D // 8, 8, 128).astype(BF16)
                for p in range(pn.ndp):
                    ac[g].src[p & 1, p >> 1, n * mu:(n + 1) * mu] = u[p * mu:(p + 1) * mu]
            ac[g].start1()
        run(each(last, 'start3') + (ac[0].start3, ac[1].halve))
        for cp in cps:
            cp.wait()
        gain = vec[0:1, :]
        tab = table_grad(rel_ref, os_, dtab)
        for n in range(3):
            small.own[2 + n] = tab[8 * n:8 * n + 8].astype(BF16)
        late = {0: (ac[3].start2,), 1: (ac[1].start3, ac[2].halve), 2: (ac[3].halve,) + each(his, 'start5'), 3: each(mids, 'start4') + (ac[2].start3,),
                4: (ac[0].start4, ac[3].start3), 5: each(last, 'start4'), 6: (ac[1].start4,) + each(mids, 'start5')}

        def rows1(t, _):
            for k, fns in late.items():
                @pl.when(t == k)
                def _():
                    for f in fns:
                        f()
            r0 = pl.multiple_of(t * BLK, BLK)
            dn = dot_nt(dq[pl.ds(r0, BLK), :], wqkv[...])
            x = x_v[pl.ds(4 * t, 4)].reshape(BLK, D).astype(F32)
            xhat, r = norm_stats(x)
            acc_rows(acc, 0, dn * xhat)
            acc_rows(acc, 1, dn)
            dg = dn * gain
            dt = r * (dg - jnp.mean(dg, -1, keepdims=True) - xhat * jnp.mean(dg * xhat, -1, keepdims=True))
            dx1[pl.ds(4 * t, 4)] += dt.reshape(4, 7, 8, D)
            return 0
        lax.fori_loop(0, NBLK, rows1, 0)
        vg = jnp.sum(acc[...].reshape(8, 8, D), 1)
        flat = [vg[n:n + 1, c * 128:(c + 1) * 128] for n in range(4) for c in range(4)]
        small.own[0] = jnp.concatenate(flat[:8], 0).astype(BF16)
        small.own[1] = jnp.concatenate(flat[8:], 0).astype(BF16)
        small.start1()
        ycs = window_copies(dx_hbm, dx1, xsem, False)
        for cp in ycs:
            cp.start()
        run((ac[2].start4, ac[3].start4, ac[0].start5, ac[1].start5, small.start2) + each(last, 'start5') + (ac[2].start5, ac[3].start5))
        for ch in shards:
            ch.finish()
        r, c, z = place()
        g = os_

        @pl.when(z >= pn.ka)
        def _():
            def piece(p, _):
                for ch in shards[:2]:
                    g[pl.ds(pl.multiple_of((p * pn.pc + ch.at) * 8, 8), ch.n * 8), :] = ch.ag[p & 1, lax.shift_right_arithmetic(p, 1)].astype(F32).reshape(ch.n * 8, 128)
                return 0
            lax.fori_loop(0, pn.ndp, piece, 0)
        mu = pn.mrow // 8

        for h in range(4):
            ac[h].finish()

            @pl.when(z < pn.ka)
            def _():
                def piece(p, _):
                    for n in range(3):
                        v = ac[h].ag[p & 1, lax.shift_right_arithmetic(p, 1), n * mu:(n + 1) * mu].astype(F32).reshape(pn.mrow, 128)
                        g[pl.ds(R_QKV + p * pn.mrow * 12 + n * 4 + h, pn.mrow, stride=12), :] = v
                    return 0
                lax.fori_loop(0, pn.ndp, piece, 0)
        small.finish()

        @pl.when(z < pn.ka)
        def _():
            for n, u in enumerate(SMALL):
                g[u * 8:u * 8 + 8, :] = small.total(n)

        @pl.when(z == pn.ka)
        def _():
            for n, u in enumerate(SMALL):
                if u >= pn.base:
                    k = (u - pn.base) * 8
                    g[k:k + 8, :] += small.total(n)
        out = local(0, g.at[pl.ds(pl.multiple_of(lax.select(z < pn.ka, z * (pn.units * 8), 0), 8), pn.units * 8)], g_hbm)
        out.start()
        out.wait()
        for cp in ycs:
            cp.wait()

    pl.run_scoped(attention, big, pltpu.VMEM((WB, 12, 64, 128), BF16), pltpu.VMEM((WB, 4, 64, 256), BF16), pltpu.VMEM((D, ROWS), BF16), pltpu.VMEM((D, 3 * D), BF16),
                  pltpu.VMEM((3 * RS, 128), F32), pltpu.VMEM((max(4 * RS, pn.gunits * 8), 128), F32), pltpu.VMEM((ROWS, 3 * D), BF16), pltpu.VMEM((4, 64, 256), F32), pltpu.SemaphoreType.DMA((NSEG,)))


def part_list(pn):
    mu = 3 * pn.mrow // 8
    h = (pn.pc + 1) // 2
    out = []
    for k in range(pn.ns - 1, pn.ka - 1, -1):
        out += [(k, k + 1, h, 0, False), (k, k + 1, pn.pc - h, h, True)]
    return out + [(0, pn.ka, mu, 0, g % 2 == 1) for g in range(4)]


def call_bc(pn, x, cot, ob, wp, w1, w2, hwt, qkv, p, wqkv, vec, rel, counts):
    any_ = pl.BlockSpec(memory_space=pl.ANY)
    vm = pl.BlockSpec(memory_space=pltpu.VMEM)
    sds = jax.ShapeDtypeStruct
    outs = [sds((14, 14, 8, D), BF16), sds((14, 14, 8, D), F32), sds((pn.units * 8, 128), F32)]
    scratch = [pltpu.VMEM((28, 7, 8, D), F32), pltpu.VMEM((D, D), BF16), pltpu.VMEM((64, D), F32), pltpu.SemaphoreType.DMA((4,))]
    for n, (k0, k1, m, at, flip) in enumerate(part_list(pn)):
        scratch += Chunk.scratch(pn, m, 1 < n < 2 * (pn.ns - pn.ka))
    scratch += Small.scratch(pn)
    return pl.pallas_call(
        functools.partial(kernel_bc, pn),
        out_shape=outs,
        in_specs=[any_] * 10 + [vm, vm, pl.BlockSpec(memory_space=pltpu.SMEM)],
        out_specs=[any_] * 3,
        scratch_shapes=scratch,
        compiler_params=pltpu.CompilerParams(vmem_limit_bytes=67000000, collective_id=1, has_side_effects=True),
        name="back",
    )(x, cot, ob, wp, w1, w2, hwt, qkv, p, wqkv, vec, rel, counts)


STEP = 2
DECAYED = (2, 6, 10, 12)
LENGTHS = [D, D, 3 * D * D, D, D, TAB * HEADS, D * D, D, D, D, D * HID, HID, HID * D, D]
AU = 128


def kernel_adam(rates, first, g, p, m1, m2, g_o, p_o, m_o, v_o):
    shape = (AU, 8, 128)
    u0 = first[0] + pl.program_id(0) * AU
    starts = [sum(LENGTHS[:n + 1]) for n in range(len(LENGTHS))]

    def group(at):
        k = jnp.int32(0)
        for s in starts:
            k = k + (at >= s).astype(jnp.int32)
        return k

    def update(rate, decay):
        grad = g[...]
        w = p[...]
        m = 0.9 * m1[...] + 0.1 * grad
        v = 0.999 * m2[...] + 0.001 * grad * grad
        mh = m / (1.0 - 0.9 ** STEP)
        vh = v / (1.0 - 0.999 ** STEP)
        p_o[...] = w - rate * (mh / (jnp.sqrt(vh) + 1e-08) + decay * w)
        m_o[...] = m
        v_o[...] = v
        g_o[...] = grad
    k0 = group(u0 * 1024)
    k1 = group((u0 + AU) * 1024 - 1)

    @pl.when(k0 == k1)
    def _():
        decay = jnp.float32(0.0)
        for n in DECAYED:
            decay = jnp.where(k0 == n, jnp.float32(0.05), decay)
        update(rates[k0], decay)

    @pl.when(k0 != k1)
    def _():
        index = ((u0 + lax.broadcasted_iota(jnp.int32, shape, 0)) * 8 + lax.broadcasted_iota(jnp.int32, shape, 1)) * 128 + lax.broadcasted_iota(jnp.int32, shape, 2)
        rate = jnp.zeros(shape, F32) + rates[0]
        decay = jnp.zeros(shape, F32)
        for n, s in enumerate(starts):
            after = index >= s
            rate = jnp.where(after, rates[n + 1], rate)
            if n in DECAYED or n + 1 in DECAYED:
                decay = jnp.where(after, 0.05 if n + 1 in DECAYED else 0.0, decay)
        update(rate, decay)


def call_adam(pn, rates, g, params, mom1, mom2):
    view = lambda t: t.reshape(pn.units, 8, 128)
    spec = pl.BlockSpec((AU, 8, 128), lambda i: (i, 0, 0))
    sm = pl.BlockSpec(memory_space=pltpu.SMEM)
    first = (lax.axis_index("opt") * pn.units).astype(jnp.int32).reshape(1)
    out = pl.pallas_call(
        kernel_adam,
        grid=(pl.cdiv(pn.units, AU),),
        out_shape=[jax.ShapeDtypeStruct((pn.units, 8, 128), F32)] * 4,
        in_specs=[sm, sm] + [spec] * 4,
        out_specs=[spec] * 4,
        compiler_params=pltpu.CompilerParams(vmem_limit_bytes=67043328),
        name="adamw",
    )(rates, first, view(g), view(params), view(mom1), view(mom2))
    return [t.reshape(-1) for t in out]


from jax.sharding import PartitionSpec as P


def solution(mesh):
    def local(images, cotangent, counts, rel_index, params, moment1, moment2, rates):
        pn = Plan(mesh, params.shape[0])
        xt = images.transpose(1, 2, 0, 3)
        ct = cotangent.transpose(1, 2, 0, 3)
        rel = rel_lanes(rel_index)
        wqkv, wp, w1, w2, vec, hwt, ob, qkv, p = call_a(pn, xt, params, rel)
        y, dx, g = call_bc(pn, xt, ct, ob, wp, w1, w2, hwt, qkv, p, wqkv, vec, rel, counts)
        grad, new_params, new_first, new_second = call_adam(pn, rates, g, params, moment1, moment2)
        return (y.transpose(2, 0, 1, 3), dx.transpose(2, 0, 1, 3), grad, new_params, new_first, new_second)

    split = P(("dp", "opt"), None, None, None)
    return jax.shard_map(
        local, mesh=mesh,
        in_specs=(split, split, P(("dp", "opt")), P(), P("opt"), P("opt"), P("opt"), P()),
        out_specs=(split, split, P("opt"), P("opt"), P("opt"), P("opt")),
        check_vma=False)
```

```python
import functools
import jax
import jax.numpy as jnp
from jax import lax
from jax.experimental import pallas as pl
from jax.experimental.pallas import tpu as pltpu

D = 512
HEADS = 16
HEAD_DIM = 32
HID = 2048
SIDE = 14
WIN = 7
SHIFT = 3
TAB = 169
F32 = jnp.float32
BF16 = jnp.bfloat16

IMGS = 8
SPAN = WIN * WIN
WROWS = SPAN * IMGS
ROWS = 4 * WROWS
RS = ROWS + 64
BLK = 224
NBLK = ROWS // BLK
BM = 784
WB = 4 * IMGS
SCALE = HEAD_DIM ** -0.5

R_G1, R_B1, R_QKV, R_BQ, R_BV, R_TAB = 0, 4, 8, 6152, 6156, 6160
R_PROJ, R_BP, R_G2, R_B2, R_W1, R_C1, R_W2, R_C2, R_END = 6181, 8229, 8233, 8237, 8241, 16433, 16449, 24641, 24645
LANE = 16
BROW = 6176


def segments(w):
    if w == 0:
        return [(SHIFT, WIN, 0)]
    return [(WIN + SHIFT, WIN - SHIFT, 0), (0, SHIFT, WIN - SHIFT)]


def window_copies(hbm, vmem, sem, inward):
    out = []
    n = 0
    for wy in range(2):
        for wx in range(2):
            for ys, yl, yo in segments(wy):
                for xs, xl, xo in segments(wx):
                    a = hbm.at[pl.ds(ys, yl), pl.ds(xs, xl)]
                    b = vmem.at[pl.ds((2 * wy + wx) * WIN + yo, yl), pl.ds(xo, xl)]
                    out.append(pltpu.make_async_copy(a, b, sem.at[n]) if inward else pltpu.make_async_copy(b, a, sem.at[n]))
                    n += 1
    return out


NSEG = 9


def dot(a, b):
    return lax.dot_general(a, b, (((1,), (0,)), ((), ())), preferred_element_type=F32)


def dot_nt(a, b):
    return lax.dot_general(a, b, (((1,), (1,)), ((), ())), preferred_element_type=F32)


def dot_tn(a, b):
    return lax.dot_general(a, b, (((0,), (0,)), ((), ())), preferred_element_type=F32)


def norm_stats(x):
    mean = jnp.mean(x, -1, keepdims=True)
    dev = x - mean
    var = jnp.mean(dev * dev, -1, keepdims=True)
    r = lax.rsqrt(var + 1e-05)
    return dev * r, r


def pieces_to_rows(pn, wb, fs, shard, count, base):
    def body(p, _):
        row = pl.multiple_of((shard * pn.units - base + p * pn.pc) * 8, 8)
        fs[pl.ds(row, pn.pc * 8), :] = wb[shard, p & 1, lax.shift_right_arithmetic(p, 1)].astype(F32).reshape(pn.pc * 8, 128)
        return 0
    lax.fori_loop(0, count, body, 0)


def vec_from(fs, row, width, shift):
    parts = []
    lane = lax.broadcasted_iota(jnp.int32, (1, 128), 1)
    for c in range(width // 128):
        a = fs[pl.ds(row + c, 1), :]
        if shift:
            b = fs[pl.ds(row + c + 1, 1), :]
            a = jnp.where(lane < 128 - LANE, pltpu.roll(a, 128 - LANE, 1), pltpu.roll(b, 128 - LANE, 1))
        parts.append(a)
    return jnp.concatenate(parts, 1)


def take_matrix(fs, row, dst, nrows, ncb, shift, step=128):
    lane = lax.broadcasted_iota(jnp.int32, (step, 128), 1)

    def body(t, _):
        base = row + t * (step * ncb)
        r0 = pl.multiple_of(t * step, step)
        for c in range(ncb):
            a = fs[pl.ds(base + c, step, stride=ncb), :]
            if shift:
                b = fs[pl.ds(base + c + 1, step, stride=ncb), :]
                a = jnp.where(lane < 128 - LANE, pltpu.roll(a, 128 - LANE, 1), pltpu.roll(b, 128 - LANE, 1))
            dst[pl.ds(r0, step), c * 128:(c + 1) * 128] = a.astype(BF16)
        return 0

    lax.fori_loop(0, nrows // step, body, 0)


def transpose_rows(src, dst):
    full = ROWS // 128

    def body(t, _):
        r0 = pl.multiple_of(t * 128, 128)
        dst[:, pl.ds(r0, 128)] = src[pl.ds(r0, 128), :].T
        return 0
    lax.fori_loop(0, full, body, 0)
    if ROWS % 128:
        dst[:, full * 128:ROWS] = src[full * 128:ROWS, :].T


def lane_head():
    return lax.broadcasted_iota(jnp.int32, (64, 128), 1) // HEAD_DIM


def block_diag(v, heads):
    zero = jnp.zeros_like(v)
    return jnp.concatenate([jnp.where(heads == h, v, zero) for h in range(4)], 0)


def diag_sum(r, heads):
    out = r[0:64]
    for h in range(1, 4):
        out = jnp.where(heads == h, r[64 * h:64 * h + 64], out)
    return out


def take_rows(fs, start):
    v = fs[pl.ds(start, 56, stride=IMGS), :]
    v = jnp.where(lax.broadcasted_iota(jnp.int32, (56, 128), 0) < SPAN, v, 0.0)
    return jnp.concatenate([v, jnp.zeros((8, 128), F32)], 0)


def put_rows(fs, start, v):
    fs[pl.ds(start, 48, stride=IMGS), :] = v[0:48]
    fs[pl.ds(start + 48 * IMGS, 1), :] = v[48:49]


def build_bias(tab3, rel_ref, big, bias):
    rel = rel_ref[...]
    row = lax.shift_right_arithmetic(rel, 3)
    low = rel & 7
    oh = (lax.broadcasted_iota(jnp.int32, (32, 4096), 0) == row).astype(F32).astype(BF16)
    tab = jnp.concatenate([tab3, jnp.zeros((8, 128), F32)], 0).astype(BF16)
    r = dot_tn(tab, oh)
    acc = jnp.zeros((16, 4096), F32)
    for j in range(8):
        acc = acc + jnp.where(low == j, r[16 * j:16 * j + 16], 0.0)
    for kk in range(32):
        big[kk * 16:kk * 16 + 16, :] = acc[:, kk * 128:kk * 128 + 128]
    k = lax.broadcasted_iota(jnp.int32, (64, 256), 0)
    q = lax.broadcasted_iota(jnp.int32, (64, 256), 1) & 63
    ki = lax.shift_right_arithmetic(k * 37, 8)
    kj = k - ki * 7
    qi = lax.shift_right_arithmetic(q * 37, 8)
    qj = q - qi * 7
    cut = WIN - SHIFT
    same_y = (ki < cut) == (qi < cut)
    same_x = (kj < cut) == (qj < cut)
    lane = lax.broadcasted_iota(jnp.int32, (32, 128), 1)
    for g in range(4):
        for pair in range(2):
            h = 4 * g + 2 * pair
            a = big[pl.ds(h, 32, stride=16), :]
            b = big[pl.ds(h + 1, 32, stride=16), :]
            even = jnp.where(lane < 64, a, pltpu.roll(b, 64, 1))
            odd = jnp.where(lane < 64, pltpu.roll(a, 64, 1), b)
            big[pl.ds(1024 + g * 256 + pair * 128, 32, stride=2), :] = even
            big[pl.ds(1024 + g * 256 + pair * 128 + 1, 32, stride=2), :] = odd
    for g in range(4):
        pos = jnp.concatenate([big[1024 + g * 256:1024 + g * 256 + 64, :], big[1024 + g * 256 + 128:1024 + g * 256 + 192, :]], 1)
        for w in range(4):
            keep = None
            if w == 1:
                keep = same_x
            elif w == 2:
                keep = same_y
            elif w == 3:
                keep = same_y & same_x
            val = pos if keep is None else pos + jnp.where(keep, 0.0, -100.0)
            bias[w * 4 + g] = jnp.where(k < SPAN, val, -1e30)


MESH = pl.DeviceIdType.MESH
NMAT = 768


class Plan:
    def __init__(self, mesh, shard_len):
        self.ndp = mesh.shape["dp"]
        self.ns = mesh.shape["opt"]
        self.rest = self.ndp // 2
        self.units = shard_len // 1024
        self.pc = -(-self.units // self.ndp)
        self.ka = (BROW // 8) // self.units
        self.base = self.ka * self.units
        self.bunits = (self.ns - self.ka - 1) * self.units + self.ndp * self.pc
        self.kh = -(-(R_W2 // 8 + 1) // self.units)
        self.mrow = D // self.ndp
        self.gunits = max(BROW // 8 + 1, self.ndp * self.pc)


def place():
    me = lax.axis_index("dp")
    return lax.shift_right_arithmetic(me, 1), me & 1, lax.axis_index("opt")


def peer(r, c):
    return {"dp": 2 * r + c}


def enter(pn, all_dp=False):
    r, c, z = place()
    bar = pltpu.get_barrier_semaphore()
    pl.semaphore_signal(bar, inc=1, device_id=peer(r, 1 - c), device_id_type=MESH)
    for j in range(1, pn.rest):
        for to in ((c, 1 - c) if all_dp else (c,)):
            pl.semaphore_signal(bar, inc=1, device_id=peer(lax.rem(r + j, pn.rest), to), device_id_type=MESH)
    for j in range(1, pn.ns):
        pl.semaphore_signal(bar, inc=1, device_id={"opt": lax.rem(z + j, pn.ns)}, device_id_type=MESH)
    pl.semaphore_wait(bar, (pn.ndp - 1 if all_dp else pn.rest) + pn.ns - 1)


def remote(src, dst, sems, n, where):
    return pltpu.make_async_remote_copy(src_ref=src, dst_ref=dst, send_sem=sems.at[0, n], recv_sem=sems.at[1, n], device_id=where, device_id_type=MESH)


class Gather:
    def __init__(self, pn, wb, osem, xsem, ysem):
        self.pn, self.wb, self.osem, self.xsem, self.ysem = pn, wb, osem, xsem, ysem
        h = (pn.pc + 1) // 2
        self.parts = [pl.ds(0, h), pl.ds(h, pn.pc - h)]

    @staticmethod
    def scratch(pn):
        return [pltpu.VMEM((pn.ns, 2, pn.rest, pn.pc, 8, 128), BF16), pltpu.SemaphoreType.DMA((2, 2 * pn.ns)),
                pltpu.SemaphoreType.DMA((2, 2 * pn.ns * pn.rest)), pltpu.SemaphoreType.DMA((2, 2 * pn.ns))]

    def o(self, j, h):
        r, c, z = place()
        own = self.wb.at[z, c, r, self.parts[h]]
        return pltpu.make_async_remote_copy(src_ref=own, dst_ref=own, send_sem=self.osem.at[0, 2 * j + h], recv_sem=self.osem.at[1, 2 * z + h],
                                            device_id={"opt": lax.rem(z + j, self.pn.ns)}, device_id_type=MESH)

    def arrived(self, s, h):
        r, c, z = place()
        own = self.wb.at[s, c, r, self.parts[h]]
        return pltpu.make_async_remote_copy(src_ref=own, dst_ref=own, send_sem=self.osem.at[0, h], recv_sem=self.osem.at[1, 2 * s + h],
                                            device_id={"opt": lax.rem(z + 1, self.pn.ns)}, device_id_type=MESH)

    def x(self, s, h, j):
        r, c, z = place()
        own = self.wb.at[s, c, r, self.parts[h]]
        return remote(own, own, self.xsem, (2 * s + h) * self.pn.rest + j, peer(lax.rem(r + j, self.pn.rest), c))

    def y(self, s, h):
        r, c, z = place()
        own = self.wb.at[s, c, :, self.parts[h]]
        return remote(own, own, self.ysem, 2 * s + h, peer(r, 1 - c))

    def start(self):
        for h in range(2):
            for j in range(1, self.pn.ns):
                self.o(j, h).start()

    def spread(self, s, h):
        r, c, z = place()

        @pl.when(z != s)
        def _():
            self.arrived(s, h).wait_recv()
            for j in range(1, self.pn.rest):
                self.x(s, h, j).start()

    def pair(self, s, h):
        r, c, z = place()

        @pl.when(z != s)
        def _():
            for j in range(1, self.pn.rest):
                self.x(s, h, j).wait_recv()
            self.y(s, h).start()

    def ready(self, s):
        r, c, z = place()

        @pl.when(z != s)
        def _():
            for h in range(2):
                self.y(s, h).wait_recv()

    def finish(self):
        r, c, z = place()
        for h in range(2):
            for j in range(1, self.pn.ns):
                self.o(j, h).wait_send()
            for s in range(self.pn.ns):
                @pl.when(z != s)
                def _():
                    for j in range(1, self.pn.rest):
                        self.x(s, h, j).wait_send()
                    self.y(s, h).wait_send()


def kernel_a(pn, x_hbm, params, rel_ref,
             wqkv_o, wp_o, w1_o, w2_o, vec_o, hw_o, ob_o, qkv_o, p_o,
             x_v, fs, os_, bias, wqkv, wp, w1, w2, vec, hw, hwt, ob, qkvb, pb, xsem, fsem, osem, wsem, flat_v, *gsems):
    cps = window_copies(x_hbm, x_v, xsem, True)
    for c in cps:
        c.start()
    r, c, z = place()
    gather = Gather(pn, flat_v, *gsems)
    fcp = pltpu.make_async_copy(params, fs.at[pl.ds(0, pn.units * 8)], fsem)
    fcp.start()
    enter(pn)
    fcp.wait()

    def cast(p):
        flat_v[z, p & 1, lax.shift_right_arithmetic(p, 1)] = fs[pl.ds(pl.multiple_of(p * pn.pc * 8, 8), pn.pc * 8), :].reshape(pn.pc, 8, 128).astype(BF16)
    me = lax.axis_index("dp")
    cast(me)
    gather.start()

    def others(j, _):
        cast(lax.rem(me + j, pn.ndp))
        return 0
    lax.fori_loop(1, pn.ndp, others, 0)
    for h in range(2):
        for k in range(pn.ka):
            gather.spread(k, h)
    for h in range(2):
        for k in range(pn.ka):
            gather.pair(k, h)
        gather.spread(pn.ka, h)
    for k in range(pn.ka):
        gather.ready(k)
    for k in range(pn.ka):
        pieces_to_rows(pn, flat_v, fs, k, pn.ndp, 0)
    take_matrix(fs, R_QKV, wqkv, D, 12, False)
    vec[0:1, :] = vec_from(fs, R_G1, D, False)
    vec[1:2, :] = vec_from(fs, R_B1, D, False)
    vec[2:3, :] = vec_from(fs, R_BQ, D, False)
    vec[3:4, :] = vec_from(fs, R_BV, D, False)
    wos = [pltpu.make_async_copy(wqkv, wqkv_o, wsem.at[0])]
    wos[0].start()
    for cp in cps:
        cp.wait()
    gain = vec[0:1, :]
    shift = vec[1:2, :]
    bq = vec[2:3, :]
    bv = vec[3:4, :]

    def rows(t, _):
        @pl.when(t == 0)
        def _():
            for k in range(pn.ka + 1, pn.ns):
                for h in range(2):
                    gather.spread(k, h)

        @pl.when(t == 1)
        def _():
            for h in range(2):
                gather.pair(pn.ka, h)
        r0 = pl.multiple_of(t * BM, BM)
        x = x_v[pl.ds(BM // 56 * t, BM // 56)].reshape(BM, D).astype(F32)
        xhat, _r = norm_stats(x)
        h = (xhat * gain + shift).astype(BF16)
        hw[pl.ds(r0, BM), :] = h
        for n in range(3):
            y = dot(h, wqkv[:, n * D:(n + 1) * D])
            if n == 0:
                y = (y + bq) * SCALE
            if n == 2:
                y = y + bv
            for c in range(4):
                fs[pl.ds((4 * n + c) * RS + r0, BM), :] = y[:, c * 128:(c + 1) * 128]
        return 0
    lax.fori_loop(0, ROWS // BM, rows, 0)
    gather.ready(pn.ka)
    tab = []
    for u in range(R_TAB // 8, R_TAB // 8 + 3):
        k, at = (pn.ka, u - pn.base) if u >= pn.base else (pn.ka - 1, u - pn.base + pn.units)
        p = at // pn.pc
        tab.append(flat_v[k, p & 1, p >> 1, at - p * pn.pc].astype(F32))
    build_bias(jnp.concatenate(tab, 0), rel_ref, os_, bias)
    heads = lane_head()

    def saved(t):
        four = pl.ds(4 * t, 4)
        return [pltpu.make_async_copy(qkvb.at[four], qkv_o.at[four], osem.at[2 + t]), pltpu.make_async_copy(pb.at[four], p_o.at[four], osem.at[2 + WB // 4 + t])]

    def attend(t, _):
        un = 4
        items = [(un * t + n, g) for n in range(un) for g in range(4)]
        ss = []
        vs = []
        for i, g in items:
            w = lax.shift_right_arithmetic(i, 3)
            base = w * WROWS + (i & 7)
            q = take_rows(fs, g * RS + base).astype(BF16)
            k = take_rows(fs, (4 + g) * RS + base).astype(BF16)
            v = take_rows(fs, (8 + g) * RS + base).astype(BF16)
            qkvb[i, g] = q
            qkvb[i, 4 + g] = k
            qkvb[i, 8 + g] = v
            vs.append(v)
            ss.append(dot_nt(k, block_diag(q, heads)) + bias[w * 4 + g])
        ps = []
        for (i, g), s in zip(items, ss):
            m = jnp.max(s, 0, keepdims=True)
            e = jnp.exp(s - m)
            p = (e * (1.0 / jnp.sum(e, 0, keepdims=True))).astype(BF16)
            pb[i, g] = p
            ps.append(p)
        for (i, g), p, v in zip(items, ps, vs):
            w = lax.shift_right_arithmetic(i, 3)
            base = w * WROWS + (i & 7)
            o = diag_sum(dot_tn(p, v), heads)
            put_rows(os_, g * RS + base, o)
        for cp in saved(t):
            cp.start()

        @pl.when(t == 2)
        def _():
            for k in range(pn.ka + 1, pn.ns):
                for h in range(2):
                    gather.pair(k, h)
        return 0
    lax.fori_loop(0, WB // 4, attend, 0)

    def outs(t, _):
        r0 = pl.multiple_of(t * BLK, BLK)
        for g in range(4):
            ob[pl.ds(r0, BLK), g * 128:(g + 1) * 128] = os_[pl.ds(g * RS + r0, BLK), :].astype(BF16)
        return 0
    lax.fori_loop(0, NBLK, outs, 0)
    transpose_rows(hw, hwt)
    cos = [pltpu.make_async_copy(a, b, osem.at[n]) for n, (a, b) in enumerate([(hwt, hw_o), (ob, ob_o)])]
    for cp in cos:
        cp.start()
    for k in range(pn.ka + 1, pn.ns):
        gather.ready(k)
    for k in range(pn.ka, pn.ns):
        pieces_to_rows(pn, flat_v, fs, k, pn.ndp, pn.base)
    first = pn.base * 8
    take_matrix(fs, R_PROJ - first, wp, D, 4, True)
    take_matrix(fs, R_W1 - first, w1, D, 16, True)
    take_matrix(fs, R_W2 - first, w2, HID, 4, True)
    for n, r in enumerate((R_BP, R_G2, R_B2, R_C2)):
        vec[4 + n:5 + n, :] = vec_from(fs, r - first, D, True)
    for n in range(4):
        vec[8 + n:9 + n, :] = vec_from(fs, R_C1 - first + 4 * n, D, True)
    for n, (a, b) in enumerate([(wp, wp_o), (w1, w1_o), (w2, w2_o), (vec, vec_o)]):
        wos.append(pltpu.make_async_copy(a, b, wsem.at[n + 1]))
        wos[-1].start()
    for t in range(WB // 4):
        cos += saved(t)
    for cp in cos + wos:
        cp.wait()
    gather.finish()


def call_a(pn, x, params, rel):
    any_ = pl.BlockSpec(memory_space=pl.ANY)
    sds = jax.ShapeDtypeStruct
    outs = [sds((D, 3 * D), BF16), sds((D, D), BF16), sds((D, HID), BF16), sds((HID, D), BF16), sds((16, D), F32),
            sds((D, ROWS), BF16), sds((ROWS, D), BF16), sds((WB, 12, 64, 128), BF16), sds((WB, 4, 64, 256), BF16)]
    return pl.pallas_call(
        functools.partial(kernel_a, pn),
        out_shape=outs,
        in_specs=[any_, any_, pl.BlockSpec(memory_space=pltpu.VMEM)],
        out_specs=[any_] * len(outs),
        scratch_shapes=[
            pltpu.VMEM((28, 7, 8, D), BF16), pltpu.VMEM((12 * RS, 128), F32), pltpu.VMEM((4 * RS, 128), F32),
            pltpu.VMEM((16, 64, 256), F32), pltpu.VMEM((D, 3 * D), BF16), pltpu.VMEM((D, D), BF16), pltpu.VMEM((D, HID), BF16), pltpu.VMEM((HID, D), BF16),
            pltpu.VMEM((16, D), F32), pltpu.VMEM((ROWS, D), BF16), pltpu.VMEM((D, ROWS), BF16), pltpu.VMEM((ROWS, D), BF16), pltpu.VMEM((WB, 12, 64, 128), BF16), pltpu.VMEM((WB, 4, 64, 256), BF16),
            pltpu.SemaphoreType.DMA((NSEG,)), pltpu.SemaphoreType.DMA, pltpu.SemaphoreType.DMA((2 + WB // 2,)), pltpu.SemaphoreType.DMA((5,)),
        ] + Gather.scratch(pn),
        compiler_params=pltpu.CompilerParams(vmem_limit_bytes=64000000, collective_id=0, has_side_effects=True),
        name="attend",
    )(x, params.reshape(pn.units * 8, 128), rel)


def rel_lanes(rel_index):
    t = jnp.full((64, 64), -1, jnp.int32).at[:SPAN, :SPAN].set(rel_index.T)
    return t.reshape(1, 4096)


CH = 512
INV_SQRT2 = 0.7071067811865476
INV_SQRT2PI = 0.3989422804014327


def gelu_parts(u):
    e = jnp.exp(u * u * -0.5)
    t = 1.0 / (1.0 + jnp.abs(u) * (0.3275911 * INV_SQRT2))
    half = t * (0.127414796 + t * (-0.142248368 + t * (0.7107068705 + t * (-0.7265760135 + t * 0.5307027145)))) * e
    cdf = jnp.where(u >= 0, 1.0 - half, half)
    return cdf, e * INV_SQRT2PI


def put_block(fs, start, stride, v):
    n = v.shape[0]
    lane = lax.broadcasted_iota(jnp.int32, (n, 128), 1)
    v = pltpu.roll(v, LANE, 1)
    here = pl.ds(start, n, stride=stride) if n > 1 else pl.ds(start, 1)
    fs[here, :] = jnp.where(lane >= LANE, v, fs[here, :])
    here = pl.ds(start + 1, n, stride=stride) if n > 1 else pl.ds(start + 1, 1)
    fs[here, :] = jnp.where(lane < LANE, v, fs[here, :])


def shifted(blocks):
    return [pltpu.roll(v, LANE, 1) for v in blocks]


def put_tile(fs, base, stride, blocks):
    n = blocks[0].shape[0]
    lane = lax.broadcasted_iota(jnp.int32, (n, 128), 1)
    head = lax.broadcasted_iota(jnp.int32, (n, 128), 0) == 0
    one = lax.broadcasted_iota(jnp.int32, (1, 128), 1)
    v = shifted(blocks)
    first = fs[pl.ds(base, 1), :]
    last = fs[pl.ds(base + n * stride, 1), :]
    before = jnp.where(head, first, pltpu.roll(v[-1], 1, 0))
    for c in range(len(blocks)):
        fs[pl.ds(base + c, n, stride=stride), :] = jnp.where(lane >= LANE, v[c], before if c == 0 else v[c - 1])
    fs[pl.ds(base + n * stride, 1), :] = jnp.where(one < LANE, v[-1][n - 1:n], last)


def put_vec(fs, row, v):
    for c in range(v.shape[1] // 128):
        put_block(fs, row + c, 1, v[:, c * 128:(c + 1) * 128])


def acc_rows(ref, i, v):
    ref[8 * i:8 * i + 8, 0:v.shape[1]] += jnp.sum(v.reshape(v.shape[0] // 8, 8, v.shape[1]), 0)


def table_grad(rel_ref, big, dtab):
    lane = lax.broadcasted_iota(jnp.int32, (32, 128), 1)
    for g in range(4):
        for pair in range(2):
            at = 1024 + g * 256 + pair * 128
            big[at:at + 64, :] = dtab[g, :, pair * 128:pair * 128 + 128]
    for g in range(4):
        for pair in range(2):
            at = 1024 + g * 256 + pair * 128
            even = big[pl.ds(at, 32, stride=2), :]
            odd = big[pl.ds(at + 1, 32, stride=2), :]
            h = 4 * g + 2 * pair
            big[pl.ds(h, 32, stride=16), :] = jnp.where(lane < 64, even, pltpu.roll(odd, 64, 1))
            big[pl.ds(h + 1, 32, stride=16), :] = jnp.where(lane < 64, pltpu.roll(even, 64, 1), odd)
    rel = rel_ref[...]
    row = lax.shift_right_arithmetic(rel, 3)
    low = rel & 7
    oh = (lax.broadcasted_iota(jnp.int32, (32, 4096), 0) == row).astype(F32).astype(BF16)
    grad = jnp.concatenate([big[kk * 16:kk * 16 + 16, :] for kk in range(32)], 1)
    out = jnp.zeros((32, 128), F32)
    high = grad.astype(BF16).astype(F32)
    for part in (high, grad - high):
        m = jnp.concatenate([jnp.where(low == j, part, 0.0) for j in range(8)], 0).astype(BF16)
        out = out + dot_nt(oh, m)
    return out


class Chunk:
    def __init__(self, pn, k0, k1, n, at, flip, src, r1, r2, sems, r3, ag):
        self.pn, self.k0, self.k1, self.n, self.at = pn, k0, k1, n, at
        self.steps = list(range(pn.rest.bit_length() - 1))
        if flip:
            self.steps.reverse()
        self.src, self.r1, self.r2, self.r3, self.ag, self.sems = src, r1, r2, r3, ag, sems
        self.k2 = 1
        self.k3 = self.k2 + pn.rest - 1
        self.k4 = self.k3 + pn.ns - 1
        self.k5 = self.k4 + pn.rest - 1

    @staticmethod
    def scratch(pn, n, shared):
        return [pltpu.VMEM((2, pn.rest, n, 8, 128), BF16), pltpu.VMEM((pn.rest, n, 8, 128), BF16), pltpu.VMEM((pn.rest - 1, n, 8, 128), BF16),
                pltpu.SemaphoreType.DMA((2, 2 * pn.rest + pn.ns - 1))] + (
            [] if shared else [pltpu.VMEM((pn.ns - 1, n, 8, 128), BF16), pltpu.VMEM((2, pn.rest, n, 8, 128), BF16)])

    def here(self, z):
        return (z >= self.k0) & (z < self.k1)

    def c1(self):
        r, c, z = place()
        return remote(self.src.at[1 - c], self.r1, self.sems, 0, peer(r, 1 - c))

    def start1(self):
        self.c1().start()

    def owners(self, i, other):
        r, c, z = place()
        bits = [lax.shift_right_arithmetic(r, b) & 1 for b in range(len(self.steps))]
        done, b, free = self.steps[:i], self.steps[i], self.steps[i + 1:]
        base = sum((bits[d] * (1 << d) for d in done), jnp.int32(0))
        base = base + (1 - bits[b] if other else bits[b]) * (1 << b)
        out = [base + sum(((q >> n) & 1) << f for n, f in enumerate(free)) for q in range(1 << len(free))]
        slot = sum(self.pn.rest >> (k + 1) for k in range(i))
        return out, slot

    def c2(self, i, q):
        r, c, z = place()
        own, slot = self.owners(i, True)
        b = self.steps[i]
        bit = lax.shift_right_arithmetic(r, b) & 1
        to = r + (1 - 2 * bit) * (1 << b)
        return remote(self.src.at[c, own[q]], self.r2.at[slot + q], self.sems, self.k2 + slot + q, peer(to, c))

    def add(self, owner, term):
        r, c, z = place()
        self.src[c, owner] = (self.src[c, owner].astype(F32) + term.astype(F32)).astype(BF16)

    def start2(self):
        self.c1().wait()
        for q, owner in enumerate(self.owners(0, True)[0]):
            self.add(owner, self.r1[owner])
            self.c2(0, q).start()
        for owner in self.owners(0, False)[0]:
            self.add(owner, self.r1[owner])

    def landed(self, i):
        own, slot = self.owners(i, False)
        for q in range(len(own)):
            self.c2(i, q).wait()
        for q, owner in enumerate(own):
            self.add(owner, self.r2[slot + q])

    def halve(self):
        for i in range(1, len(self.steps)):
            self.landed(i - 1)
            for q in range(len(self.owners(i, True)[0])):
                self.c2(i, q).start()

    def c3(self, j):
        r, c, z = place()
        to = lax.rem(z + j, self.pn.ns)
        return to, remote(self.src.at[c, r], self.r3.at[j - 1], self.sems, self.k3 + j - 1, {"opt": to})

    def start3(self):
        r, c, z = place()
        self.landed(len(self.steps) - 1)
        for j in range(1, self.pn.ns):
            to, cp = self.c3(j)

            @pl.when(self.here(to))
            def _():
                cp.start()

    def c4(self, j):
        r, c, z = place()
        return remote(self.ag.at[c, r], self.ag.at[c, r], self.sems, self.k4 + j - 1, peer(lax.rem(r + j, self.pn.rest), c))

    def start4(self):
        r, c, z = place()
        for j in range(1, self.pn.ns):
            to, cp = self.c3(j)

            @pl.when(self.here(to))
            def _():
                cp.wait_send()

        @pl.when(self.here(z))
        def _():
            for j in range(1, self.pn.ns):
                self.c3(j)[1].wait_recv()
            v = self.src[c, r].astype(F32)
            for j in range(1, self.pn.ns):
                v = v + self.r3[j - 1].astype(F32)
            self.ag[c, r] = v.astype(BF16)
            for j in range(1, self.pn.rest):
                self.c4(j).start()

    def c5(self):
        r, c, z = place()
        return remote(self.ag.at[c], self.ag.at[c], self.sems, self.k5, peer(r, 1 - c))

    def start5(self):
        r, c, z = place()

        @pl.when(self.here(z))
        def _():
            for j in range(1, self.pn.rest):
                self.c4(j).wait()
            self.c5().start()

    def finish(self):
        r, c, z = place()

        @pl.when(self.here(z))
        def _():
            self.c5().wait()


SMALL = (0, 769, 770, 771, 772)


class Small:
    def __init__(self, pn, own, r1, mid, r2, sems):
        self.pn, self.own, self.r1, self.mid, self.r2, self.sems = pn, own, r1, mid, r2, sems

    @staticmethod
    def scratch(pn):
        u = len(SMALL)
        return [pltpu.VMEM((u, 8, 128), BF16), pltpu.VMEM((pn.ndp, u, 8, 128), BF16), pltpu.VMEM((u, 8, 128), BF16), pltpu.VMEM((pn.ns, u, 8, 128), BF16),
                pltpu.SemaphoreType.DMA((2, pn.ndp + pn.ns - 2))]

    def c1(self, j):
        me = lax.axis_index("dp")
        return remote(self.own, self.r1.at[me], self.sems, j - 1, {"dp": lax.rem(me + j, self.pn.ndp)})

    def w1(self, j):
        me = lax.axis_index("dp")
        return remote(self.own, self.r1.at[lax.rem(me - j + self.pn.ndp, self.pn.ndp)], self.sems, j - 1, {"dp": lax.rem(me + j, self.pn.ndp)})

    def start1(self):
        me = lax.axis_index("dp")
        for j in range(1, self.pn.ndp):
            self.c1(j).start()
        self.r1[me] = self.own[...]

    def c2(self, j):
        z = lax.axis_index("opt")
        to = lax.rem(z + j, self.pn.ns)
        return to, remote(self.mid, self.r2.at[z], self.sems, self.pn.ndp - 2 + j, {"opt": to})

    def w2(self, j):
        z = lax.axis_index("opt")
        return remote(self.mid, self.r2.at[lax.rem(z - j + self.pn.ns, self.pn.ns)], self.sems, self.pn.ndp - 2 + j, {"opt": lax.rem(z + j, self.pn.ns)})

    def start2(self):
        z = lax.axis_index("opt")
        for j in range(1, self.pn.ndp):
            self.c1(j).wait_send()
            self.w1(j).wait_recv()
        v = self.r1[0].astype(F32)
        for n in range(1, self.pn.ndp):
            v = v + self.r1[n].astype(F32)
        self.mid[...] = v.astype(BF16)
        for j in range(1, self.pn.ns):
            to, cp = self.c2(j)

            @pl.when(to <= self.pn.ka)
            def _():
                cp.start()
        self.r2[z] = v.astype(BF16)

    def finish(self):
        z = lax.axis_index("opt")
        for j in range(1, self.pn.ns):
            to, cp = self.c2(j)

            @pl.when(to <= self.pn.ka)
            def _():
                cp.wait_send()

            @pl.when(z <= self.pn.ka)
            def _():
                self.w2(j).wait_recv()

    def total(self, n):
        v = self.r2[0, n].astype(F32)
        for k in range(1, self.pn.ns):
            v = v + self.r2[k, n].astype(F32)
        return v.astype(BF16).astype(F32)


NSEMS = 32


def put_rows_grad(fs, start, v):
    put_rows(fs, start, v)


def kernel_bc(pn, x_hbm, cot_hbm, ob_hbm, wp_hbm, w1_hbm, w2_hbm, hwt_hbm, qkv_hbm, p_hbm, wqkv_hbm, vec, rel_ref, counts,
              y_hbm, dx_hbm, g_hbm, *refs):
    refs = list(refs)
    dx1, wp, acc, dsem = refs[:4]
    refs = refs[4:]
    chunks = []
    nb = 2 * (pn.ns - pn.ka)
    for n, (k0, k1, m, at, flip) in enumerate(part_list(pn)):
        if 1 < n < nb:
            refs[4:4] = [chunks[n % 2].r3, chunks[n % 2].ag]
        chunks.append(Chunk(pn, k0, k1, m, at, flip, *refs[:6]))
        refs = refs[6:]
    shards, ac = chunks[:nb], chunks[nb:]
    his = [ch for ch in shards if ch.k0 >= pn.kh]
    los = [ch for ch in shards if ch.k0 < pn.kh]
    mids, last = los[:-2], los[-2:]

    def each(chs, name):
        return tuple(getattr(ch, name) for ch in chs)

    def run(fns):
        for f in fns:
            f()
    small = Small(pn, *refs)
    count = counts[0]

    def local(n, src, dst):
        return pltpu.make_async_copy(src, dst, dsem.at[n])

    def mlp(x_v, dy_v, ob, a, du, h2, w1, w2, fs, xsem, csem):
        ins = [local(n, s, d) for n, (s, d) in enumerate([(ob_hbm, ob), (wp_hbm, wp), (w1_hbm, w1), (w2_hbm, w2)])]
        cps = window_copies(x_hbm, x_v, xsem, True) + window_copies(cot_hbm, dy_v, csem, True)
        for cp in cps + ins:
            cp.start()
        acc[...] = jnp.zeros_like(acc)
        bp, g2, b2, c2 = (vec[n:n + 1, :] for n in range(4, 8))
        enter(pn, True)
        for cp in cps + ins:
            cp.wait()
        nb = BM // 56

        def rows(t, _):
            r0 = pl.multiple_of(t * BM, BM)
            x = x_v[pl.ds(nb * t, nb)].reshape(BM, D).astype(F32)
            alive = lax.broadcasted_iota(jnp.int32, (nb, 7, 8, D), 2) < count
            dy = jnp.where(alive, dy_v[pl.ds(nb * t, nb)].astype(F32), 0.0)
            dyb = dy.astype(BF16)
            dy_v[pl.ds(nb * t, nb)] = dyb
            dy = dy.reshape(BM, D)
            dyb = dyb.reshape(BM, D)
            x1 = x + dot(ob[pl.ds(r0, BM), :], wp[...]) + bp
            xhat, r = norm_stats(x1)
            h = (xhat * g2 + b2).astype(BF16)
            h2[pl.ds(r0, BM), :] = h
            y = x1 + c2
            dh = jnp.zeros((BM, D), F32)
            for j in range(HID // CH):
                cs = slice(j * CH, (j + 1) * CH)
                u = dot(h, w1[:, cs]) + vec[8 + j:9 + j, :]
                cdf, pdf = gelu_parts(u)
                av = (u * cdf).astype(BF16)
                a[pl.ds(r0, BM), cs] = av
                y = y + dot(av, w2[cs, :])
                da = dot_nt(dyb, w2[cs, :])
                duv = da * (cdf + u * pdf)
                acc_rows(acc, 4 + j, duv)
                dub = duv.astype(BF16)
                du[pl.ds(r0, BM), cs] = dub
                dh = dh + dot_nt(dub, w1[:, cs])
            x_v[pl.ds(nb * t, nb)] = y.reshape(nb, 7, 8, D).astype(BF16)
            acc_rows(acc, 0, dy)
            acc_rows(acc, 1, dh * xhat)
            acc_rows(acc, 2, dh)
            dg = dh * g2
            dt = r * (dg - jnp.mean(dg, -1, keepdims=True) - xhat * jnp.mean(dg * xhat, -1, keepdims=True))
            dxv = dy + dt
            acc_rows(acc, 3, dxv)
            dx1[pl.ds(nb * t, nb)] = dxv.reshape(nb, 7, 8, D)
            return 0
        lax.fori_loop(0, ROWS // BM, rows, 0)
        ycs = window_copies(y_hbm, x_v, xsem, False)
        for cp in ycs:
            cp.start()
        vg = jnp.sum(acc[...].reshape(8, 8, D), 1)
        first = pn.base * 8
        nrow = pn.bunits * 8
        lo_row = (R_PROJ // 8 + 1) * 8 - first
        hi_row = R_END // 8 * 8 - first
        fs[0:lo_row, :] = jnp.zeros((lo_row, 128), F32)
        fs[hi_row:nrow, :] = jnp.zeros((nrow - hi_row, 128), F32)
        dyf = dy_v[...].reshape(ROWS, D)

        def w2rows(t, _):
            r0 = pl.multiple_of(t * 512, 512)
            v = dot_tn(a[:, pl.ds(r0, 512)], dyf)
            put_tile(fs, R_W2 - first + r0 * 4, 4, [v[:, c * 128:(c + 1) * 128] for c in range(4)])
            return 0
        lax.fori_loop(0, HID // 512, w2rows, 0)
        put_vec(fs, R_C2 - first, vg[0:1])

        def fill(ch):
            def piece(p, _):
                row = pl.multiple_of(((ch.k0 - pn.ka) * pn.units + p * pn.pc + ch.at) * 8, 8)
                ch.src[p & 1, lax.shift_right_arithmetic(p, 1)] = fs[pl.ds(row, ch.n * 8), :].reshape(ch.n, 8, 128).astype(BF16)
                return 0
            lax.fori_loop(0, pn.ndp, piece, 0)
            ch.start1()
        for ch in his:
            fill(ch)
        h2t = a.at[0:D, 0:1664]
        transpose_rows(h2, h2t)

        lane = lax.broadcasted_iota(jnp.int32, (D, 128), 1)
        at = R_W1 - first
        keep = fs[pl.ds(at, 1), :]

        def w1rows(t, before):
            r0 = pl.multiple_of(t * 512, 512)
            u = dot(h2t[:, 0:ROWS], du[:, pl.ds(r0, 512)])
            v = shifted([u[:, c * 128:(c + 1) * 128] for c in range(4)])
            for c in range(4):
                fs[pl.ds(at + 4 * t + c, D, stride=16), :] = jnp.where(lane >= LANE, v[c], before if c == 0 else v[c - 1])
            return v[3]
        v = lax.fori_loop(0, HID // 512, w1rows, jnp.zeros((D, 128), F32))
        one = lax.broadcasted_iota(jnp.int32, (1, 128), 1)
        v = jnp.where(lax.broadcasted_iota(jnp.int32, (D, 128), 0) == 0, keep, pltpu.roll(v, 1, 0)), v[D - 1:D]
        fs[pl.ds(at, D, stride=16), :] = jnp.where(lane < LANE, v[0], fs[pl.ds(at, D, stride=16), :])
        fs[pl.ds(at + D * 16, 1), :] = jnp.where(one < LANE, v[1], fs[pl.ds(at + D * 16, 1), :])
        run(each(his, 'start2'))
        v = dot_tn(ob[...], dx1[...].reshape(ROWS, D).astype(BF16))
        put_tile(fs, R_PROJ - first, 4, [v[:, c * 128:(c + 1) * 128] for c in range(4)])
        for row, n in ((R_BP, 3), (R_G2, 1), (R_B2, 2)):
            put_vec(fs, row - first, vg[n:n + 1])
        for j in range(4):
            put_vec(fs, R_C1 - first + 4 * j, vg[4 + j:5 + j])
        for ch in los:
            fill(ch)
        for cp in ycs:
            cp.wait()

    big = pltpu.VMEM((28, 7, 8, D), BF16)
    pl.run_scoped(mlp, big, big, pltpu.VMEM((ROWS, D), BF16), pltpu.VMEM((ROWS, HID), BF16), pltpu.VMEM((ROWS, HID), BF16), pltpu.VMEM((ROWS, D), BF16),
                  pltpu.VMEM((D, HID), BF16), pltpu.VMEM((HID, D), BF16), pltpu.VMEM((pn.bunits * 8, 128), F32),
                  pltpu.SemaphoreType.DMA((NSEG,)), pltpu.SemaphoreType.DMA((NSEG,)))

    def attention(x_v, qkvb, pb, hwt, wqkv, fs, os_, dq, dtab, xsem):
        ins = [local(n, s, d) for n, (s, d) in enumerate([(qkv_hbm, qkvb), (p_hbm, pb), (hwt_hbm, hwt), (wqkv_hbm, wqkv)])]
        for cp in ins:
            cp.start()
        cps = window_copies(x_hbm, x_v, xsem, True)
        for cp in cps:
            cp.start()
        acc[...] = jnp.zeros_like(acc)
        dtab[...] = jnp.zeros_like(dtab)

        def rows0(t, _):
            r0 = pl.multiple_of(t * 392, 8)
            ev = dx1[pl.ds(7 * t, 7)].reshape(392, D).astype(BF16)
            v = dot_nt(ev, wp[...])
            for g in range(4):
                os_[pl.ds(g * RS + r0, 392), :] = v[:, g * 128:(g + 1) * 128]
            return 0
        lax.fori_loop(0, 4, rows0, 0)
        ins[0].wait()
        ins[1].wait()
        run(each(his, 'halve') + each(los, 'start2'))
        heads = lane_head()

        def several(g, items):
            bases = [lax.shift_right_arithmetic(i, 3) * WROWS + (i & 7) for i in items]
            dobds = [block_diag(take_rows(os_, g * RS + base).astype(BF16), heads) for base in bases]
            dps = [dot_nt(qkvb[i, 8 + g], d) for i, d in zip(items, dobds)]
            total = dtab[g]
            dsbs = []
            for i, dp in zip(items, dps):
                p = pb[i, g].astype(F32)
                t = p * dp
                ds = t - p * jnp.sum(t, 0, keepdims=True)
                total = total + ds
                dsbs.append(ds.astype(BF16))
            dtab[g] = total
            dvs = [dot(pb[i, g], d) for i, d in zip(items, dobds)]
            dks = [dot(d, block_diag(qkvb[i, g], heads)) for i, d in zip(items, dsbs)]
            dqs = [dot_tn(d, qkvb[i, 4 + g]) for i, d in zip(items, dsbs)]
            for base, dv, dk, dqv in zip(bases, dvs, dks, dqs):
                put_rows(fs, 2 * RS + base, dv)
                put_rows(fs, RS + base, dk)
                put_rows(fs, base, diag_sum(dqv, heads) * SCALE)

        mid = {0: each(his, 'start3'), 1: each(mids, 'halve') + (ac[0].start2,), 2: each(last, 'halve') + (ac[1].start2,) + each(his, 'start4'),
               3: each(mids, 'start3') + (ac[0].halve, ac[2].start2)}
        for g in range(4):
            def attend(t, _):
                @pl.when(t == 1)
                def _():
                    for f in mid[g]:
                        f()
                several(g, [16 * t + n for n in range(16)])
                return 0
            lax.fori_loop(0, WB // 16, attend, 0)
            parts = []
            for n in range(3):
                v = fs[n * RS:n * RS + ROWS, :]
                if n != 1:
                    acc[8 * (2 + n // 2):8 * (3 + n // 2), g * 128:(g + 1) * 128] = jnp.sum(v.reshape(ROWS // 8, 8, 128), 0)
                v = v.astype(BF16)
                dq[:, n * D + g * 128:n * D + (g + 1) * 128] = v
                parts.append(v)
            if g == 0:
                ins[2].wait()
                ins[3].wait()
            v = dot(hwt[...], jnp.concatenate(parts, 1))
            mu = pn.mrow // 8
            for n in range(3):
                u = v[:, n * 128:(n + 1) * 128].reshape(D // 8, 8, 128).astype(BF16)
                for p in range(pn.ndp):
                    ac[g].src[p & 1, p >> 1, n * mu:(n + 1) * mu] = u[p * mu:(p + 1) * mu]
            ac[g].start1()
        run(each(last, 'start3') + (ac[0].start3, ac[1].halve))
        for cp in cps:
            cp.wait()
        gain = vec[0:1, :]
        tab = table_grad(rel_ref, os_, dtab)
        for n in range(3):
            small.own[2 + n] = tab[8 * n:8 * n + 8].astype(BF16)
        late = {0: (ac[3].start2,), 1: (ac[1].start3, ac[2].halve), 2: (ac[3].halve,) + each(his, 'start5'), 3: each(mids, 'start4') + (ac[2].start3,),
                4: (ac[0].start4, ac[3].start3), 5: each(last, 'start4'), 6: (ac[1].start4,) + each(mids, 'start5')}

        def rows1(t, _):
            for k, fns in late.items():
                @pl.when(t == k)
                def _():
                    for f in fns:
                        f()
            r0 = pl.multiple_of(t * BLK, BLK)
            dn = dot_nt(dq[pl.ds(r0, BLK), :], wqkv[...])
            x = x_v[pl.ds(4 * t, 4)].reshape(BLK, D).astype(F32)
            xhat, r = norm_stats(x)
            acc_rows(acc, 0, dn * xhat)
            acc_rows(acc, 1, dn)
            dg = dn * gain
            dt = r * (dg - jnp.mean(dg, -1, keepdims=True) - xhat * jnp.mean(dg * xhat, -1, keepdims=True))
            dx1[pl.ds(4 * t, 4)] += dt.reshape(4, 7, 8, D)
            return 0
        lax.fori_loop(0, NBLK, rows1, 0)
        vg = jnp.sum(acc[...].reshape(8, 8, D), 1)
        flat = [vg[n:n + 1, c * 128:(c + 1) * 128] for n in range(4) for c in range(4)]
        small.own[0] = jnp.concatenate(flat[:8], 0).astype(BF16)
        small.own[1] = jnp.concatenate(flat[8:], 0).astype(BF16)
        small.start1()
        ycs = window_copies(dx_hbm, dx1, xsem, False)
        for cp in ycs:
            cp.start()
        run((ac[2].start4, ac[3].start4, ac[0].start5, ac[1].start5, small.start2) + each(last, 'start5') + (ac[2].start5, ac[3].start5))
        for ch in shards:
            ch.finish()
        r, c, z = place()
        g = os_

        @pl.when(z >= pn.ka)
        def _():
            def piece(p, _):
                for ch in shards[:2]:
                    g[pl.ds(pl.multiple_of((p * pn.pc + ch.at) * 8, 8), ch.n * 8), :] = ch.ag[p & 1, lax.shift_right_arithmetic(p, 1)].astype(F32).reshape(ch.n * 8, 128)
                return 0
            lax.fori_loop(0, pn.ndp, piece, 0)
        mu = pn.mrow // 8

        for h in range(4):
            ac[h].finish()

            @pl.when(z < pn.ka)
            def _():
                def piece(p, _):
                    for n in range(3):
                        v = ac[h].ag[p & 1, lax.shift_right_arithmetic(p, 1), n * mu:(n + 1) * mu].astype(F32).reshape(pn.mrow, 128)
                        g[pl.ds(R_QKV + p * pn.mrow * 12 + n * 4 + h, pn.mrow, stride=12), :] = v
                    return 0
                lax.fori_loop(0, pn.ndp, piece, 0)
        small.finish()

        @pl.when(z < pn.ka)
        def _():
            for n, u in enumerate(SMALL):
                g[u * 8:u * 8 + 8, :] = small.total(n)

        @pl.when(z == pn.ka)
        def _():
            for n, u in enumerate(SMALL):
                if u >= pn.base:
                    k = (u - pn.base) * 8
                    g[k:k + 8, :] += small.total(n)
        out = local(0, g.at[pl.ds(pl.multiple_of(lax.select(z < pn.ka, z * (pn.units * 8), 0), 8), pn.units * 8)], g_hbm)
        out.start()
        out.wait()
        for cp in ycs:
            cp.wait()

    pl.run_scoped(attention, big, pltpu.VMEM((WB, 12, 64, 128), BF16), pltpu.VMEM((WB, 4, 64, 256), BF16), pltpu.VMEM((D, ROWS), BF16), pltpu.VMEM((D, 3 * D), BF16),
                  pltpu.VMEM((3 * RS, 128), F32), pltpu.VMEM((max(4 * RS, pn.gunits * 8), 128), F32), pltpu.VMEM((ROWS, 3 * D), BF16), pltpu.VMEM((4, 64, 256), F32), pltpu.SemaphoreType.DMA((NSEG,)))


def part_list(pn):
    mu = 3 * pn.mrow // 8
    h = (pn.pc + 1) // 2
    out = []
    for k in range(pn.ns - 1, pn.ka - 1, -1):
        out += [(k, k + 1, h, 0, False), (k, k + 1, pn.pc - h, h, True)]
    return out + [(0, pn.ka, mu, 0, g % 2 == 1) for g in range(4)]


def call_bc(pn, x, cot, ob, wp, w1, w2, hwt, qkv, p, wqkv, vec, rel, counts):
    any_ = pl.BlockSpec(memory_space=pl.ANY)
    vm = pl.BlockSpec(memory_space=pltpu.VMEM)
    sds = jax.ShapeDtypeStruct
    outs = [sds((14, 14, 8, D), BF16), sds((14, 14, 8, D), F32), sds((pn.units * 8, 128), F32)]
    scratch = [pltpu.VMEM((28, 7, 8, D), F32), pltpu.VMEM((D, D), BF16), pltpu.VMEM((64, D), F32), pltpu.SemaphoreType.DMA((4,))]
    for n, (k0, k1, m, at, flip) in enumerate(part_list(pn)):
        scratch += Chunk.scratch(pn, m, 1 < n < 2 * (pn.ns - pn.ka))
    scratch += Small.scratch(pn)
    return pl.pallas_call(
        functools.partial(kernel_bc, pn),
        out_shape=outs,
        in_specs=[any_] * 10 + [vm, vm, pl.BlockSpec(memory_space=pltpu.SMEM)],
        out_specs=[any_] * 3,
        scratch_shapes=scratch,
        compiler_params=pltpu.CompilerParams(vmem_limit_bytes=67000000, collective_id=1, has_side_effects=True),
        name="back",
    )(x, cot, ob, wp, w1, w2, hwt, qkv, p, wqkv, vec, rel, counts)


STEP = 2
DECAYED = (2, 6, 10, 12)
LENGTHS = [D, D, 3 * D * D, D, D, TAB * HEADS, D * D, D, D, D, D * HID, HID, HID * D, D]
AU = 129


def kernel_adam(rates, first, g, p, m1, m2, g_o, p_o, m_o, v_o):
    shape = (AU, 8, 128)
    u0 = first[0] + pl.program_id(0) * AU
    starts = [sum(LENGTHS[:n + 1]) for n in range(len(LENGTHS))]

    def group(at):
        k = jnp.int32(0)
        for s in starts:
            k = k + (at >= s).astype(jnp.int32)
        return k

    def update(rate, decay):
        grad = g[...]
        w = p[...]
        m = 0.9 * m1[...] + 0.1 * grad
        v = 0.999 * m2[...] + 0.001 * grad * grad
        mh = m / (1.0 - 0.9 ** STEP)
        vh = v / (1.0 - 0.999 ** STEP)
        p_o[...] = w - rate * (mh / (jnp.sqrt(vh) + 1e-08) + decay * w)
        m_o[...] = m
        v_o[...] = v
        g_o[...] = grad
    k0 = group(u0 * 1024)
    k1 = group((u0 + AU) * 1024 - 1)

    @pl.when(k0 == k1)
    def _():
        decay = jnp.float32(0.0)
        for n in DECAYED:
            decay = jnp.where(k0 == n, jnp.float32(0.05), decay)
        update(rates[k0], decay)

    @pl.when(k0 != k1)
    def _():
        index = ((u0 + lax.broadcasted_iota(jnp.int32, shape, 0)) * 8 + lax.broadcasted_iota(jnp.int32, shape, 1)) * 128 + lax.broadcasted_iota(jnp.int32, shape, 2)
        rate = jnp.zeros(shape, F32) + rates[0]
        decay = jnp.zeros(shape, F32)
        for n, s in enumerate(starts):
            after = index >= s
            rate = jnp.where(after, rates[n + 1], rate)
            if n in DECAYED or n + 1 in DECAYED:
                decay = jnp.where(after, 0.05 if n + 1 in DECAYED else 0.0, decay)
        update(rate, decay)


def call_adam(pn, rates, g, params, mom1, mom2):
    view = lambda t: t.reshape(pn.units, 8, 128)
    spec = pl.BlockSpec((AU, 8, 128), lambda i: (i, 0, 0))
    sm = pl.BlockSpec(memory_space=pltpu.SMEM)
    first = (lax.axis_index("opt") * pn.units).astype(jnp.int32).reshape(1)
    out = pl.pallas_call(
        kernel_adam,
        grid=(pl.cdiv(pn.units, AU),),
        out_shape=[jax.ShapeDtypeStruct((pn.units, 8, 128), F32)] * 4,
        in_specs=[sm, sm] + [spec] * 4,
        out_specs=[spec] * 4,
        compiler_params=pltpu.CompilerParams(vmem_limit_bytes=67043328),
        name="adamw",
    )(rates, first, view(g), view(params), view(mom1), view(mom2))
    return [t.reshape(-1) for t in out]


from jax.sharding import PartitionSpec as P


def solution(mesh):
    def local(images, cotangent, counts, rel_index, params, moment1, moment2, rates):
        pn = Plan(mesh, params.shape[0])
        xt = images.transpose(1, 2, 0, 3)
        ct = cotangent.transpose(1, 2, 0, 3)
        rel = rel_lanes(rel_index)
        wqkv, wp, w1, w2, vec, hwt, ob, qkv, p = call_a(pn, xt, params, rel)
        y, dx, g = call_bc(pn, xt, ct, ob, wp, w1, w2, hwt, qkv, p, wqkv, vec, rel, counts)
        grad, new_params, new_first, new_second = call_adam(pn, rates, g, params, moment1, moment2)
        return (y.transpose(2, 0, 1, 3), dx.transpose(2, 0, 1, 3), grad, new_params, new_first, new_second)

    split = P(("dp", "opt"), None, None, None)
    return jax.shard_map(
        local, mesh=mesh,
        in_specs=(split, split, P(("dp", "opt")), P(), P("opt"), P("opt"), P("opt"), P()),
        out_specs=(split, split, P("opt"), P("opt"), P("opt"), P("opt")),
        check_vma=False)
```
